32 devices in a mesh: grp: 4 (over z), kv: 4 (over y, x), tp: 2 (over core).
Axes of the slice: x: 2, y: 2, z: 4, core: 2. Of those that a mesh axis runs over, the one named last changes fastest.
Arguments:
- hidden_states: bfloat16 [512, 4096], P('grp', 'kv'), may hold values from -6 to 6
- attn_gain: float32 [4096], P('kv'), may hold values from 0.25 to 1.75
- mlp_gain: float32 [4096], replicated, may hold values from 0.25 to 1.75
- w_query: bfloat16 [4096, 4096], P('kv', 'tp'), may hold values from -0.09375 to 0.09375
- w_out: bfloat16 [32, 128, 4096], P('tp', 'kv'), may hold values from -1 to 1
- w_gate: bfloat16 [4096, 14336], P(None, ('kv', 'tp')), may hold values from -0.09375 to 0.09375
- w_up: bfloat16 [4096, 14336], P(None, ('kv', 'tp')), may hold values from -0.09375 to 0.09375
- w_down: bfloat16 [14336, 4096], P(('kv', 'tp')), may hold values from -0.046875 to 0.046875
- kv_pool: bfloat16 [256, 2, 128, 1024], P(('grp', 'kv'), None, None, 'tp'), may hold values from -110 to 110
- resident_cache: bfloat16 [4, 32, 2, 128, 1024], P('grp', 'kv', None, None, 'tp'), may hold values from -110 to 110
- resident_slot: int32 [4, 32], P('grp', 'kv'), may hold values from 0 to 127
- resident_len: int32 [4, 32], P('grp', 'kv'), may hold values from 1 to 128
- new_owner: int32 [4, 64], replicated, may hold values from 0 to 15, as said below
- new_local: int32 [4, 64], replicated, may hold values from 0 to 15
- new_slot: int32 [4, 64], P('grp', 'kv'), may hold values from 0 to 127
- new_len: int32 [4, 64], P('grp', 'kv'), may hold values from 1 to 128
- token_kv: bfloat16 [512, 2, 1024], P('grp', None, 'tp'), may hold values from -6 to 6
Outputs:
- mixed: bfloat16 [512, 4096], P(('grp', 'kv', 'tp'))
- new_cache: bfloat16 [4, 64, 2, 128, 1024], P('grp', 'kv', None, None, 'tp')
The draws below stay inside these ranges and needn't reach their ends.
Inputs may be any that keep to these rules, and one draw needn't show every extreme that they name: New page c of group g is kept by the device of kv index c // 16 of group g and comes from the device whose index along grp+kv is new_owner[g, c]; every decode device receives exactly 4 new pages from the owners of each grp index; no owner sends more than 4 pages to the devices of one kv index over all groups, so at most 4 to one device; every owner sends each of its 16 pages exactly once.
All inputs are finite; a program needn't handle non-finite values.
Results may differ from the reference program's by a relative error of at most 0.018.
Values may be sent and summed in bfloat16 or wider, within the bound.
A program may use at most 128 MiB of HBM per device.

```python
import jax
import jax.numpy as jnp
from jax import lax

D = 4096
HEADS = 32
KV_HEADS = 8
HEAD_DIM = 128
FF = 14336
PAGE = 128
NPR = 4
SLOT_G = 128
GROUPS = 4
KV_RANKS = 4
SLOTS = 512
NEW_DEV = 16
CAP1 = 4
POOL = 256
CACHE_G = 32
NEWC = 64


def page_values(key, count):
    width = KV_HEADS * HEAD_DIM
    values = jnp.clip(jax.random.normal(key, (count, 2, PAGE, width), jnp.float32), -6.0, 6.0)
    return values.astype(jnp.bfloat16)


def draw_kv_pool(key, part):
    return page_values(jax.random.fold_in(key, 3), POOL)


def draw_resident_cache(key, part):
    values = page_values(jax.random.fold_in(key, 5), GROUPS * CACHE_G)
    return values.reshape(GROUPS, CACHE_G, 2, PAGE, KV_HEADS * HEAD_DIM)


def batch_perms(key, count, length):
    subkeys = jax.random.split(key, count)
    return jax.vmap(lambda subkey: jax.random.permutation(subkey, length))(subkeys)


def route_tables(key):
    key = jax.random.fold_in(key, 11)
    keys = jax.random.split(key, 4)
    cap = CAP1
    col_perm = batch_perms(keys[0], GROUPS * KV_RANKS, KV_RANKS).reshape(GROUPS, KV_RANKS, KV_RANKS)
    shift = jax.random.randint(keys[1], (GROUPS, KV_RANKS), 0, KV_RANKS)
    dest_perm = batch_perms(keys[2], GROUPS * KV_RANKS, NEW_DEV).reshape(GROUPS, KV_RANKS, NEW_DEV)
    local_perm = batch_perms(keys[3], GROUPS * KV_RANKS, NEW_DEV)
    src_grp = jnp.arange(GROUPS).reshape(GROUPS, 1, 1, 1)
    dst_col = jnp.arange(KV_RANKS).reshape(1, KV_RANKS, 1, 1)
    dst_grp = jnp.arange(GROUPS).reshape(1, 1, GROUPS, 1)
    within = jnp.arange(NPR).reshape(1, 1, 1, NPR)
    flat = dst_grp * NPR + within
    turned = (flat + shift[src_grp, dst_col] * cap) % NEW_DEV
    block = turned // cap
    place = turned % cap
    src_col = col_perm[src_grp, dst_col, block]
    owner = src_grp * KV_RANKS + src_col
    local_ids = local_perm[owner, dst_col * cap + place]
    slot_in = dest_perm[dst_grp, dst_col, src_grp * NPR + within]
    column = dst_col * NEW_DEV + slot_in
    full_rows = jnp.broadcast_to(dst_grp, owner.shape)
    owners = jnp.zeros((GROUPS, KV_RANKS * NEW_DEV), jnp.int32).at[full_rows, column].set(owner.astype(jnp.int32))
    locals_out = jnp.zeros((GROUPS, KV_RANKS * NEW_DEV), jnp.int32).at[full_rows, column].set(local_ids.astype(jnp.int32))
    return (owners, locals_out)


def draw_new_owner(key, part):
    return route_tables(key)[0]


def draw_new_local(key, part):
    return route_tables(key)[1]


def set_ends(drawn, key, least, high):
    longest = drawn.shape.index(max(drawn.shape))
    spots = []
    for shift in (0, 1):
        where = [jax.random.randint(jax.random.fold_in(key, axis), (), 0, length) for axis, length in enumerate(drawn.shape)]
        where[longest] = (where[longest] + shift) % drawn.shape[longest]
        spots.append(tuple(where))
    return drawn.at[spots[0]].set(least).at[spots[1]].set(high)


def block_levels(key, dims, shards, smallest, largest):
    factor_of, own = 1.0, jax.random.fold_in(key, 6)
    for position, blocks in shards:
        steps = jnp.exp(jax.random.uniform(jax.random.fold_in(own, position), (blocks,), jnp.float32, smallest / len(shards), largest / len(shards)))
        factor_of = factor_of * jnp.repeat(steps, dims[position] // blocks).reshape([-1 if axis == position else 1 for axis in range(len(dims))])
    return factor_of


def gaussian(stream_key, shape, spread, most, pieces=(), held_as=jnp.bfloat16):
    values = spread * jax.random.normal(stream_key, shape, jnp.float32)
    if pieces:
        values = values * block_levels(stream_key, shape, pieces, -0.22, 0.18)
    return jnp.clip(values, -most, most).astype(held_as)


def setup_inputs(seed: int = 0) -> dict:
    key_list = jax.random.split(jax.random.key(seed), 18)
    return {
        "hidden_states": gaussian(key_list[0], (SLOTS, D), 1.0, 6.0, ((0, 4), (1, 4))),
        "attn_gain": jnp.clip(1.0 + 0.15 * jax.random.normal(key_list[1], (D,), jnp.float32), 0.25, 1.75),
        "mlp_gain": jnp.clip(1.0 + 0.15 * jax.random.normal(key_list[2], (D,), jnp.float32), 0.25, 1.75),
        "w_query": gaussian(key_list[3], (D, HEADS * HEAD_DIM), D ** -0.5, 0.09375, ((0, 4), (1, 2))),
        "w_out": gaussian(key_list[4], (HEADS, HEAD_DIM, D), HEADS ** -0.5, 1.0, ((0, 2), (1, 4))),
        "w_gate": gaussian(key_list[5], (D, FF), D ** -0.5, 0.09375, ((1, 8),)),
        "w_up": gaussian(key_list[6], (D, FF), D ** -0.5, 0.09375, ((1, 8),)),
        "w_down": gaussian(key_list[7], (FF, D), FF ** -0.5, 0.046875, ((0, 8),)),
        "kv_pool": draw_kv_pool(jax.random.fold_in(key_list[17], 71), 0),
        "resident_cache": draw_resident_cache(jax.random.fold_in(key_list[17], 71), 0),
        "resident_slot": set_ends(jax.random.randint(key_list[10], (GROUPS, CACHE_G), 0, SLOT_G), jax.random.fold_in(key_list[10], 1), 0, SLOT_G - 1).astype(jnp.int32),
        "resident_len": set_ends(jax.random.randint(key_list[11], (GROUPS, CACHE_G), 1, PAGE + 1), jax.random.fold_in(key_list[11], 1), 1, PAGE).astype(jnp.int32),
        "new_owner": draw_new_owner(jax.random.fold_in(key_list[17], 71), 0),
        "new_local": draw_new_local(jax.random.fold_in(key_list[17], 71), 0),
        "new_slot": set_ends(jax.random.randint(key_list[14], (GROUPS, NEWC), 0, SLOT_G), jax.random.fold_in(key_list[14], 1), 0, SLOT_G - 1).astype(jnp.int32),
        "new_len": set_ends(jax.random.randint(key_list[15], (GROUPS, NEWC), 1, PAGE + 1), jax.random.fold_in(key_list[15], 1), 1, PAGE).astype(jnp.int32),
        "token_kv": gaussian(key_list[16], (SLOTS, 2, KV_HEADS * HEAD_DIM), 1.0, 6.0, ((0, 4), (2, 2))),
    }


neg_fill = -1e+30
norm_eps = 1e-05

def local_partials(query, resident, arrived, res_slot, res_len, arr_slot, arr_len, token_kv, first):
    pages = jnp.concatenate([resident, arrived], axis=0)
    owner_slot = jnp.concatenate([res_slot, arr_slot]).astype(jnp.int32)
    filled = jnp.concatenate([res_len, arr_len]).astype(jnp.int32)
    count = pages.shape[0]
    tokens = pages.shape[2]
    kv_here = pages.shape[3] // HEAD_DIM
    slots = query.shape[0]
    ratio = HEADS // KV_HEADS
    keys = pages[:, 0].astype(jnp.float32).reshape(count, tokens, kv_here, HEAD_DIM)
    values = pages[:, 1].astype(jnp.float32).reshape(count, tokens, kv_here, HEAD_DIM)
    grouped = query.reshape(slots, kv_here, ratio, HEAD_DIM)
    picked = jnp.take(grouped, owner_slot, axis=0)
    scores = jnp.einsum('ikgd,itkd->ikgt', picked, keys, precision=lax.Precision.HIGHEST)
    usable = (jnp.arange(tokens, dtype=jnp.int32)[None, :] < filled[:, None])[:, None, None, :]
    scores = jnp.where(usable, scores, neg_fill)
    page_top = lax.optimization_barrier(jnp.max(scores, axis=3))
    member = owner_slot[None, :] == jnp.arange(slots, dtype=jnp.int32)[:, None]
    slot_top = lax.optimization_barrier(jnp.max(jnp.where(member[:, :, None, None], page_top[None], neg_fill), axis=1))
    own_keys = token_kv[:, 0].astype(jnp.float32).reshape(slots, kv_here, HEAD_DIM)
    own_values = token_kv[:, 1].astype(jnp.float32).reshape(slots, kv_here, HEAD_DIM)
    own_score = jnp.einsum('skgd,skd->skg', grouped, own_keys, precision=lax.Precision.HIGHEST)
    own_score = jnp.where(first, own_score, neg_fill)
    slot_top = jnp.maximum(slot_top, own_score)
    reach = jnp.take(slot_top, owner_slot, axis=0)
    weights = jnp.where(usable, jnp.exp(scores - reach[..., None]), 0.0)
    page_sum = lax.optimization_barrier(jnp.sum(weights, axis=3))
    page_acc = jnp.einsum('ikgt,itkd->ikgd', weights, values, precision=lax.Precision.HIGHEST)
    own_weight = jnp.where(first, jnp.exp(own_score - slot_top), 0.0)
    member_f = member.astype(jnp.float32)
    total = jnp.dot(member_f, page_sum.reshape(count, -1), precision=lax.Precision.HIGHEST)
    total = total + own_weight.reshape(slots, -1)
    weighted = jnp.dot(member_f, page_acc.reshape(count, -1), precision=lax.Precision.HIGHEST)
    weighted = weighted.reshape(slots, kv_here, ratio, HEAD_DIM) + own_weight[..., None] * own_values[:, :, None, :]
    return (slot_top.reshape(slots, -1), total, weighted.reshape(slots, kv_here * ratio, HEAD_DIM))

def reference(hidden_states, attn_gain, mlp_gain, w_query, w_out, w_gate, w_up, w_down, kv_pool, resident_cache, resident_slot, resident_len, new_owner, new_local, new_slot, new_len, token_kv):
    groups = SLOTS // SLOT_G
    features = hidden_states.astype(jnp.float32)
    attn_scale = lax.rsqrt(lax.optimization_barrier(jnp.sum(features * features, axis=1)) / D + norm_eps)
    normed = (features * attn_gain).astype(jnp.bfloat16)
    query = jnp.dot(normed, w_query, preferred_element_type=jnp.float32) * attn_scale[:, None] * HEAD_DIM ** (-0.5)
    index = (new_owner * NEW_DEV + new_local).reshape(-1).astype(jnp.int32)
    new_cache = jnp.take(kv_pool, index, axis=0).reshape(groups, NEWC, 2, PAGE, KV_HEADS * HEAD_DIM)

    def attend(packed):
        grp_query, resident, arrived, res_slot, res_len, arr_slot, arr_len, own_kv = packed
        top, total, weighted = local_partials(grp_query, resident, arrived, res_slot, res_len, arr_slot, arr_len, own_kv, True)
        return (weighted / total[..., None]).astype(jnp.bfloat16)
    attn = lax.map(attend, (query.reshape(groups, SLOT_G, HEADS * HEAD_DIM), resident_cache, new_cache, resident_slot, resident_len, new_slot, new_len, token_kv.reshape(groups, SLOT_G, 2, KV_HEADS * HEAD_DIM)))
    attn = attn.reshape(SLOTS, HEADS * HEAD_DIM)
    branch = jnp.dot(attn, w_out.reshape(HEADS * HEAD_DIM, D), preferred_element_type=jnp.float32)
    resid = (features + branch).astype(jnp.bfloat16)
    resid_f = resid.astype(jnp.float32)
    mlp_scale = lax.rsqrt(lax.optimization_barrier(jnp.sum(resid_f * resid_f, axis=1)) / D + norm_eps)
    normed_mlp = (resid_f * mlp_gain).astype(jnp.bfloat16)
    gate = jnp.dot(normed_mlp, w_gate, preferred_element_type=jnp.float32) * mlp_scale[:, None]
    upward = jnp.dot(normed_mlp, w_up, preferred_element_type=jnp.float32) * mlp_scale[:, None]
    hidden_units = (jax.nn.silu(gate) * upward).astype(jnp.bfloat16)
    mixed = (resid_f + jnp.dot(hidden_units, w_down, preferred_element_type=jnp.float32)).astype(jnp.bfloat16)
    return (mixed, new_cache)
```

```python
import functools

import jax
import jax.numpy as jnp
from jax import lax
from jax.experimental import pallas as pl
from jax.experimental.pallas import tpu as pltpu
from jax.sharding import PartitionSpec as P

D = 4096
HEADS = 32
KV_HEADS = 8
HEAD_DIM = 128
NPR = 4


neg_fill = -1e30
norm_eps = 1e-05


def push_kernel(axes, spread, src, out, send_sem, recv_sem, own_sem):
    sizes = [lax.axis_size(axis) for axis in axes]
    count = 1
    me = jnp.int32(0)
    for axis, size in zip(axes, sizes):
        me = me * size + lax.axis_index(axis)
        count *= size

    def device(index):
        where = {}
        for axis, size in reversed(list(zip(axes, sizes))):
            where[axis] = lax.rem(index, size)
            index = index // size
        return where

    barrier = pltpu.get_barrier_semaphore()
    for step in range(1, count):
        pl.semaphore_signal(
            barrier,
            inc=1,
            device_id=device(lax.rem(me + step, count)),
            device_id_type=pl.DeviceIdType.MESH,
        )
    pl.semaphore_wait(barrier, count - 1)
    copies = []
    for step in range(1, count):
        peer = lax.rem(me + step, count)
        copy = pltpu.make_async_remote_copy(
            src_ref=src if spread else src.at[peer],
            dst_ref=out.at[me],
            send_sem=send_sem.at[step],
            recv_sem=recv_sem.at[step],
            device_id=device(peer),
            device_id_type=pl.DeviceIdType.MESH,
        )
        copy.start()
        copies.append(copy)
    own = pltpu.make_async_copy(src if spread else src.at[me], out.at[me], own_sem)
    own.start()
    own.wait()
    for step in range(1, count):
        source = lax.rem(me - step + count, count)
        pltpu.make_async_remote_copy(
            src_ref=src if spread else src.at[source],
            dst_ref=out.at[source],
            send_sem=send_sem.at[step],
            recv_sem=recv_sem.at[step],
            device_id=device(source),
            device_id_type=pl.DeviceIdType.MESH,
        ).wait_recv()
    for copy in copies:
        copy.wait_send()


def push(blocks, axes, call_id, spread=False):
    count = 1
    for axis in axes:
        count *= lax.axis_size(axis)
    shape = (count,) + blocks.shape if spread else blocks.shape
    moved = 2 * blocks.size * blocks.dtype.itemsize
    return pl.pallas_call(
        functools.partial(push_kernel, axes, spread),
        out_shape=jax.ShapeDtypeStruct(shape, blocks.dtype),
        in_specs=[pl.BlockSpec(memory_space=pltpu.VMEM)],
        out_specs=pl.BlockSpec(memory_space=pltpu.VMEM),
        scratch_shapes=[
            pltpu.SemaphoreType.DMA((count,)),
            pltpu.SemaphoreType.DMA((count,)),
            pltpu.SemaphoreType.DMA,
        ],
        cost_estimate=pl.CostEstimate(flops=0, bytes_accessed=moved, transcendentals=0),
        compiler_params=pltpu.CompilerParams(collective_id=call_id, has_side_effects=True),
        name="push_%d" % call_id,
    )(blocks)


def nth_match(table, wanted, places):
    matched = (table == wanted).astype(jnp.int32)
    ranking = jnp.cumsum(matched, axis=1) - 1
    return (matched[:, None, :] == 1) & (ranking[:, None, :] == places[None, :, None])


def arrival_places(new_owner):
    groups = lax.axis_size("grp")
    ranks = lax.axis_size("kv")
    per_dev = new_owner.shape[1] // ranks
    owners = new_owner.reshape(groups * ranks, per_dev)
    myself = lax.axis_index("grp") * ranks + lax.axis_index("kv")
    mine = lax.dynamic_index_in_dim(owners, myself, 0, keepdims=False)
    order = jnp.arange(per_dev, dtype=jnp.int32)
    src_grp = mine // ranks
    earlier = (src_grp[:, None] == src_grp[None, :]) & (order[:, None] < order[None, :])
    before = jnp.sum(earlier.astype(jnp.int32), axis=0)
    return src_grp * NPR + before


def lanes(values, width):
    return jnp.pad(values, [(0, 0)] * (values.ndim - 1) + [(0, width - values.shape[-1])])


NEAR_ROWS = 8


def split2(x):
    high = x.astype(jnp.bfloat16)
    return high, (x - high.astype(jnp.float32)).astype(jnp.bfloat16)


def split3(x):
    high = x.astype(jnp.bfloat16)
    rest = x - high.astype(jnp.float32)
    middle = rest.astype(jnp.bfloat16)
    return high, middle, (rest - middle.astype(jnp.float32)).astype(jnp.bfloat16)


def mm(a, b):
    return jnp.dot(a, b, preferred_element_type=jnp.float32)


def mm_nt(a, b):
    return lax.dot_general(a, b, (((1,), (1,)), ((), ())), preferred_element_type=jnp.float32)


def rows_of(shape):
    return lax.broadcasted_iota(jnp.int32, shape, 0)


def lanes_of(shape):
    return lax.broadcasted_iota(jnp.int32, shape, 1)


def half_turn(x):
    return pltpu.roll(x, 4, 0)


def fold(tile, odd):
    if tile.shape[1] < 256:
        return tile
    half = tile.shape[1] // 2
    low, high = tile[:, :half], tile[:, half:]
    top = rows_of(low.shape) < 4
    if odd:
        return jnp.where(top, half_turn(low), high)
    return jnp.where(top, low, half_turn(high))


def pick_rows(first, second, odd):
    first = jnp.where(odd, half_turn(first), first)
    second = jnp.where(odd, second, half_turn(second))
    return jnp.where(rows_of(first.shape) < 4, first, second)


def unfold(first, second, width, odd):
    if width < 256:
        return pick_rows(first, second, odd)
    top = rows_of(first.shape) < 4
    low = jnp.where(top, first, half_turn(second))
    high = jnp.where(top, half_turn(first), second)
    return jnp.concatenate([low, high], axis=1)


def column_of(row, offset):
    wide = jnp.broadcast_to(row, (8, 128)).astype(jnp.float32)
    hit = lanes_of((8, 128)) == rows_of((8, 128)) + offset
    return jnp.sum(jnp.where(hit, wide, 0.0), axis=1, keepdims=True)


def place_in_group(groups, ranks):
    grp = lax.axis_index("grp")
    kv = lax.axis_index("kv")
    me = grp * ranks + kv

    def flat(index):
        return {"grp": index // ranks, "kv": lax.rem(index, ranks)}

    return grp, kv, me, flat


def front_kernel(
    dims,
    picked,
    inverse,
    meta,
    hidden,
    gain,
    token_keys,
    token_values,
    wq_hbm,
    pool_hbm,
    res_hbm,
    wo_hbm,
    branch_out,
    sorted_out,
    pool_v,
    send_v,
    recv_v,
    sorted_v,
    res_v,
    wq_v,
    wo_v,
    meta_v,
    qpart,
    qrecv,
    ss_send,
    ss_recv,
    onehot,
    onehot_t,
    near_q_send,
    near_q_recv,
    far_q_send,
    far_q_recv,
    own_t,
    own_send,
    own_recv,
    near_acc,
    near_lse,
    far_acc,
    far_lse,
    near_a_send,
    near_a_recv,
    near_l_send,
    near_l_recv,
    far_a_send,
    far_a_recv,
    far_l_send,
    far_l_recv,
    all_lse,
    all_acc,
    load_sem,
    meta_ss,
    meta_rs,
    page_ss,
    page_rs,
    q_ss,
    q_rs,
    s_ss,
    s_rs,
    nq_ss,
    nq_rs,
    fq_ss,
    fq_rs,
    own_ss,
    own_rs,
    na_ss,
    na_rs,
    nl_ss,
    nl_rs,
    fa_ss,
    fa_rs,
    fl_ss,
    fl_rs,
    out_sem,
):
    groups, ranks, cap, kv_here, heads = (dims[name] for name in ("groups", "ranks", "cap", "kv_here", "heads"))
    ratio = heads // kv_here
    hg = heads // ranks
    hgw = hg * HEAD_DIM
    span = HEAD_DIM // ranks
    part = heads * span
    per_tile = HEAD_DIM // span
    rep = HEAD_DIM // heads
    everyone = groups * ranks
    tiles = groups * NPR // 8
    count_tiles = ranks + ranks * tiles
    grp, kv, me, flat = place_in_group(groups, ranks)
    odd_here = lax.rem(grp, 2) == 1
    slots = hidden.shape[0]

    def kv_peer(step):
        return lax.rem(kv + step, ranks)

    def kv_from(step):
        return lax.rem(kv - step + ranks, ranks)

    def all_peer(step):
        return lax.rem(me + step, everyone)

    def all_from(step):
        return lax.rem(me - step + everyone, everyone)

    pending = []

    def remote(src, dst, ss, rs, where):
        copy = pltpu.make_async_remote_copy(
            src_ref=src,
            dst_ref=dst,
            send_sem=ss,
            recv_sem=rs,
            device_id=where,
            device_id_type=pl.DeviceIdType.MESH,
        )
        copy.start()
        pending.append(copy)

    def arrive(src, dst, ss, rs, where):
        pltpu.make_async_remote_copy(
            src_ref=src,
            dst_ref=dst,
            send_sem=ss,
            recv_sem=rs,
            device_id=where,
            device_id_type=pl.DeviceIdType.MESH,
        ).wait_recv()

    loads = []
    for c in range(kv_here):
        cols = pl.ds(c * HEAD_DIM, HEAD_DIM)
        loads.append(
            pltpu.make_async_copy(pool_hbm.at[:, :, :, cols], pool_v[c], load_sem.at[c])
        )
    load_q = pltpu.make_async_copy(wq_hbm, wq_v, load_sem.at[kv_here])
    load_r = pltpu.make_async_copy(res_hbm, res_v, load_sem.at[kv_here + 1])
    load_o = pltpu.make_async_copy(wo_hbm, wo_v, load_sem.at[kv_here + 2])
    loads[0].start()
    load_q.start()
    for copy in loads[1:]:
        copy.start()
    load_r.start()
    load_o.start()

    barrier = pltpu.get_barrier_semaphore()
    for step in range(1, everyone):
        pl.semaphore_signal(
            barrier, inc=1, device_id=flat(all_peer(step)), device_id_type=pl.DeviceIdType.MESH
        )
    pl.semaphore_wait(barrier, everyone - 1)

    for step in range(1, everyone):
        remote(meta, meta_v.at[me], meta_ss.at[step], meta_rs.at[step], flat(all_peer(step)))
    meta_v[me] = meta[...]

    def send_pages(c):
        loads[c].wait()

        def pick(i, carry):
            for a in range(cap):
                where = i * cap + a
                target = lax.rem(kv + i, ranks) * cap + a
                send_v[c][where] = pool_v[c][picked[target]]
            return carry

        for a in range(cap):
            recv_v[c][kv * cap + a] = pool_v[c][picked[kv * cap + a]]
        lax.fori_loop(1, ranks, pick, 0)
        for step in range(1, ranks):
            remote(
                send_v[c].at[pl.ds(step * cap, cap)],
                recv_v[c].at[pl.ds(kv * cap, cap)],
                page_ss.at[c, step],
                page_rs.at[c, step],
                {"kv": kv_peer(step)},
            )

    send_pages(0)

    load_q.wait()
    features = hidden[...].astype(jnp.float32)
    normed = (features * gain[...]).astype(jnp.bfloat16)
    for j in range(ranks):
        qpart[j] = mm(normed, wq_v[:, j * hgw : (j + 1) * hgw])
    squares = jnp.sum(features * features, axis=1, keepdims=True)
    ss_send[...] = jnp.transpose(jnp.broadcast_to(squares, (slots, 128)))[:8]
    ss_recv[kv] = ss_send[...]
    for step in range(1, ranks):
        peer = kv_peer(step)
        remote(ss_send, ss_recv.at[kv], s_ss.at[step], s_rs.at[step], {"kv": peer})
        remote(qpart.at[peer], qrecv.at[kv], q_ss.at[step], q_rs.at[step], {"kv": peer})

    for step in range(1, everyone):
        source = all_from(step)
        arrive(meta, meta_v.at[source], meta_ss.at[step], meta_rs.at[step], flat(source))
    slot_rows = []
    for k in range(ranks):
        slot_rows.append(column_of(meta_v[grp * ranks + k][2:3], 0))
    for k in range(ranks):
        for t in range(tiles):
            slot_rows.append(column_of(meta_v[grp * ranks + k][0:1], 8 * t))
    for i, column in enumerate(slot_rows):
        onehot[8 * i : 8 * i + 8, :] = (
            column == lanes_of((8, slots)).astype(jnp.float32)
        ).astype(jnp.float32)
    for i in range(8 * count_tiles, onehot.shape[0], 8):
        onehot[i : i + 8, :] = jnp.zeros((8, slots), jnp.float32)

    send_pages(1)

    for step in range(1, ranks):
        source = kv_from(step)
        arrive(ss_send, ss_recv.at[source], s_ss.at[step], s_rs.at[step], {"kv": source})
        arrive(
            qpart.at[source], qrecv.at[source], q_ss.at[step], q_rs.at[step], {"kv": source}
        )
    total_ss = ss_recv[0]
    for j in range(1, ranks):
        total_ss = total_ss + ss_recv[j]
    total_ss = jnp.transpose(jnp.broadcast_to(total_ss[0:1], (128, slots)))
    scale = lax.rsqrt(total_ss / D + norm_eps) * HEAD_DIM ** (-0.5)
    pieces = []
    for i in range(hg):
        cols = slice(i * HEAD_DIM, (i + 1) * HEAD_DIM)
        piece = qpart[kv, :, cols]
        for step in range(1, ranks):
            piece = piece + qrecv[kv_from(step), :, cols]
        pieces.append(piece * scale)
    kv_head = (kv * hg) // ratio
    own_key = token_keys[:, pl.ds(pl.multiple_of(kv_head * HEAD_DIM, HEAD_DIM), HEAD_DIM)]
    own_key = own_key.astype(jnp.float32)
    lane_head = lanes_of((slots, 128)) // rep
    own = jnp.zeros((slots, 128), jnp.float32)
    for i in range(hg):
        score = jnp.sum(pieces[i] * own_key, axis=1, keepdims=True)
        own = jnp.where(lane_head == kv * hg + i, score, own)
    own_t[...] = jnp.transpose(own)
    own_send[...] = own_t[pl.ds(pl.multiple_of(kv * (hg * rep), 8), hg * rep), :]
    own_recv[kv] = own_send[...]
    hot = onehot[...].astype(jnp.bfloat16)
    chosen = []
    for piece in pieces:
        high, middle, low = split3(piece)
        chosen.append(mm(hot, high) + mm(hot, middle) + mm(hot, low))
    chosen = jnp.concatenate(chosen, axis=1)
    for k in range(ranks):
        near_q_send[k] = chosen[8 * k : 8 * k + 8]
        for t in range(tiles):
            at = 8 * (ranks + k * tiles + t)
            tile = chosen[at : at + 8]
            far_q_send[(2 * t) * ranks + k] = fold(tile, False)
            far_q_send[(2 * t + 1) * ranks + k] = fold(tile, True)
    near_q_recv[kv] = near_q_send[kv]
    far_q_recv[me] = far_q_send[me]
    for step in range(1, ranks):
        peer = kv_peer(step)
        remote(
            near_q_send.at[peer], near_q_recv.at[kv], nq_ss.at[step], nq_rs.at[step], {"kv": peer}
        )
        remote(own_send, own_recv.at[kv], own_ss.at[step], own_rs.at[step], {"kv": peer})
    for step in range(1, everyone):
        peer = all_peer(step)
        remote(
            far_q_send.at[peer], far_q_recv.at[me], fq_ss.at[step], fq_rs.at[step], flat(peer)
        )

    for c in range(2, kv_here):
        send_pages(c)

    row_id = rows_of((8, 128))
    row_masks = [
        jnp.concatenate([(row_id == p).astype(jnp.bfloat16)] * ratio, axis=0) for p in range(8)
    ]

    def page_tile(queries, keys, values, lengths):
        q_high, q_middle, q_low = split3(jnp.concatenate(queries, axis=0))
        rows = 8 * ratio
        scores = jnp.zeros((3 * rows, HEAD_DIM), jnp.float32)
        for p in range(8):
            mask = row_masks[p]
            stacked = jnp.concatenate([q_high * mask, q_middle * mask, q_low * mask], axis=0)
            scores = scores + mm_nt(stacked, keys(p))
        scores = scores[:rows] + scores[rows : 2 * rows] + scores[2 * rows :]
        usable = lanes_of((rows, 128)).astype(jnp.float32) < jnp.concatenate(
            [lengths] * ratio, axis=0
        )
        scores = jnp.where(usable, scores, neg_fill)
        top = jnp.max(scores, axis=1, keepdims=True)
        weights = jnp.where(usable, jnp.exp(scores - top), 0.0)
        total = jnp.sum(weights, axis=1, keepdims=True)
        w_high, w_low = split2(weights)
        acc = jnp.zeros((2 * rows, HEAD_DIM), jnp.float32)
        for p in range(8):
            mask = row_masks[p]
            stacked = jnp.concatenate([w_high * mask, w_low * mask], axis=0)
            acc = acc + mm(stacked, values(p))
        acc = (acc[:rows] + acc[rows:]) / total
        return acc, top + jnp.log(total)

    lane_id = lanes_of((8, 128))

    def pack_acc(load, k):
        columns = []
        for first in range(0, heads, per_tile):
            merged = None
            for i in range(per_tile):
                turn = (span * (i - k)) % HEAD_DIM
                moved = load(first + i)
                if turn:
                    moved = pltpu.roll(moved, turn, 1)
                merged = moved if merged is None else jnp.where(lane_id // span == i, moved, merged)
            columns.append(merged)
        return columns[0] if len(columns) == 1 else jnp.concatenate(columns, axis=1)

    for step in range(1, ranks):
        source = kv_from(step)
        arrive(
            near_q_send.at[source],
            near_q_recv.at[source],
            nq_ss.at[step],
            nq_rs.at[step],
            {"kv": source},
        )
    load_r.wait()
    near_length = column_of(meta[3:4], 0)
    lse_tile = jnp.zeros((8, 128), jnp.float32)
    for j in range(kv_here):
        queries = []
        for i in range(ratio):
            head = j * ratio + i
            at = (head % hg) * HEAD_DIM
            queries.append(near_q_recv[head // hg, :, at : at + HEAD_DIM])
        cols = slice(j * HEAD_DIM, (j + 1) * HEAD_DIM)
        acc, lse = page_tile(
            queries,
            lambda p: res_v[p, 0, :, cols],
            lambda p: res_v[p, 1, :, cols],
            near_length,
        )
        for i in range(ratio):
            head = j * ratio + i
            near_acc[head] = acc[8 * i : 8 * i + 8]
            lse_tile = jnp.where(lane_id // rep == head, lse[8 * i : 8 * i + 8], lse_tile)
    near_l_send[...] = lse_tile
    near_l_recv[kv] = lse_tile
    for k in range(ranks):
        near_a_send[k] = pack_acc(lambda head: near_acc[head], k)
    near_a_recv[kv] = near_a_send[kv]
    for step in range(1, ranks):
        peer = kv_peer(step)
        remote(near_l_send, near_l_recv.at[kv], nl_ss.at[step], nl_rs.at[step], {"kv": peer})
        remote(
            near_a_send.at[peer], near_a_recv.at[kv], na_ss.at[step], na_rs.at[step], {"kv": peer}
        )

    for step in range(1, everyone):
        source = all_from(step)
        arrive(
            far_q_send.at[source],
            far_q_recv.at[source],
            fq_ss.at[step],
            fq_rs.at[step],
            flat(source),
        )
    far_lengths = []
    for t in range(tiles):
        offset = grp * NPR
        first = column_of(meta_v[(2 * t) * ranks + kv][1:2], offset)
        second = column_of(meta_v[(2 * t + 1) * ranks + kv][1:2], offset - 4)
        far_lengths.append(jnp.where(rows_of((8, 1)) < 4, first, second))
    far_lse_tiles = [jnp.zeros((8, 128), jnp.float32) for _ in range(tiles)]
    stores = []
    for c in range(kv_here):
        for step in range(1, ranks):
            source = kv_from(step)
            arrive(
                send_v[c].at[pl.ds(step * cap, cap)],
                recv_v[c].at[pl.ds(source * cap, cap)],
                page_ss.at[c, step],
                page_rs.at[c, step],
                {"kv": source},
            )

        def sort(i, carry):
            sorted_v[c][i] = recv_v[c][inverse[i]]
            return carry

        lax.fori_loop(0, groups * NPR, sort, 0)
        cols = pl.ds(c * HEAD_DIM, HEAD_DIM)
        store = pltpu.make_async_copy(
            sorted_v[c], sorted_out.at[:, :, :, cols], out_sem.at[c]
        )
        store.start()
        stores.append(store)
        for t in range(tiles):
            queries = []
            for i in range(ratio):
                head = c * ratio + i
                k = head // hg
                wide = unfold(
                    far_q_recv[(2 * t) * ranks + k],
                    far_q_recv[(2 * t + 1) * ranks + k],
                    hgw,
                    odd_here,
                )
                at = (head % hg) * HEAD_DIM
                queries.append(wide[:, at : at + HEAD_DIM])
            acc, lse = page_tile(
                queries,
                lambda p: sorted_v[c][8 * t + p, 0],
                lambda p: sorted_v[c][8 * t + p, 1],
                far_lengths[t],
            )
            for i in range(ratio):
                head = c * ratio + i
                far_acc[t, head] = acc[8 * i : 8 * i + 8]
                far_lse_tiles[t] = jnp.where(
                    lane_id // rep == head, lse[8 * i : 8 * i + 8], far_lse_tiles[t]
                )
    for t in range(tiles):
        for k in range(ranks):
            tile = pack_acc(lambda head: far_acc[t, head], k)
            far_a_send[(2 * t) * ranks + k] = fold(tile, False)
            far_a_send[(2 * t + 1) * ranks + k] = fold(tile, True)
        far_l_send[t] = far_lse_tiles[t]
    far_a_recv[me] = far_a_send[me]
    far_l_recv[me] = far_l_send[grp // 2]
    for step in range(1, everyone):
        peer = all_peer(step)
        remote(
            far_l_send.at[peer // (2 * ranks)],
            far_l_recv.at[me],
            fl_ss.at[step],
            fl_rs.at[step],
            flat(peer),
        )
        remote(
            far_a_send.at[peer], far_a_recv.at[me], fa_ss.at[step], fa_rs.at[step], flat(peer)
        )

    onehot_t[...] = jnp.transpose(onehot[...]).astype(jnp.bfloat16)
    lane = lanes_of((1, part))
    wanted = (lane // (span * ratio)) * HEAD_DIM + kv * span + lax.rem(lane, span)
    choose = (rows_of((kv_here * HEAD_DIM, part)) == wanted).astype(jnp.bfloat16)
    own_piece = mm(token_values[...], choose)
    widen = (
        rows_of((128, part)) == (lanes_of((128, part)) // span) * rep
    ).astype(jnp.bfloat16)
    for step in range(1, ranks):
        source = kv_from(step)
        arrive(own_send, own_recv.at[source], own_ss.at[step], own_rs.at[step], {"kv": source})
        arrive(
            near_l_send, near_l_recv.at[source], nl_ss.at[step], nl_rs.at[step], {"kv": source}
        )
        arrive(
            near_a_send.at[source],
            near_a_recv.at[source],
            na_ss.at[step],
            na_rs.at[step],
            {"kv": source},
        )
    own_all = jnp.transpose(own_recv[...].reshape(128, slots))
    for k in range(ranks):
        all_lse[8 * k : 8 * k + 8, :] = near_l_recv[k]
        all_acc[8 * k : 8 * k + 8, :] = near_a_recv[k]
    for step in range(1, everyone):
        source = all_from(step)
        arrive(
            far_l_send.at[0],
            far_l_recv.at[source],
            fl_ss.at[step],
            fl_rs.at[step],
            flat(source),
        )
        arrive(
            far_a_send.at[source],
            far_a_recv.at[source],
            fa_ss.at[step],
            fa_rs.at[step],
            flat(source),
        )
    for k in range(ranks):
        for t in range(tiles):
            at = 8 * (ranks + k * tiles + t)
            one, two = (2 * t) * ranks + k, (2 * t + 1) * ranks + k
            all_lse[at : at + 8, :] = pick_rows(far_l_recv[one], far_l_recv[two], odd_here)
            all_acc[at : at + 8, :] = unfold(far_a_recv[one], far_a_recv[two], part, odd_here)
    used = 8 * count_tiles
    for at in range(used, all_lse.shape[0], 8):
        all_lse[at : at + 8, :] = jnp.zeros((8, 128), jnp.float32)
        all_acc[at : at + 8, :] = jnp.zeros((8, part), jnp.float32)
    top = jnp.full((slots, 128), neg_fill, jnp.float32)
    slot_id = rows_of((slots, 128)).astype(jnp.float32)
    diagonal = lax.rem(lane_id, rep)
    turns = [(row_id == diagonal + rep * h).astype(jnp.float32) for h in range(8 // rep if rep < 8 else 1)]
    for i, column in enumerate(slot_rows):
        tile = all_lse[8 * i : 8 * i + 8, :]
        for hit in turns:
            value = jnp.sum(tile * hit, axis=0, keepdims=True)
            owner = jnp.sum(column * hit, axis=0, keepdims=True)
            top = jnp.maximum(top, jnp.where(slot_id == owner, value, neg_fill))
    wide_lane = lanes_of((slots, 128))
    shift = 1
    while shift < rep:
        up = pltpu.roll(top, shift, 1)
        down = pltpu.roll(top, 128 - shift, 1)
        top = jnp.maximum(top, jnp.where((wide_lane & shift) != 0, up, down))
        shift *= 2
    top = jnp.maximum(top, own_all)
    high, middle, low = split3(top)
    page_top = mm(hot, high) + mm(hot, middle) + mm(hot, low)
    page_weight = jnp.exp(all_lse[...] - page_top)
    own_weight = jnp.exp(own_all - top)
    hot_t = onehot_t[...]
    high, low = split2(page_weight)
    total = mm(hot_t, high) + mm(hot_t, low) + own_weight
    high, low = split2(
        jnp.concatenate([page_weight, own_weight, pl.reciprocal(total)], axis=0)
    )
    spread = mm(high, widen) + mm(low, widen)
    padded = all_lse.shape[0]
    high, low = split2(all_acc[...] * spread[:padded])
    gathered = mm(hot_t, high) + mm(hot_t, low)
    gathered = gathered + own_piece * spread[padded : padded + slots]
    piece = (gathered * spread[padded + slots :]).astype(jnp.bfloat16)
    load_o.wait()
    columns = branch_out.shape[1]
    for at in range(0, columns, 512):
        branch_out[:, at : at + 512] = mm(piece, wo_v[:, at : at + 512])
    for store in stores:
        store.wait()
    for copy in pending:
        copy.wait_send()


def front(dims, picked, inverse, meta, hidden, gain, token_keys, token_values, wq, pool, res, wo):
    groups, ranks, cap, kv_here, heads = (dims[name] for name in ("groups", "ranks", "cap", "kv_here", "heads"))
    hgw = heads // ranks * HEAD_DIM
    part = heads * HEAD_DIM // ranks
    everyone = groups * ranks
    pages = groups * NPR
    tiles = pages // 8
    slots = hidden.shape[0]
    rep = HEAD_DIM // heads
    tokens = pool.shape[2]
    rows = 8 * (ranks + ranks * tiles)
    rows = -(-rows // 128) * 128
    half = lambda width: width // 2 if width >= 256 else width
    f32, bf16 = jnp.float32, jnp.bfloat16
    chunk = lambda count: [pltpu.VMEM((count, 2, tokens, HEAD_DIM), bf16) for _ in range(kv_here)]
    dma = lambda *shape: pltpu.SemaphoreType.DMA(shape)
    scratch = [
        chunk(pool.shape[0]),
        chunk(pages),
        chunk(pages),
        chunk(pages),
        pltpu.VMEM(res.shape, bf16),
        pltpu.VMEM(wq.shape, bf16),
        pltpu.VMEM(wo.shape, bf16),
        pltpu.VMEM((everyone, 8, 128), jnp.int32),
        pltpu.VMEM((ranks, slots, hgw), f32),
        pltpu.VMEM((ranks, slots, hgw), f32),
        pltpu.VMEM((8, slots), f32),
        pltpu.VMEM((ranks, 8, slots), f32),
        pltpu.VMEM((rows, slots), f32),
        pltpu.VMEM((slots, rows), bf16),
        pltpu.VMEM((ranks, 8, hgw), f32),
        pltpu.VMEM((ranks, 8, hgw), f32),
        pltpu.VMEM((everyone, 8, half(hgw)), f32),
        pltpu.VMEM((everyone, 8, half(hgw)), f32),
        pltpu.VMEM((128, slots), f32),
        pltpu.VMEM((heads // ranks * rep, slots), f32),
        pltpu.VMEM((ranks, heads // ranks * rep, slots), f32),
        pltpu.VMEM((heads, 8, HEAD_DIM), f32),
        pltpu.VMEM((8, 128), f32),
        pltpu.VMEM((tiles, heads, 8, HEAD_DIM), f32),
        pltpu.VMEM((tiles, 8, 128), f32),
        pltpu.VMEM((ranks, 8, part), f32),
        pltpu.VMEM((ranks, 8, part), f32),
        pltpu.VMEM((8, 128), f32),
        pltpu.VMEM((ranks, 8, 128), f32),
        pltpu.VMEM((everyone, 8, half(part)), f32),
        pltpu.VMEM((everyone, 8, half(part)), f32),
        pltpu.VMEM((tiles, 8, 128), f32),
        pltpu.VMEM((everyone, 8, 128), f32),
        pltpu.VMEM((rows, 128), f32),
        pltpu.VMEM((rows, part), f32),
        dma(kv_here + 3),
        dma(everyone),
        dma(everyone),
        dma(kv_here, ranks),
        dma(kv_here, ranks),
        dma(ranks),
        dma(ranks),
        dma(ranks),
        dma(ranks),
        dma(ranks),
        dma(ranks),
        dma(everyone),
        dma(everyone),
        dma(ranks),
        dma(ranks),
        dma(ranks),
        dma(ranks),
        dma(ranks),
        dma(ranks),
        dma(everyone),
        dma(everyone),
        dma(everyone),
        dma(everyone),
        dma(kv_here),
    ]
    vmem = pl.BlockSpec(memory_space=pltpu.VMEM)
    smem = pl.BlockSpec(memory_space=pltpu.SMEM)
    hbm = pl.BlockSpec(memory_space=pl.ANY)
    return pl.pallas_call(
        functools.partial(front_kernel, dims),
        out_shape=(
            jax.ShapeDtypeStruct((slots, wo.shape[1]), f32),
            jax.ShapeDtypeStruct((pages,) + pool.shape[1:], bf16),
        ),
        in_specs=[smem, smem, vmem, vmem, vmem, vmem, vmem, hbm, hbm, hbm, hbm],
        out_specs=(vmem, hbm),
        scratch_shapes=scratch,
        compiler_params=pltpu.CompilerParams(
            collective_id=1, has_side_effects=True, vmem_limit_bytes=60 << 20
        ),
        name="front",
    )(picked, inverse, meta, hidden, gain, token_keys, token_values, wq, pool, res, wo)


def route_tables(new_owner, new_local):
    groups = lax.axis_size("grp")
    ranks = lax.axis_size("kv")
    per_dev = new_owner.shape[1] // ranks
    cap = groups * NPR // ranks
    grp_rank = lax.axis_index("grp")
    kv_rank = lax.axis_index("kv")
    myself = grp_rank * ranks + kv_rank
    places = jnp.arange(cap, dtype=jnp.int32)
    by_col = (
        new_owner.reshape(groups, ranks, per_dev)
        .transpose(1, 0, 2)
        .reshape(ranks, groups * per_dev)
    )
    local_col = (
        new_local.reshape(groups, ranks, per_dev)
        .transpose(1, 0, 2)
        .reshape(ranks, groups * per_dev)
    )
    select = nth_match(by_col, myself, places)
    picked = jnp.sum(jnp.where(select, local_col[:, None, :], 0), axis=2)
    row_here = lax.dynamic_index_in_dim(by_col, kv_rank, 0, keepdims=False)
    sources = grp_rank * ranks + jnp.arange(ranks, dtype=jnp.int32)
    hits = nth_match(
        jnp.broadcast_to(row_here[None, :], (ranks, row_here.shape[0])), sources[:, None], places
    )
    spots = jnp.arange(row_here.shape[0], dtype=jnp.int32)
    where_f = jnp.sum(jnp.where(hits, spots[None, None, :], 0), axis=2).reshape(-1)
    dest_grp = where_f // per_dev
    dest_pos = where_f % per_dev
    same = (dest_grp[:, None] == dest_grp[None, :]) & (dest_pos[:, None] < dest_pos[None, :])
    rank_in = jnp.sum(same.astype(jnp.int32), axis=0)
    target = dest_grp * NPR + rank_in
    items = jnp.arange(target.shape[0], dtype=jnp.int32)
    inverse = jnp.sum(jnp.where(target[None, :] == items[:, None], items[None, :], 0), axis=1)
    return picked.reshape(-1), inverse


def per_device(
    hidden_states,
    attn_gain,
    mlp_gain,
    w_query,
    w_out,
    w_gate,
    w_up,
    w_down,
    kv_pool,
    resident_cache,
    resident_slot,
    resident_len,
    new_owner,
    new_local,
    new_slot,
    new_len,
    token_kv,
):
    groups = lax.axis_size("grp")
    ranks = lax.axis_size("kv")
    pairs = lax.axis_size("tp")
    kv_rank = lax.axis_index("kv")
    tp_rank = lax.axis_index("tp")
    features = hidden_states.astype(jnp.float32)
    slots = features.shape[0]
    heads_here = w_query.shape[1] // HEAD_DIM
    kv_here = token_kv.shape[2] // HEAD_DIM
    dims = {
        "groups": groups,
        "ranks": ranks,
        "cap": groups * NPR // ranks,
        "kv_here": kv_here,
        "heads": heads_here,
    }
    arrived_at = arrival_places(new_owner)
    picked, inverse = route_tables(new_owner, new_local)
    items = jnp.arange(arrived_at.shape[0], dtype=jnp.int32)
    hit = arrived_at[None, :] == items[:, None]
    slot_by = jnp.sum(jnp.where(hit, new_slot, 0), axis=1)
    len_by = jnp.sum(jnp.where(hit, new_len, 0), axis=1)
    meta = jnp.stack(
        [
            lanes(values[None], 128)[0]
            for values in (slot_by, len_by, resident_slot[0], resident_len[0])
        ]
    )
    meta = jnp.pad(meta, ((0, 4), (0, 0)))
    branch, sorted_pages = front(
        dims,
        picked,
        inverse,
        meta,
        hidden_states,
        attn_gain[None],
        token_kv[:, 0],
        token_kv[:, 1],
        w_query,
        kv_pool,
        resident_cache[0],
        w_out.reshape(-1, w_out.shape[2]),
    )
    arrived = lax.all_to_all(sorted_pages, "grp", split_axis=0, concat_axis=0, tiled=True)
    width_here = features.shape[1]
    column = jnp.arange(ranks * width_here, dtype=jnp.int32)
    mine = (column // width_here == kv_rank) & (tp_rank == 0)
    branch = branch + jnp.where(mine[None, :], jnp.tile(features, (1, ranks)), 0.0)
    row_count = slots // (ranks * pairs)
    blocks = (ranks * pairs, row_count, ranks * width_here)
    laid = push(branch.astype(jnp.bfloat16).reshape(blocks), ("kv", "tp"), 6)
    kept = jnp.sum(laid.astype(jnp.float32), axis=0).astype(jnp.bfloat16)
    resid = push(kept, ("kv", "tp"), 7, True).reshape(slots, ranks * width_here)
    resid_f = resid.astype(jnp.float32)
    mlp_scale = lax.rsqrt(jnp.sum(resid_f * resid_f, axis=1) / D + norm_eps)
    normed_mlp = (resid_f * mlp_gain).astype(jnp.bfloat16)
    gate = jnp.dot(normed_mlp, w_gate, preferred_element_type=jnp.float32) * mlp_scale[:, None]
    upward = jnp.dot(normed_mlp, w_up, preferred_element_type=jnp.float32) * mlp_scale[:, None]
    hidden_units = (jax.nn.silu(gate) * upward).astype(jnp.bfloat16)
    down = jnp.dot(hidden_units, w_down, preferred_element_type=jnp.float32)
    down = push(down.astype(jnp.bfloat16).reshape(blocks), ("kv", "tp"), 8)
    down = jnp.sum(down.astype(jnp.float32), axis=0)
    mixed = (kept.astype(jnp.float32) + down).astype(jnp.bfloat16)
    new_pages = jnp.take(arrived, arrived_at, axis=0, mode="clip")
    return (mixed, new_pages[None])


def solution(mesh):
    return jax.shard_map(
        per_device,
        mesh=mesh,
        in_specs=(
            P("grp", "kv"),
            P("kv"),
            P(),
            P("kv", "tp"),
            P("tp", "kv", None),
            P(None, ("kv", "tp")),
            P(None, ("kv", "tp")),
            P(("kv", "tp"), None),
            P(("grp", "kv"), None, None, "tp"),
            P("grp", "kv", None, None, "tp"),
            P("grp", "kv"),
            P("grp", "kv"),
            P(),
            P(),
            P("grp", "kv"),
            P("grp", "kv"),
            P("grp", None, "tp"),
        ),
        out_specs=(P(("grp", "kv", "tp"), None), P("grp", "kv", None, None, "tp")),
        check_vma=False,
    )
```

```python
import functools

import jax
import jax.numpy as jnp
from jax import lax
from jax.experimental import pallas as pl
from jax.experimental.pallas import tpu as pltpu
from jax.sharding import PartitionSpec as P

D = 4096
HEADS = 32
KV_HEADS = 8
HEAD_DIM = 128
NPR = 4


neg_fill = -1e30
norm_eps = 1e-05


def nth_match(table, wanted, places):
    matched = (table == wanted).astype(jnp.int32)
    ranking = jnp.cumsum(matched, axis=1) - 1
    return (matched[:, None, :] == 1) & (ranking[:, None, :] == places[None, :, None])


def arrival_places(new_owner):
    groups = lax.axis_size("grp")
    ranks = lax.axis_size("kv")
    per_dev = new_owner.shape[1] // ranks
    owners = new_owner.reshape(groups * ranks, per_dev)
    myself = lax.axis_index("grp") * ranks + lax.axis_index("kv")
    mine = lax.dynamic_index_in_dim(owners, myself, 0, keepdims=False)
    order = jnp.arange(per_dev, dtype=jnp.int32)
    src_grp = mine // ranks
    earlier = (src_grp[:, None] == src_grp[None, :]) & (order[:, None] < order[None, :])
    before = jnp.sum(earlier.astype(jnp.int32), axis=0)
    return src_grp * NPR + before


def lanes(values, width):
    return jnp.pad(values, [(0, 0)] * (values.ndim - 1) + [(0, width - values.shape[-1])])


RING = 4
DOWN_RING = 4


def split2(x):
    high = x.astype(jnp.bfloat16)
    return high, (x - high.astype(jnp.float32)).astype(jnp.bfloat16)


def split3(x):
    high = x.astype(jnp.bfloat16)
    rest = x - high.astype(jnp.float32)
    middle = rest.astype(jnp.bfloat16)
    return high, middle, (rest - middle.astype(jnp.float32)).astype(jnp.bfloat16)


def mm(a, b):
    return jnp.dot(a, b, preferred_element_type=jnp.float32)


def mm_nt(a, b):
    return lax.dot_general(a, b, (((1,), (1,)), ((), ())), preferred_element_type=jnp.float32)


def rows_of(shape):
    return lax.broadcasted_iota(jnp.int32, shape, 0)


def lanes_of(shape):
    return lax.broadcasted_iota(jnp.int32, shape, 1)


def half_turn(x):
    return pltpu.roll(x, 4, 0)


def fold(tile, odd):
    if tile.shape[1] < 256:
        return tile
    half = tile.shape[1] // 2
    low, high = tile[:, :half], tile[:, half:]
    top = rows_of(low.shape) < 4
    if odd:
        return jnp.where(top, half_turn(low), high)
    return jnp.where(top, low, half_turn(high))


def pick_rows(first, second, odd):
    first = jnp.where(odd, half_turn(first), first)
    second = jnp.where(odd, second, half_turn(second))
    return jnp.where(rows_of(first.shape) < 4, first, second)


def unfold(first, second, width, odd):
    if width < 256:
        return pick_rows(first, second, odd)
    top = rows_of(first.shape) < 4
    low = jnp.where(top, first, half_turn(second))
    high = jnp.where(top, half_turn(first), second)
    return jnp.concatenate([low, high], axis=1)


def column_of(row, offset):
    wide = jnp.broadcast_to(row, (8, 128)).astype(jnp.float32)
    hit = lanes_of((8, 128)) == rows_of((8, 128)) + offset
    return jnp.sum(jnp.where(hit, wide, 0.0), axis=1, keepdims=True)


def place_in_group(groups, ranks):
    grp = lax.axis_index("grp")
    kv = lax.axis_index("kv")
    me = grp * ranks + kv

    def flat(index):
        return {"grp": index // ranks, "kv": lax.rem(index, ranks)}

    return grp, kv, me, flat


def step_kernel(
    dims,
    picked,
    inverse,
    meta,
    hidden,
    gain,
    token_keys,
    token_values,
    wq_hbm,
    pool_hbm,
    res_hbm,
    wo_hbm,
    mlp_gain,
    wg_hbm,
    wu_hbm,
    wd_hbm,
    mixed_out,
    arrived_out,
    pool_v,
    send_v,
    recv_v,
    sorted_v,
    res_v,
    wq_v,
    wo_v,
    meta_v,
    qpart,
    qrecv,
    ss_send,
    ss_recv,
    onehot,
    onehot_t,
    near_q_send,
    near_q_recv,
    far_q_send,
    far_q_recv,
    own_t,
    own_send,
    own_recv,
    near_acc,
    near_lse,
    far_acc,
    far_lse,
    near_a_send,
    near_a_recv,
    near_l_send,
    near_l_recv,
    far_a_send,
    far_a_recv,
    far_l_send,
    far_l_recv,
    all_lse,
    all_acc,
    piece_v,
    keep_v,
    r1_send,
    r1_recv,
    r2_send,
    r2_recv,
    d1_send,
    d1_recv,
    d2_send,
    d2_recv,
    kept_v,
    resid_v,
    normed_v,
    units_v,
    wg_v,
    wu_v,
    wd_v,
    load_sem,
    gate_sem,
    down_sem,
    meta_ss,
    meta_rs,
    page_ss,
    page_rs,
    q_ss,
    q_rs,
    s_ss,
    s_rs,
    nq_ss,
    nq_rs,
    fq_ss,
    fq_rs,
    own_ss,
    own_rs,
    na_ss,
    na_rs,
    nl_ss,
    nl_rs,
    fa_ss,
    fa_rs,
    fl_ss,
    fl_rs,
    z_ss,
    z_rs,
    z_own,
    r1_ss,
    r1_rs,
    r2_ss,
    r2_rs,
    d1_ss,
    d1_rs,
    d2_ss,
    d2_rs,
    g_ss,
    g_rs,
    gp_ss,
    gp_rs,
):
    groups, ranks, cap, kv_here, heads = (dims[name] for name in ("groups", "ranks", "cap", "kv_here", "heads"))
    ratio = heads // kv_here
    hg = heads // ranks
    hgw = hg * HEAD_DIM
    span = HEAD_DIM // ranks
    part = heads * span
    per_tile = HEAD_DIM // span
    rep = HEAD_DIM // heads
    everyone = groups * ranks
    tiles = groups * NPR // 8
    count_tiles = ranks + ranks * tiles
    grp, kv, me, flat = place_in_group(groups, ranks)
    tp = lax.axis_index("tp")
    partner = {"tp": 1 - tp}
    odd_here = lax.rem(grp, 2) == 1
    slots = hidden.shape[0]

    def kv_peer(step):
        return lax.rem(kv + step, ranks)

    def kv_from(step):
        return lax.rem(kv - step + ranks, ranks)

    def all_peer(step):
        return lax.rem(me + step, everyone)

    def all_from(step):
        return lax.rem(me - step + everyone, everyone)

    pending = []

    def remote(src, dst, ss, rs, where):
        copy = pltpu.make_async_remote_copy(
            src_ref=src,
            dst_ref=dst,
            send_sem=ss,
            recv_sem=rs,
            device_id=where,
            device_id_type=pl.DeviceIdType.MESH,
        )
        copy.start()
        pending.append(copy)

    def arrive(src, dst, ss, rs, where):
        pltpu.make_async_remote_copy(
            src_ref=src,
            dst_ref=dst,
            send_sem=ss,
            recv_sem=rs,
            device_id=where,
            device_id_type=pl.DeviceIdType.MESH,
        ).wait_recv()

    loads = []
    for c in range(kv_here):
        cols = pl.ds(c * HEAD_DIM, HEAD_DIM)
        loads.append(
            pltpu.make_async_copy(pool_hbm.at[:, :, :, cols], pool_v[c], load_sem.at[c])
        )
    load_q = pltpu.make_async_copy(wq_hbm, wq_v, load_sem.at[kv_here])
    load_r = pltpu.make_async_copy(res_hbm, res_v, load_sem.at[kv_here + 1])
    load_o = pltpu.make_async_copy(wo_hbm, wo_v, load_sem.at[kv_here + 2])
    loads[0].start()
    load_q.start()
    for copy in loads[1:]:
        copy.start()
    load_r.start()
    load_o.start()

    barrier = pltpu.get_barrier_semaphore()
    for step in range(1, everyone):
        pl.semaphore_signal(
            barrier, inc=1, device_id=flat(all_peer(step)), device_id_type=pl.DeviceIdType.MESH
        )
    pl.semaphore_signal(
        barrier, inc=1, device_id=partner, device_id_type=pl.DeviceIdType.MESH
    )
    pl.semaphore_wait(barrier, everyone)

    for step in range(1, everyone):
        remote(meta, meta_v.at[me], meta_ss.at[step], meta_rs.at[step], flat(all_peer(step)))
    meta_v[me] = meta[...]

    def send_pages(c):
        loads[c].wait()

        def pick(i, carry):
            for a in range(cap):
                where = i * cap + a
                target = lax.rem(kv + i, ranks) * cap + a
                send_v[c][where] = pool_v[c][picked[target]]
            return carry

        for a in range(cap):
            recv_v[c][kv * cap + a] = pool_v[c][picked[kv * cap + a]]
        lax.fori_loop(1, ranks, pick, 0)
        for step in range(1, ranks):
            remote(
                send_v[c].at[pl.ds(step * cap, cap)],
                recv_v[c].at[pl.ds(kv * cap, cap)],
                page_ss.at[c, step],
                page_rs.at[c, step],
                {"kv": kv_peer(step)},
            )

    def sort_pages(c):
        for step in range(1, ranks):
            source = kv_from(step)
            arrive(
                send_v[c].at[pl.ds(step * cap, cap)],
                recv_v[c].at[pl.ds(source * cap, cap)],
                page_ss.at[c, step],
                page_rs.at[c, step],
                {"kv": source},
            )

        def sort(i, carry):
            sorted_v[c][i] = recv_v[c][inverse[i]]
            return carry

        lax.fori_loop(0, groups * NPR, sort, 0)

    def pages_of(group):
        return pl.ds(pl.multiple_of(group * NPR, NPR), NPR)

    def grp_peer(step):
        return lax.rem(grp + step, groups)

    def grp_from(step):
        return lax.rem(grp - step + groups, groups)

    stores = []

    def forward_pages(c, kind):
        cols = pl.ds(c * HEAD_DIM, HEAD_DIM)
        for step in range(1, groups):
            peer = grp_peer(step)
            remote(
                sorted_v[c].at[pages_of(peer), kind],
                arrived_out.at[pages_of(grp), kind, :, cols],
                z_ss.at[c, kind, step],
                z_rs.at[c, kind, step],
                {"grp": peer},
            )
        store = pltpu.make_async_copy(
            sorted_v[c].at[pages_of(grp), kind],
            arrived_out.at[pages_of(grp), kind, :, cols],
            z_own.at[c, kind],
        )
        store.start()
        stores.append(store)

    send_pages(0)

    load_q.wait()
    features = hidden[...].astype(jnp.float32)
    normed = (features * gain[...]).astype(jnp.bfloat16)
    for j in range(ranks):
        qpart[j] = mm(normed, wq_v[:, j * hgw : (j + 1) * hgw])
    tile_n = wg_v.shape[2]
    gate_tiles = wg_hbm.shape[1] // tile_n
    ring = wg_v.shape[0]
    cw = wd_v.shape[2]
    chunks = wd_hbm.shape[1] // cw
    down_ring = wd_v.shape[0]

    def gate_loads(n):
        cols = pl.ds(n * tile_n, tile_n)
        slot = n % ring
        return (
            pltpu.make_async_copy(wg_hbm.at[:, cols], wg_v.at[slot], gate_sem.at[0, slot]),
            pltpu.make_async_copy(wu_hbm.at[:, cols], wu_v.at[slot], gate_sem.at[1, slot]),
        )

    def down_load(c):
        slot = c % down_ring
        return pltpu.make_async_copy(
            wd_hbm.at[:, pl.ds(c * cw, cw)], wd_v.at[slot], down_sem.at[slot]
        )

    for n in range(min(ring, gate_tiles)):
        for copy in gate_loads(n):
            copy.start()
    for c in range(min(down_ring, chunks)):
        down_load(c).start()
    squares = jnp.sum(features * features, axis=1, keepdims=True)
    ss_send[...] = jnp.transpose(jnp.broadcast_to(squares, (slots, 128)))[:8]
    ss_recv[kv] = ss_send[...]
    for step in range(1, ranks):
        peer = kv_peer(step)
        remote(ss_send, ss_recv.at[kv], s_ss.at[step], s_rs.at[step], {"kv": peer})
        remote(qpart.at[peer], qrecv.at[kv], q_ss.at[step], q_rs.at[step], {"kv": peer})

    for step in range(1, everyone):
        source = all_from(step)
        arrive(meta, meta_v.at[source], meta_ss.at[step], meta_rs.at[step], flat(source))
    slot_rows = []
    for k in range(ranks):
        slot_rows.append(column_of(meta_v[grp * ranks + k][2:3], 0))
    for k in range(ranks):
        for t in range(tiles):
            slot_rows.append(column_of(meta_v[grp * ranks + k][0:1], 8 * t))
    for i, column in enumerate(slot_rows):
        onehot[8 * i : 8 * i + 8, :] = (
            column == lanes_of((8, slots)).astype(jnp.float32)
        ).astype(jnp.float32)
    for i in range(8 * count_tiles, onehot.shape[0], 8):
        onehot[i : i + 8, :] = jnp.zeros((8, slots), jnp.float32)

    send_pages(1)
    sort_pages(0)
    forward_pages(0, 0)
    forward_pages(0, 1)

    for step in range(1, ranks):
        source = kv_from(step)
        arrive(ss_send, ss_recv.at[source], s_ss.at[step], s_rs.at[step], {"kv": source})
        arrive(
            qpart.at[source], qrecv.at[source], q_ss.at[step], q_rs.at[step], {"kv": source}
        )
    total_ss = ss_recv[0]
    for j in range(1, ranks):
        total_ss = total_ss + ss_recv[j]
    total_ss = jnp.transpose(jnp.broadcast_to(total_ss[0:1], (128, slots)))
    scale = lax.rsqrt(total_ss / D + norm_eps) * HEAD_DIM ** (-0.5)
    pieces = []
    for i in range(hg):
        cols = slice(i * HEAD_DIM, (i + 1) * HEAD_DIM)
        piece = qpart[kv, :, cols]
        for step in range(1, ranks):
            piece = piece + qrecv[kv_from(step), :, cols]
        pieces.append(piece * scale)
    kv_head = (kv * hg) // ratio
    own_key = token_keys[:, pl.ds(pl.multiple_of(kv_head * HEAD_DIM, HEAD_DIM), HEAD_DIM)]
    own_key = own_key.astype(jnp.float32)
    lane_head = lanes_of((slots, 128)) // rep
    own = jnp.zeros((slots, 128), jnp.float32)
    for i in range(hg):
        score = jnp.sum(pieces[i] * own_key, axis=1, keepdims=True)
        own = jnp.where(lane_head == kv * hg + i, score, own)
    own_t[...] = jnp.transpose(own)
    own_send[...] = own_t[pl.ds(pl.multiple_of(kv * (hg * rep), 8), hg * rep), :]
    own_recv[kv] = own_send[...]
    hot = onehot[...].astype(jnp.bfloat16)
    chosen = []
    for piece in pieces:
        high, middle, low = split3(piece)
        chosen.append(mm(hot, high) + mm(hot, middle) + mm(hot, low))
    chosen = jnp.concatenate(chosen, axis=1)
    for k in range(ranks):
        near_q_send[k] = chosen[8 * k : 8 * k + 8]
        for t in range(tiles):
            at = 8 * (ranks + k * tiles + t)
            tile = chosen[at : at + 8]
            far_q_send[(2 * t) * ranks + k] = fold(tile, False)
            far_q_send[(2 * t + 1) * ranks + k] = fold(tile, True)
    near_q_recv[kv] = near_q_send[kv]
    far_q_recv[me] = far_q_send[me]
    for step in range(1, ranks):
        peer = kv_peer(step)
        remote(
            near_q_send.at[peer], near_q_recv.at[kv], nq_ss.at[step], nq_rs.at[step], {"kv": peer}
        )
        remote(own_send, own_recv.at[kv], own_ss.at[step], own_rs.at[step], {"kv": peer})
    for step in range(1, everyone):
        peer = all_peer(step)
        remote(
            far_q_send.at[peer], far_q_recv.at[me], fq_ss.at[step], fq_rs.at[step], flat(peer)
        )

    for c in range(2, kv_here):
        send_pages(c)

    row_id = rows_of((8, 128))
    row_masks = [
        jnp.concatenate([(row_id == p).astype(jnp.bfloat16)] * ratio, axis=0) for p in range(8)
    ]

    def page_tile(queries, keys, values, lengths):
        q_high, q_middle, q_low = split3(jnp.concatenate(queries, axis=0))
        rows = 8 * ratio
        scores = jnp.zeros((3 * rows, HEAD_DIM), jnp.float32)
        for p in range(8):
            mask = row_masks[p]
            stacked = jnp.concatenate([q_high * mask, q_middle * mask, q_low * mask], axis=0)
            scores = scores + mm_nt(stacked, keys(p))
        scores = scores[:rows] + scores[rows : 2 * rows] + scores[2 * rows :]
        usable = lanes_of((rows, 128)).astype(jnp.float32) < jnp.concatenate(
            [lengths] * ratio, axis=0
        )
        scores = jnp.where(usable, scores, neg_fill)
        top = jnp.max(scores, axis=1, keepdims=True)
        weights = jnp.where(usable, jnp.exp(scores - top), 0.0)
        total = jnp.sum(weights, axis=1, keepdims=True)
        w_high, w_low = split2(weights)
        acc = jnp.zeros((2 * rows, HEAD_DIM), jnp.float32)
        for p in range(8):
            mask = row_masks[p]
            stacked = jnp.concatenate([w_high * mask, w_low * mask], axis=0)
            acc = acc + mm(stacked, values(p))
        acc = (acc[:rows] + acc[rows:]) / total
        return acc, top + jnp.log(total)

    lane_id = lanes_of((8, 128))

    def pack_acc(load, k):
        columns = []
        for first in range(0, heads, per_tile):
            merged = None
            for i in range(per_tile):
                turn = (span * (i - k)) % HEAD_DIM
                moved = load(first + i)
                if turn:
                    moved = pltpu.roll(moved, turn, 1)
                merged = moved if merged is None else jnp.where(lane_id // span == i, moved, merged)
            columns.append(merged)
        return columns[0] if len(columns) == 1 else jnp.concatenate(columns, axis=1)

    for step in range(1, ranks):
        source = kv_from(step)
        arrive(
            near_q_send.at[source],
            near_q_recv.at[source],
            nq_ss.at[step],
            nq_rs.at[step],
            {"kv": source},
        )
    load_r.wait()
    near_length = column_of(meta[3:4], 0)
    lse_tile = jnp.zeros((8, 128), jnp.float32)
    for j in range(kv_here):
        queries = []
        for i in range(ratio):
            head = j * ratio + i
            at = (head % hg) * HEAD_DIM
            queries.append(near_q_recv[head // hg, :, at : at + HEAD_DIM])
        cols = slice(j * HEAD_DIM, (j + 1) * HEAD_DIM)
        acc, lse = page_tile(
            queries,
            lambda p: res_v[p, 0, :, cols],
            lambda p: res_v[p, 1, :, cols],
            near_length,
        )
        for i in range(ratio):
            head = j * ratio + i
            near_acc[head] = acc[8 * i : 8 * i + 8]
            lse_tile = jnp.where(lane_id // rep == head, lse[8 * i : 8 * i + 8], lse_tile)
    near_l_send[...] = lse_tile
    near_l_recv[kv] = lse_tile
    for k in range(ranks):
        near_a_send[k] = pack_acc(lambda head: near_acc[head], k)
    near_a_recv[kv] = near_a_send[kv]
    for step in range(1, ranks):
        peer = kv_peer(step)
        remote(near_l_send, near_l_recv.at[kv], nl_ss.at[step], nl_rs.at[step], {"kv": peer})
        remote(
            near_a_send.at[peer], near_a_recv.at[kv], na_ss.at[step], na_rs.at[step], {"kv": peer}
        )

    for step in range(1, everyone):
        source = all_from(step)
        arrive(
            far_q_send.at[source],
            far_q_recv.at[source],
            fq_ss.at[step],
            fq_rs.at[step],
            flat(source),
        )
    far_lengths = []
    for t in range(tiles):
        offset = grp * NPR
        first = column_of(meta_v[(2 * t) * ranks + kv][1:2], offset)
        second = column_of(meta_v[(2 * t + 1) * ranks + kv][1:2], offset - 4)
        far_lengths.append(jnp.where(rows_of((8, 1)) < 4, first, second))
    far_lse_tiles = [jnp.zeros((8, 128), jnp.float32) for _ in range(tiles)]
    for c in range(kv_here):
        if c > 0:
            sort_pages(c)
        if c == 1:
            forward_pages(1, 0)
            forward_pages(1, 1)
        for t in range(tiles):
            queries = []
            for i in range(ratio):
                head = c * ratio + i
                k = head // hg
                wide = unfold(
                    far_q_recv[(2 * t) * ranks + k],
                    far_q_recv[(2 * t + 1) * ranks + k],
                    hgw,
                    odd_here,
                )
                at = (head % hg) * HEAD_DIM
                queries.append(wide[:, at : at + HEAD_DIM])
            acc, lse = page_tile(
                queries,
                lambda p: sorted_v[c][8 * t + p, 0],
                lambda p: sorted_v[c][8 * t + p, 1],
                far_lengths[t],
            )
            for i in range(ratio):
                head = c * ratio + i
                far_acc[t, head] = acc[8 * i : 8 * i + 8]
                far_lse_tiles[t] = jnp.where(
                    lane_id // rep == head, lse[8 * i : 8 * i + 8], far_lse_tiles[t]
                )
    for t in range(tiles):
        for k in range(ranks):
            tile = pack_acc(lambda head: far_acc[t, head], k)
            far_a_send[(2 * t) * ranks + k] = fold(tile, False)
            far_a_send[(2 * t + 1) * ranks + k] = fold(tile, True)
        far_l_send[t] = far_lse_tiles[t]
    far_a_recv[me] = far_a_send[me]
    far_l_recv[me] = far_l_send[grp // 2]
    for step in range(1, everyone):
        peer = all_peer(step)
        remote(
            far_l_send.at[peer // (2 * ranks)],
            far_l_recv.at[me],
            fl_ss.at[step],
            fl_rs.at[step],
            flat(peer),
        )
        remote(
            far_a_send.at[peer], far_a_recv.at[me], fa_ss.at[step], fa_rs.at[step], flat(peer)
        )

    for c in range(2, kv_here):
        forward_pages(c, 0)
        forward_pages(c, 1)

    onehot_t[...] = jnp.transpose(onehot[...]).astype(jnp.bfloat16)
    lane = lanes_of((1, part))
    wanted = (lane // (span * ratio)) * HEAD_DIM + kv * span + lax.rem(lane, span)
    choose = (rows_of((kv_here * HEAD_DIM, part)) == wanted).astype(jnp.bfloat16)
    own_piece = mm(token_values[...], choose)
    widen = (
        rows_of((128, part)) == (lanes_of((128, part)) // span) * rep
    ).astype(jnp.bfloat16)
    for step in range(1, ranks):
        source = kv_from(step)
        arrive(own_send, own_recv.at[source], own_ss.at[step], own_rs.at[step], {"kv": source})
        arrive(
            near_l_send, near_l_recv.at[source], nl_ss.at[step], nl_rs.at[step], {"kv": source}
        )
        arrive(
            near_a_send.at[source],
            near_a_recv.at[source],
            na_ss.at[step],
            na_rs.at[step],
            {"kv": source},
        )
    own_all = jnp.transpose(own_recv[...].reshape(128, slots))
    for k in range(ranks):
        all_lse[8 * k : 8 * k + 8, :] = near_l_recv[k]
        all_acc[8 * k : 8 * k + 8, :] = near_a_recv[k]
    for step in range(1, everyone):
        source = all_from(step)
        arrive(
            far_l_send.at[0],
            far_l_recv.at[source],
            fl_ss.at[step],
            fl_rs.at[step],
            flat(source),
        )
        arrive(
            far_a_send.at[source],
            far_a_recv.at[source],
            fa_ss.at[step],
            fa_rs.at[step],
            flat(source),
        )
    for k in range(ranks):
        for t in range(tiles):
            at = 8 * (ranks + k * tiles + t)
            one, two = (2 * t) * ranks + k, (2 * t + 1) * ranks + k
            all_lse[at : at + 8, :] = pick_rows(far_l_recv[one], far_l_recv[two], odd_here)
            all_acc[at : at + 8, :] = unfold(far_a_recv[one], far_a_recv[two], part, odd_here)
    used = 8 * count_tiles
    for at in range(used, all_lse.shape[0], 8):
        all_lse[at : at + 8, :] = jnp.zeros((8, 128), jnp.float32)
        all_acc[at : at + 8, :] = jnp.zeros((8, part), jnp.float32)
    top = jnp.full((slots, 128), neg_fill, jnp.float32)
    slot_id = rows_of((slots, 128)).astype(jnp.float32)
    diagonal = lax.rem(lane_id, rep)
    turns = [(row_id == diagonal + rep * h).astype(jnp.float32) for h in range(8 // rep if rep < 8 else 1)]
    for i, column in enumerate(slot_rows):
        tile = all_lse[8 * i : 8 * i + 8, :]
        for hit in turns:
            value = jnp.sum(tile * hit, axis=0, keepdims=True)
            owner = jnp.sum(column * hit, axis=0, keepdims=True)
            top = jnp.maximum(top, jnp.where(slot_id == owner, value, neg_fill))
    wide_lane = lanes_of((slots, 128))
    shift = 1
    while shift < rep:
        up = pltpu.roll(top, shift, 1)
        down = pltpu.roll(top, 128 - shift, 1)
        top = jnp.maximum(top, jnp.where((wide_lane & shift) != 0, up, down))
        shift *= 2
    top = jnp.maximum(top, own_all)
    high, middle, low = split3(top)
    page_top = mm(hot, high) + mm(hot, middle) + mm(hot, low)
    page_weight = jnp.exp(all_lse[...] - page_top)
    own_weight = jnp.exp(own_all - top)
    hot_t = onehot_t[...]
    high, low = split2(page_weight)
    total = mm(hot_t, high) + mm(hot_t, low) + own_weight
    high, low = split2(
        jnp.concatenate([page_weight, own_weight, pl.reciprocal(total)], axis=0)
    )
    spread = mm(high, widen) + mm(low, widen)
    padded = all_lse.shape[0]
    high, low = split2(all_acc[...] * spread[:padded])
    gathered = mm(hot_t, high) + mm(hot_t, low)
    gathered = gathered + own_piece * spread[padded : padded + slots]
    piece = (gathered * spread[padded + slots :]).astype(jnp.bfloat16)
    piece_v[...] = piece.reshape(piece_v.shape)
    rows16 = piece_v.shape[2]
    half = ranks * rows16

    def halves_last(ref):
        return jnp.concatenate(
            [ref[:, 1 - tp].reshape(half, part), ref[:, tp].reshape(half, part)], axis=0
        )

    def scatter_start(c, value, send, recv, ss, rs):
        send[c] = value[:half].astype(jnp.bfloat16)
        remote(send.at[c], recv.at[c], ss.at[c], rs.at[c], partner)
        keep_v[c] = value[half:]

    def scatter_middle(c, extra, first, second, sems1, sems2):
        arrive(first[0].at[c], first[1].at[c], sems1[0].at[c], sems1[1].at[c], partner)
        both = keep_v[c] + first[1][c].astype(jnp.float32)
        if extra is not None:
            both = both + extra
        second[0][c] = both.astype(jnp.bfloat16).reshape(ranks, rows16, cw)
        second[1][c, kv] = second[0][c, kv]
        for step in range(1, ranks):
            peer = kv_peer(step)
            remote(
                second[0].at[c, peer],
                second[1].at[c, kv],
                sems2[0].at[c, step],
                sems2[1].at[c, step],
                {"kv": peer},
            )

    def scatter_end(c, second, sems2):
        for step in range(1, ranks):
            source = kv_from(step)
            arrive(
                second[0].at[c, source],
                second[1].at[c, source],
                sems2[0].at[c, step],
                sems2[1].at[c, step],
                {"kv": source},
            )
        total = second[1][c, 0].astype(jnp.float32)
        for j in range(1, ranks):
            total = total + second[1][c, j].astype(jnp.float32)
        return total

    load_o.wait()
    ordered = halves_last(piece_v)
    width_here = hidden.shape[1]
    lag = 2
    for c in range(chunks + lag):
        if c < chunks:
            scatter_start(
                c, mm(ordered, wo_v[:, c * cw : (c + 1) * cw]), r1_send, r1_recv, r1_ss, r1_rs
            )
        if c >= lag:
            d = c - lag
            at = (d * cw) % width_here
            mine = hidden[:, at : at + cw].reshape(ranks, 2, rows16, cw)
            mine = jnp.where(tp == 0, mine[:, 0], mine[:, 1]).reshape(half, cw)
            mine = mine.astype(jnp.float32)
            mine = jnp.where(kv == (d * cw) // width_here, mine, 0.0)
            scatter_middle(
                d, mine, (r1_send, r1_recv), (r2_send, r2_recv), (r1_ss, r1_rs), (r2_ss, r2_rs)
            )
    for c in range(chunks):
        block = scatter_end(c, (r2_send, r2_recv), (r2_ss, r2_rs)).astype(jnp.bfloat16)
        kept_v[c] = block
        resid_v[c, 1, kv] = block
        for step in range(1, ranks):
            remote(
                kept_v.at[c],
                resid_v.at[c, 1, kv],
                g_ss.at[c, step],
                g_rs.at[c, step],
                {"kv": kv_peer(step)},
            )
        remote(kept_v.at[c], resid_v.at[c, 0, kv], gp_ss.at[c, 0], gp_rs.at[c, 0], partner)
    square_sum = jnp.zeros((2 * half, 1), jnp.float32)
    for c in range(chunks):
        for step in range(1, ranks):
            source = kv_from(step)
            arrive(
                kept_v.at[c],
                resid_v.at[c, 1, source],
                g_ss.at[c, step],
                g_rs.at[c, step],
                {"kv": source},
            )
            remote(
                resid_v.at[c, 1, source],
                resid_v.at[c, 0, source],
                gp_ss.at[c, step],
                gp_rs.at[c, step],
                partner,
            )
    for c in range(chunks):
        for step in range(ranks):
            source = kv_from(step)
            arrive(
                kept_v.at[c],
                resid_v.at[c, 0, source],
                gp_ss.at[c, step],
                gp_rs.at[c, step],
                partner,
            )
        block = resid_v[c].reshape(2 * half, cw).astype(jnp.float32)
        square_sum = square_sum + jnp.sum(block * block, axis=1, keepdims=True)
        cols = slice(c * cw, (c + 1) * cw)
        normed_v[:, cols] = (block * mlp_gain[:, cols]).astype(jnp.bfloat16)
    mlp_scale = lax.rsqrt(square_sum / D + norm_eps)
    for n in range(gate_tiles):
        slot = n % ring
        for copy in gate_loads(n):
            copy.wait()
        gate = mm(normed_v[...], wg_v[slot]) * mlp_scale
        upward = mm(normed_v[...], wu_v[slot]) * mlp_scale
        units = gate / (1.0 + jnp.exp(-gate)) * upward
        units_v[:, n * tile_n : (n + 1) * tile_n] = units.astype(jnp.bfloat16)
        if n + ring < gate_tiles:
            for copy in gate_loads(n + ring):
                copy.start()
    for c in range(chunks + lag):
        if c < chunks:
            down_load(c).wait()
            value = mm(units_v[...], wd_v[c % down_ring])
            scatter_start(c, value, d1_send, d1_recv, d1_ss, d1_rs)
            if c + down_ring < chunks:
                down_load(c + down_ring).start()
        if c >= lag:
            scatter_middle(
                c - lag,
                None,
                (d1_send, d1_recv),
                (d2_send, d2_recv),
                (d1_ss, d1_rs),
                (d2_ss, d2_rs),
            )
    for c in range(chunks):
        total = scatter_end(c, (d2_send, d2_recv), (d2_ss, d2_rs))
        total = total + kept_v[c].astype(jnp.float32)
        mixed_out[:, c * cw : (c + 1) * cw] = total.astype(jnp.bfloat16)
    for c in range(kv_here):
        cols = pl.ds(c * HEAD_DIM, HEAD_DIM)
        for kind in range(2):
            for step in range(1, groups):
                source = grp_from(step)
                arrive(
                    sorted_v[c].at[pages_of(source), kind],
                    arrived_out.at[pages_of(source), kind, :, cols],
                    z_ss.at[c, kind, step],
                    z_rs.at[c, kind, step],
                    {"grp": source},
                )
    for store in stores:
        store.wait()
    for copy in pending:
        copy.wait_send()


def fused_step(dims, picked, inverse, *args):
    meta, hidden, gain, token_keys, token_values, wq, pool, res, wo, mlp_gain, wg, wu, wd = args
    groups, ranks, cap, kv_here, heads = (dims[name] for name in ("groups", "ranks", "cap", "kv_here", "heads"))
    hgw = heads // ranks * HEAD_DIM
    part = heads * HEAD_DIM // ranks
    everyone = groups * ranks
    pages = groups * NPR
    tiles = pages // 8
    slots = hidden.shape[0]
    rep = HEAD_DIM // heads
    tokens = pool.shape[2]
    rows = 8 * (ranks + ranks * tiles)
    rows = -(-rows // 128) * 128
    model = wo.shape[1]
    cw = min(512, hidden.shape[1])
    chunks = model // cw
    block = slots // (2 * ranks)
    half_rows = slots // 2
    tile_n = 256 if wg.shape[1] % 256 == 0 else wg.shape[1]
    ring = min(RING, wg.shape[1] // tile_n)
    down_ring = min(DOWN_RING, chunks)
    half = lambda width: width // 2 if width >= 256 else width
    f32, bf16 = jnp.float32, jnp.bfloat16
    chunk = lambda count: [pltpu.VMEM((count, 2, tokens, HEAD_DIM), bf16) for _ in range(kv_here)]
    dma = lambda *shape: pltpu.SemaphoreType.DMA(shape)
    scratch = [
        chunk(pool.shape[0]),
        chunk(pages),
        chunk(pages),
        chunk(pages),
        pltpu.VMEM(res.shape, bf16),
        pltpu.VMEM(wq.shape, bf16),
        pltpu.VMEM(wo.shape, bf16),
        pltpu.VMEM((everyone, 8, 128), jnp.int32),
        pltpu.VMEM((ranks, slots, hgw), f32),
        pltpu.VMEM((ranks, slots, hgw), f32),
        pltpu.VMEM((8, slots), f32),
        pltpu.VMEM((ranks, 8, slots), f32),
        pltpu.VMEM((rows, slots), f32),
        pltpu.VMEM((slots, rows), bf16),
        pltpu.VMEM((ranks, 8, hgw), f32),
        pltpu.VMEM((ranks, 8, hgw), f32),
        pltpu.VMEM((everyone, 8, half(hgw)), f32),
        pltpu.VMEM((everyone, 8, half(hgw)), f32),
        pltpu.VMEM((128, slots), f32),
        pltpu.VMEM((heads // ranks * rep, slots), f32),
        pltpu.VMEM((ranks, heads // ranks * rep, slots), f32),
        pltpu.VMEM((heads, 8, HEAD_DIM), f32),
        pltpu.VMEM((8, 128), f32),
        pltpu.VMEM((tiles, heads, 8, HEAD_DIM), f32),
        pltpu.VMEM((tiles, 8, 128), f32),
        pltpu.VMEM((ranks, 8, part), f32),
        pltpu.VMEM((ranks, 8, part), f32),
        pltpu.VMEM((8, 128), f32),
        pltpu.VMEM((ranks, 8, 128), f32),
        pltpu.VMEM((everyone, 8, half(part)), f32),
        pltpu.VMEM((everyone, 8, half(part)), f32),
        pltpu.VMEM((tiles, 8, 128), f32),
        pltpu.VMEM((everyone, 8, 128), f32),
        pltpu.VMEM((rows, 128), f32),
        pltpu.VMEM((rows, part), f32),
        pltpu.VMEM((ranks, 2, block, part), bf16),
        pltpu.VMEM((chunks, half_rows, cw), f32),
        pltpu.VMEM((chunks, half_rows, cw), bf16),
        pltpu.VMEM((chunks, half_rows, cw), bf16),
        pltpu.VMEM((chunks, ranks, block, cw), bf16),
        pltpu.VMEM((chunks, ranks, block, cw), bf16),
        pltpu.VMEM((chunks, half_rows, cw), bf16),
        pltpu.VMEM((chunks, half_rows, cw), bf16),
        pltpu.VMEM((chunks, ranks, block, cw), bf16),
        pltpu.VMEM((chunks, ranks, block, cw), bf16),
        pltpu.VMEM((chunks, block, cw), bf16),
        pltpu.VMEM((chunks, 2, ranks, block, cw), bf16),
        pltpu.VMEM((slots, model), bf16),
        pltpu.VMEM((slots, wg.shape[1]), bf16),
        pltpu.VMEM((ring, model, tile_n), bf16),
        pltpu.VMEM((ring, model, tile_n), bf16),
        pltpu.VMEM((down_ring, wd.shape[0], cw), bf16),
        dma(kv_here + 3),
        dma(2, ring),
        dma(down_ring),
        dma(everyone),
        dma(everyone),
        dma(kv_here, ranks),
        dma(kv_here, ranks),
        dma(ranks),
        dma(ranks),
        dma(ranks),
        dma(ranks),
        dma(ranks),
        dma(ranks),
        dma(everyone),
        dma(everyone),
        dma(ranks),
        dma(ranks),
        dma(ranks),
        dma(ranks),
        dma(ranks),
        dma(ranks),
        dma(everyone),
        dma(everyone),
        dma(everyone),
        dma(everyone),
        dma(kv_here, 2, groups),
        dma(kv_here, 2, groups),
        dma(kv_here, 2),
        dma(chunks),
        dma(chunks),
        dma(chunks, ranks),
        dma(chunks, ranks),
        dma(chunks),
        dma(chunks),
        dma(chunks, ranks),
        dma(chunks, ranks),
        dma(chunks, ranks),
        dma(chunks, ranks),
        dma(chunks, ranks),
        dma(chunks, ranks),
    ]
    vmem = pl.BlockSpec(memory_space=pltpu.VMEM)
    smem = pl.BlockSpec(memory_space=pltpu.SMEM)
    hbm = pl.BlockSpec(memory_space=pl.ANY)
    return pl.pallas_call(
        functools.partial(step_kernel, dims),
        out_shape=(
            jax.ShapeDtypeStruct((block, model), bf16),
            jax.ShapeDtypeStruct((pages,) + pool.shape[1:], bf16),
        ),
        in_specs=[smem, smem] + [vmem] * 5 + [hbm] * 4 + [vmem] + [hbm] * 3,
        out_specs=(vmem, hbm),
        scratch_shapes=scratch,
        compiler_params=pltpu.CompilerParams(
            collective_id=1, has_side_effects=True, vmem_limit_bytes=67043328
        ),
        name="fused_step",
    )(picked, inverse, *args)


def route_tables(new_owner, new_local):
    groups = lax.axis_size("grp")
    ranks = lax.axis_size("kv")
    per_dev = new_owner.shape[1] // ranks
    cap = groups * NPR // ranks
    grp_rank = lax.axis_index("grp")
    kv_rank = lax.axis_index("kv")
    myself = grp_rank * ranks + kv_rank
    places = jnp.arange(cap, dtype=jnp.int32)
    by_col = (
        new_owner.reshape(groups, ranks, per_dev)
        .transpose(1, 0, 2)
        .reshape(ranks, groups * per_dev)
    )
    local_col = (
        new_local.reshape(groups, ranks, per_dev)
        .transpose(1, 0, 2)
        .reshape(ranks, groups * per_dev)
    )
    select = nth_match(by_col, myself, places)
    picked = jnp.sum(jnp.where(select, local_col[:, None, :], 0), axis=2)
    row_here = lax.dynamic_index_in_dim(by_col, kv_rank, 0, keepdims=False)
    sources = grp_rank * ranks + jnp.arange(ranks, dtype=jnp.int32)
    hits = nth_match(
        jnp.broadcast_to(row_here[None, :], (ranks, row_here.shape[0])), sources[:, None], places
    )
    spots = jnp.arange(row_here.shape[0], dtype=jnp.int32)
    where_f = jnp.sum(jnp.where(hits, spots[None, None, :], 0), axis=2).reshape(-1)
    dest_grp = where_f // per_dev
    dest_pos = where_f % per_dev
    same = (dest_grp[:, None] == dest_grp[None, :]) & (dest_pos[:, None] < dest_pos[None, :])
    rank_in = jnp.sum(same.astype(jnp.int32), axis=0)
    target = dest_grp * NPR + rank_in
    items = jnp.arange(target.shape[0], dtype=jnp.int32)
    inverse = jnp.sum(jnp.where(target[None, :] == items[:, None], items[None, :], 0), axis=1)
    return picked.reshape(-1), inverse


def per_device(
    hidden_states,
    attn_gain,
    mlp_gain,
    w_query,
    w_out,
    w_gate,
    w_up,
    w_down,
    kv_pool,
    resident_cache,
    resident_slot,
    resident_len,
    new_owner,
    new_local,
    new_slot,
    new_len,
    token_kv,
):
    groups = lax.axis_size("grp")
    ranks = lax.axis_size("kv")
    heads_here = w_query.shape[1] // HEAD_DIM
    kv_here = token_kv.shape[2] // HEAD_DIM
    dims = {
        "groups": groups,
        "ranks": ranks,
        "cap": groups * NPR // ranks,
        "kv_here": kv_here,
        "heads": heads_here,
    }
    arrived_at = arrival_places(new_owner)
    picked, inverse = route_tables(new_owner, new_local)
    items = jnp.arange(arrived_at.shape[0], dtype=jnp.int32)
    hit = arrived_at[None, :] == items[:, None]
    slot_by = jnp.sum(jnp.where(hit, new_slot, 0), axis=1)
    len_by = jnp.sum(jnp.where(hit, new_len, 0), axis=1)
    meta = jnp.stack(
        [
            lanes(values[None], 128)[0]
            for values in (slot_by, len_by, resident_slot[0], resident_len[0])
        ]
    )
    meta = jnp.pad(meta, ((0, 4), (0, 0)))
    mixed, arrived = fused_step(
        dims,
        picked,
        inverse,
        meta,
        hidden_states,
        attn_gain[None],
        token_kv[:, 0],
        token_kv[:, 1],
        w_query,
        kv_pool,
        resident_cache[0],
        w_out.reshape(-1, w_out.shape[2]),
        mlp_gain[None],
        w_gate,
        w_up,
        w_down,
    )
    new_pages = jnp.take(arrived, arrived_at, axis=0, mode="clip")
    return (mixed, new_pages[None])


def solution(mesh):
    return jax.shard_map(
        per_device,
        mesh=mesh,
        in_specs=(
            P("grp", "kv"),
            P("kv"),
            P(),
            P("kv", "tp"),
            P("tp", "kv", None),
            P(None, ("kv", "tp")),
            P(None, ("kv", "tp")),
            P(("kv", "tp"), None),
            P(("grp", "kv"), None, None, "tp"),
            P("grp", "kv", None, None, "tp"),
            P("grp", "kv"),
            P("grp", "kv"),
            P(),
            P(),
            P("grp", "kv"),
            P("grp", "kv"),
            P("grp", None, "tp"),
        ),
        out_specs=(P(("grp", "kv", "tp"), None), P("grp", "kv", None, None, "tp")),
        check_vma=False,
    )
```

```python
import functools

import jax
import jax.numpy as jnp
from jax import lax
from jax.experimental import pallas as pl
from jax.experimental.pallas import tpu as pltpu
from jax.sharding import PartitionSpec as P

D = 4096
HEADS = 32
KV_HEADS = 8
HEAD_DIM = 128
NPR = 4


neg_fill = -1e30
norm_eps = 1e-05


RING = 4
DOWN_RING = 4


def split2(x):
    high = x.astype(jnp.bfloat16)
    return high, (x - high.astype(jnp.float32)).astype(jnp.bfloat16)


def split3(x):
    high = x.astype(jnp.bfloat16)
    rest = x - high.astype(jnp.float32)
    middle = rest.astype(jnp.bfloat16)
    return high, middle, (rest - middle.astype(jnp.float32)).astype(jnp.bfloat16)


def mm(a, b):
    return jnp.dot(a, b, preferred_element_type=jnp.float32)


def mm_nt(a, b):
    return lax.dot_general(a, b, (((1,), (1,)), ((), ())), preferred_element_type=jnp.float32)


def rows_of(shape):
    return lax.broadcasted_iota(jnp.int32, shape, 0)


def lanes_of(shape):
    return lax.broadcasted_iota(jnp.int32, shape, 1)


def half_turn(x):
    return pltpu.roll(x, 4, 0)


def fold(tile, odd):
    if tile.shape[1] < 256:
        return tile
    half = tile.shape[1] // 2
    low, high = tile[:, :half], tile[:, half:]
    top = rows_of(low.shape) < 4
    if odd:
        return jnp.where(top, half_turn(low), high)
    return jnp.where(top, low, half_turn(high))


def pick_rows(first, second, odd):
    first = jnp.where(odd, half_turn(first), first)
    second = jnp.where(odd, second, half_turn(second))
    return jnp.where(rows_of(first.shape) < 4, first, second)


def unfold(first, second, width, odd):
    if width < 256:
        return pick_rows(first, second, odd)
    top = rows_of(first.shape) < 4
    low = jnp.where(top, first, half_turn(second))
    high = jnp.where(top, half_turn(first), second)
    return jnp.concatenate([low, high], axis=1)


def column_of(row, keys, offset):
    wide = jnp.broadcast_to(row, (8, 128)).astype(jnp.float32)
    hit = jnp.broadcast_to(keys, (8, 128)) == rows_of((8, 128)) + offset
    return jnp.sum(jnp.where(hit, wide, 0.0), axis=1, keepdims=True)


def place_in_group(groups, ranks):
    grp = lax.axis_index("grp")
    kv = lax.axis_index("kv")
    me = grp * ranks + kv

    def flat(index):
        return {"grp": index // ranks, "kv": lax.rem(index, ranks)}

    return grp, kv, me, flat


def step_kernel(
    dims,
    owner,
    local,
    new_slot,
    new_len,
    kept_slot,
    kept_len,
    hidden_hbm,
    gain,
    token_hbm,
    wq_hbm,
    pool_hbm,
    res_hbm,
    wo_hbm,
    mlp_gain,
    wg_hbm,
    wu_hbm,
    wd_hbm,
    mixed_out,
    arrived_out,
    meta_out,
    table,
    owner_v,
    local_v,
    meta,
    hidden,
    token_v,
    pool_v,
    send_v,
    recv_v,
    sorted_v,
    res_v,
    wq_v,
    wo_v,
    meta_v,
    qpart,
    ss_send,
    ss_recv,
    onehot,
    onehot_t,
    near_q_send,
    near_q_recv,
    rows_send,
    rows_recv,
    far_q_send,
    far_q_recv,
    own_t,
    own_send,
    own_recv,
    near_send,
    near_recv,
    far_send,
    far_recv,
    all_lse,
    all_acc,
    piece_v,
    branch_v,
    feature_v,
    keep_v,
    r1_send,
    r1_recv,
    r2_send,
    r2_recv,
    d1_send,
    d1_recv,
    d2_send,
    d2_recv,
    kept_v,
    resid_v,
    gate_v,
    up_v,
    units_v,
    wg_v,
    wu_v,
    wd_v,
    load_sem,
    gate_sem,
    down_sem,
    meta_ss,
    meta_rs,
    page_ss,
    page_rs,
    q_ss,
    q_rs,
    s_ss,
    s_rs,
    nq_ss,
    nq_rs,
    fq_ss,
    fq_rs,
    own_ss,
    own_rs,
    na_ss,
    na_rs,
    fa_ss,
    fa_rs,
    z_ss,
    z_rs,
    z_own,
    r1_ss,
    r1_rs,
    r2_ss,
    r2_rs,
    d1_ss,
    d1_rs,
    d2_ss,
    d2_rs,
    g_ss,
    g_rs,
    gp_ss,
    gp_rs,
):
    groups, ranks, cap, kv_here, heads = (dims[name] for name in ("groups", "ranks", "cap", "kv_here", "heads"))
    ratio = heads // kv_here
    hg = heads // ranks
    hgw = hg * HEAD_DIM
    span = HEAD_DIM // ranks
    part = heads * span
    per_tile = HEAD_DIM // span
    everyone = groups * ranks
    tiles = groups * NPR // 8
    count_tiles = ranks + ranks * tiles
    grp, kv, me, flat = place_in_group(groups, ranks)
    tp = lax.axis_index("tp")
    partner = {"tp": 1 - tp}
    odd_here = lax.rem(grp, 2) == 1
    slots = hidden.shape[0]

    def kv_peer(step):
        return lax.rem(kv + step, ranks)

    def kv_from(step):
        return lax.rem(kv - step + ranks, ranks)

    def all_peer(step):
        return lax.rem(me + step, everyone)

    def all_from(step):
        return lax.rem(me - step + everyone, everyone)

    pending = []

    def remote(src, dst, ss, rs, where):
        copy = pltpu.make_async_remote_copy(
            src_ref=src,
            dst_ref=dst,
            send_sem=ss,
            recv_sem=rs,
            device_id=where,
            device_id_type=pl.DeviceIdType.MESH,
        )
        copy.start()
        pending.append(copy)

    def arrive(src, dst, ss, rs, where):
        pltpu.make_async_remote_copy(
            src_ref=src,
            dst_ref=dst,
            send_sem=ss,
            recv_sem=rs,
            device_id=where,
            device_id_type=pl.DeviceIdType.MESH,
        ).wait_recv()

    loads = []
    for c in range(kv_here):
        cols = pl.ds(c * HEAD_DIM, HEAD_DIM)
        loads.append(
            pltpu.make_async_copy(pool_hbm.at[:, :, :, cols], pool_v[c], load_sem.at[c])
        )
    load_q = pltpu.make_async_copy(wq_hbm, wq_v, load_sem.at[kv_here])
    load_r = pltpu.make_async_copy(res_hbm, res_v, load_sem.at[kv_here + 1])
    load_o = pltpu.make_async_copy(wo_hbm, wo_v, load_sem.at[kv_here + 2])
    load_h = pltpu.make_async_copy(hidden_hbm, hidden, load_sem.at[kv_here + 3])
    load_t = pltpu.make_async_copy(token_hbm, token_v, load_sem.at[kv_here + 4])
    loads[0].start()
    load_h.start()
    load_q.start()
    for copy in loads[1:]:
        copy.start()
    load_r.start()
    load_t.start()
    load_o.start()

    barrier = pltpu.get_barrier_semaphore()
    for step in range(1, everyone):
        pl.semaphore_signal(
            barrier, inc=1, device_id=flat(all_peer(step)), device_id_type=pl.DeviceIdType.MESH
        )
    pl.semaphore_signal(
        barrier, inc=1, device_id=partner, device_id_type=pl.DeviceIdType.MESH
    )
    per = owner.shape[1] // ranks
    wide = owner_v.shape[1]
    owner_v[...] = jnp.full((8, wide), -1, jnp.int32)
    local_v[...] = jnp.zeros((8, wide), jnp.int32)
    owner_v[: owner.shape[0], : owner.shape[1]] = owner[...]
    local_v[: owner.shape[0], : owner.shape[1]] = local[...]
    owners, locals_ = owner_v[...], local_v[...]
    table_row, table_lane = rows_of((8, wide)), lanes_of((8, wide))
    place = lax.rem(table_lane, per)
    column = table_lane // per

    def before(match):
        count = match.astype(jnp.int32)
        ahead, behind = count, count
        shift = 1
        while shift < per:
            ahead = ahead + jnp.where(place >= shift, pltpu.roll(ahead, shift, 1), 0)
            behind = behind + jnp.where(
                place < per - shift, pltpu.roll(behind, wide - shift, 1), 0
            )
            shift *= 2
        return ahead - count, ahead - count + behind

    def order(match):
        ahead, whole = before(match)
        for shift in range(1, groups):
            ahead = ahead + jnp.where(table_row >= shift, pltpu.roll(whole, shift, 0), 0)
        return ahead

    def total_of(values):
        return jnp.sum(jnp.sum(values, axis=0, keepdims=True))

    mine = owners == me
    mine_order = order(mine)
    for k in range(ranks):
        for a in range(cap):
            hit = mine & (mine_order == a) & (column == k)
            table[k * cap + a] = total_of(jnp.where(hit, locals_, 0))
    row_base = grp * ranks
    here = (owners >= row_base) & (owners < row_base + ranks) & (column == kv)
    here_order = order(here)
    landed = jnp.zeros((8, wide), jnp.int32)
    for k in range(ranks):
        match = here & (owners == row_base + k)
        landed = landed + jnp.where(match, k * cap + order(match), 0)
    for i in range(groups * NPR):
        hit = here & (here_order == i)
        table[ranks * cap + i] = total_of(jnp.where(hit, landed, 0))
    spot = jnp.zeros((8, wide), jnp.int32)
    for g in range(groups):
        match = (owners >= g * ranks) & (owners < (g + 1) * ranks)
        spot = spot + jnp.where(match, g * NPR + before(match)[0], 0)
    spot = jnp.where((table_row == grp) & (column == kv), spot, 0)
    spot = jnp.broadcast_to(jnp.sum(spot, axis=0, keepdims=True), (8, wide))
    spot = pltpu.roll(spot, lax.rem(wide - kv * per, wide), 1)[:1, :128]
    meta[...] = jnp.zeros((8, 128), jnp.int32)
    meta[0:1, :per] = new_slot[...]
    meta[1:2, :per] = new_len[...]
    meta[2:3, : kept_slot.shape[1]] = kept_slot[...]
    meta[3:4, : kept_slot.shape[1]] = kept_len[...]
    meta[4:5, :] = jnp.where(lanes_of((1, 128)) < per, spot, -1)
    meta[5:6, :] = lanes_of((1, 128))
    meta_out[...] = meta[...]
    pl.semaphore_wait(barrier, everyone)

    for step in range(1, everyone):
        remote(meta, meta_v.at[me], meta_ss.at[step], meta_rs.at[step], flat(all_peer(step)))
    meta_v[me] = meta[...]

    loaded = set()

    def send_pages(c, kind):
        if c not in loaded:
            loads[c].wait()
            loaded.add(c)

        def pick(i, carry):
            for a in range(cap):
                target = lax.rem(kv + i, ranks) * cap + a
                send_v[c][kind, i * cap + a] = pool_v[c][table[target], kind]
            return carry

        for a in range(cap):
            recv_v[2 * c + kind][kv * cap + a] = pool_v[c][table[kv * cap + a], kind]
        lax.fori_loop(1, ranks, pick, 0)
        for step in range(1, ranks):
            remote(
                send_v[c].at[kind, pl.ds(step * cap, cap)],
                recv_v[2 * c + kind].at[pl.ds(kv * cap, cap)],
                page_ss.at[c, kind, step],
                page_rs.at[c, kind, step],
                {"kv": kv_peer(step)},
            )

    def sort_pages(c, kind):
        for step in range(1, ranks):
            source = kv_from(step)
            arrive(
                send_v[c].at[kind, pl.ds(step * cap, cap)],
                recv_v[2 * c + kind].at[pl.ds(source * cap, cap)],
                page_ss.at[c, kind, step],
                page_rs.at[c, kind, step],
                {"kv": source},
            )

        def sort(i, carry):
            sorted_v[c][kind, i] = recv_v[2 * c + kind][table[ranks * cap + i]]
            return carry

        lax.fori_loop(0, groups * NPR, sort, 0)

    def pages_of(group):
        return pl.ds(pl.multiple_of(group * NPR, NPR), NPR)

    def grp_peer(step):
        return lax.rem(grp + step, groups)

    def grp_from(step):
        return lax.rem(grp - step + groups, groups)

    stores = []

    every_step = tuple(range(1, groups))

    def forward_pages(c, kind, steps=every_step, own=True):
        cols = pl.ds(c * HEAD_DIM, HEAD_DIM)
        for step in steps:
            peer = grp_peer(step)
            remote(
                sorted_v[c].at[kind, pages_of(peer)],
                arrived_out.at[pages_of(grp), kind, :, cols],
                z_ss.at[c, kind, step],
                z_rs.at[c, kind, step],
                {"grp": peer},
            )
        if not own:
            return
        store = pltpu.make_async_copy(
            sorted_v[c].at[kind, pages_of(grp)],
            arrived_out.at[pages_of(grp), kind, :, cols],
            z_own.at[c, kind],
        )
        store.start()
        stores.append(store)

    send_pages(0, 0)
    send_pages(0, 1)

    load_h.wait()
    load_q.wait()
    features = hidden[...].astype(jnp.float32)
    normed = (features * gain[...]).astype(jnp.bfloat16)
    for j in range(ranks):
        qpart[j] = mm(normed, wq_v[:, j * hgw : (j + 1) * hgw])
    ring, cw = wg_v.shape[0], wg_v.shape[1]
    chunks = wd_hbm.shape[1] // cw
    down_ring = wd_v.shape[0]

    def gate_loads(n):
        rows = pl.ds(n * cw, cw)
        slot = n % ring
        return (
            pltpu.make_async_copy(wg_hbm.at[rows], wg_v.at[slot], gate_sem.at[0, slot]),
            pltpu.make_async_copy(wu_hbm.at[rows], wu_v.at[slot], gate_sem.at[1, slot]),
        )

    def down_load(c):
        slot = c % down_ring
        return pltpu.make_async_copy(
            wd_hbm.at[:, pl.ds(c * cw, cw)], wd_v.at[slot], down_sem.at[slot]
        )

    for n in range(ring):
        for copy in gate_loads(n):
            copy.start()
    for c in range(down_ring):
        down_load(c).start()
    squares = jnp.sum(features * features, axis=1, keepdims=True)
    ss_send[...] = jnp.transpose(jnp.broadcast_to(squares, (slots, 128)))[:8]
    ss_recv[kv] = ss_send[...]
    for step in range(1, ranks):
        peer = kv_peer(step)
        remote(ss_send, ss_recv.at[kv], s_ss.at[step], s_rs.at[step], {"kv": peer})
    load_t.wait()
    own_keys = token_v[...].astype(jnp.float32)[:, 0]
    slot_lane = lanes_of((slots, 128))
    own = jnp.zeros((slots, 128), jnp.float32)
    for head in range(heads):
        at = (head % hg) * HEAD_DIM
        key = own_keys[:, (head // ratio) * HEAD_DIM : (head // ratio + 1) * HEAD_DIM]
        score = jnp.sum(qpart[head // hg, :, at : at + HEAD_DIM] * key, axis=1, keepdims=True)
        own = jnp.where(slot_lane == head, score, own)
    own_send[...] = jnp.transpose(own)[:heads]
    own_recv[kv] = own_send[...]

    for step in range(1, everyone):
        source = all_from(step)
        arrive(meta, meta_v.at[source], meta_ss.at[step], meta_rs.at[step], flat(source))
    slot_rows = []
    for k in range(ranks):
        facts = meta_v[grp * ranks + k]
        slot_rows.append(column_of(facts[2:3], facts[5:6], 0))
    for k in range(ranks):
        facts = meta_v[grp * ranks + k]
        for t in range(tiles):
            slot_rows.append(column_of(facts[0:1], facts[4:5], 8 * t))
    for i, column in enumerate(slot_rows):
        onehot[8 * i : 8 * i + 8, :] = (
            column == lanes_of((8, slots)).astype(jnp.float32)
        ).astype(jnp.float32)
    for i in range(8 * count_tiles, onehot.shape[0], 8):
        onehot[i : i + 8, :] = jnp.zeros((8, slots), jnp.float32)

    hot = onehot[...].astype(jnp.bfloat16)

    def spread_rows(value):
        high, middle, low = split3(value)
        return mm(hot, high) + mm(hot, middle) + mm(hot, low)

    far_rows = 8 * ranks * tiles
    for j in range(ranks):
        chosen = spread_rows(qpart[j])
        for k in range(ranks):
            near_q_send[k, :, j * hgw : (j + 1) * hgw] = chosen[8 * k : 8 * k + 8]
        rows_send[j] = chosen[8 * ranks : 8 * ranks + far_rows]
    for step in range(1, ranks):
        peer = kv_peer(step)
        remote(rows_send.at[peer], rows_recv.at[kv], q_ss.at[step], q_rs.at[step], {"kv": peer})
        remote(
            near_q_send.at[peer], near_q_recv.at[kv], nq_ss.at[step], nq_rs.at[step], {"kv": peer}
        )
        remote(own_send, own_recv.at[kv], own_ss.at[step], own_rs.at[step], {"kv": peer})
    send_pages(1, 0)
    send_pages(1, 1)
    sort_pages(0, 0)
    forward_pages(0, 0)
    sort_pages(0, 1)
    forward_pages(0, 1)

    for step in range(1, ranks):
        source = kv_from(step)
        arrive(ss_send, ss_recv.at[source], s_ss.at[step], s_rs.at[step], {"kv": source})
        arrive(
            rows_send.at[source], rows_recv.at[source], q_ss.at[step], q_rs.at[step], {"kv": source}
        )
    total_ss = ss_recv[0]
    for j in range(1, ranks):
        total_ss = total_ss + ss_recv[j]
    row_scale = lax.rsqrt(total_ss[0:1] / D + norm_eps) * HEAD_DIM ** (-0.5)
    page_scale = spread_rows(jnp.transpose(jnp.broadcast_to(row_scale, (128, slots))))
    far_scale = page_scale[8 * ranks : 8 * ranks + far_rows]
    chosen = []
    for i in range(hg):
        cols = slice(i * HEAD_DIM, (i + 1) * HEAD_DIM)
        total = rows_send[kv, :, cols]
        for step in range(1, ranks):
            total = total + rows_recv[kv_from(step), :, cols]
        chosen.append(total * far_scale)
    chosen = jnp.concatenate(chosen, axis=1)
    for k in range(ranks):
        for t in range(tiles):
            at = 8 * (k * tiles + t)
            tile = chosen[at : at + 8]
            far_q_send[(2 * t) * ranks + k] = fold(tile, False)
            far_q_send[(2 * t + 1) * ranks + k] = fold(tile, True)
    far_q_recv[me] = far_q_send[me]
    for step in range(1, everyone):
        peer = all_peer(step)
        remote(
            far_q_send.at[peer], far_q_recv.at[me], fq_ss.at[step], fq_rs.at[step], flat(peer)
        )

    send_pages(2, 0)
    sort_pages(1, 0)
    forward_pages(1, 0)

    row_id = rows_of((8, 128))
    row_masks = [
        jnp.concatenate([(row_id == p).astype(jnp.bfloat16)] * ratio, axis=0) for p in range(8)
    ]

    def page_tile(queries, keys, values, lengths):
        q_high, q_middle, q_low = split3(jnp.concatenate(queries, axis=0))
        rows = 8 * ratio
        scores = jnp.zeros((3 * rows, HEAD_DIM), jnp.float32)
        for p in range(8):
            mask = row_masks[p]
            stacked = jnp.concatenate([q_high * mask, q_middle * mask, q_low * mask], axis=0)
            scores = scores + mm_nt(stacked, keys(p))
        scores = scores[:rows] + scores[rows : 2 * rows] + scores[2 * rows :]
        usable = lanes_of((rows, 128)).astype(jnp.float32) < jnp.concatenate(
            [lengths] * ratio, axis=0
        )
        scores = jnp.where(usable, scores, neg_fill)
        top = jnp.max(scores, axis=1, keepdims=True)
        weights = jnp.where(usable, jnp.exp(scores - top), 0.0)
        total = jnp.sum(weights, axis=1, keepdims=True)
        w_high, w_low = split2(weights)
        acc = jnp.zeros((2 * rows, HEAD_DIM), jnp.float32)
        for p in range(8):
            mask = row_masks[p]
            stacked = jnp.concatenate([w_high * mask, w_low * mask], axis=0)
            acc = acc + mm(stacked, values(p))
        acc = (acc[:rows] + acc[rows:]) / total
        return acc, top + jnp.log(total)

    lane_id = lanes_of((8, 128))

    lane_part = lane_id // span
    chunk_lanes = ratio * span

    def pack_acc(acc, k):
        merged = None
        for i in range(ratio):
            turn = (span * (i - k)) % HEAD_DIM
            moved = acc[8 * i : 8 * i + 8]
            if turn:
                moved = pltpu.roll(moved, turn, 1)
            merged = moved if merged is None else jnp.where(lane_part == i, moved, merged)
        return merged

    def pack_lse(lse):
        merged = jnp.zeros((8, 128), jnp.float32)
        for i in range(ratio):
            merged = jnp.where(lane_part == i, lse[8 * i : 8 * i + 8], merged)
        return merged

    for step in range(1, ranks):
        source = kv_from(step)
        arrive(
            near_q_send.at[source],
            near_q_recv.at[source],
            nq_ss.at[step],
            nq_rs.at[step],
            {"kv": source},
        )
    load_r.wait()
    near_scale = jnp.zeros((8, 128), jnp.float32)
    for k in range(ranks):
        near_scale = jnp.where(kv == k, page_scale[8 * k : 8 * k + 8], near_scale)
    near_length = column_of(meta[3:4], meta[5:6], 0)
    for j in range(kv_here):
        queries = []
        for i in range(ratio):
            head = j * ratio + i
            cols = slice(head * HEAD_DIM, (head + 1) * HEAD_DIM)
            total = near_q_send[kv, :, cols]
            for step in range(1, ranks):
                total = total + near_q_recv[kv_from(step), :, cols]
            queries.append(total * near_scale)
        cols = slice(j * HEAD_DIM, (j + 1) * HEAD_DIM)
        acc, lse = page_tile(
            queries,
            lambda p: res_v[p, 0, :, cols],
            lambda p: res_v[p, 1, :, cols],
            near_length,
        )
        near_lse = pack_lse(lse)
        for k in range(ranks):
            near_send[k, j, :8] = pack_acc(acc, k)
            near_send[k, j, 8:] = near_lse
    near_recv[kv] = near_send[kv]
    for step in range(1, ranks):
        peer = kv_peer(step)
        remote(near_send.at[peer], near_recv.at[kv], na_ss.at[step], na_rs.at[step], {"kv": peer})
    send_pages(2, 1)
    send_pages(3, 0)
    send_pages(3, 1)

    for step in range(1, everyone):
        source = all_from(step)
        arrive(
            far_q_send.at[source],
            far_q_recv.at[source],
            fq_ss.at[step],
            fq_rs.at[step],
            flat(source),
        )
    far_lengths = []
    for t in range(tiles):
        offset = grp * NPR
        one, two = meta_v[(2 * t) * ranks + kv], meta_v[(2 * t + 1) * ranks + kv]
        first = column_of(one[1:2], one[4:5], offset)
        second = column_of(two[1:2], two[4:5], offset - 4)
        far_lengths.append(jnp.where(rows_of((8, 1)) < 4, first, second))
    upper = rows_of((8, 128)) < 4

    def far_attention(c):
        for t in range(tiles):
            queries = []
            for i in range(ratio):
                head = c * ratio + i
                k = head // hg
                wide_q = unfold(
                    far_q_recv[(2 * t) * ranks + k],
                    far_q_recv[(2 * t + 1) * ranks + k],
                    hgw,
                    odd_here,
                )
                at = (head % hg) * HEAD_DIM
                queries.append(wide_q[:, at : at + HEAD_DIM])
            acc, lse = page_tile(
                queries,
                lambda p: sorted_v[c][0, 8 * t + p],
                lambda p: sorted_v[c][1, 8 * t + p],
                far_lengths[t],
            )
            lse = pack_lse(lse)
            for k in range(ranks):
                tile = pack_acc(acc, k)
                far_send[c, (2 * t) * ranks + k] = jnp.where(upper, tile, half_turn(lse))
                far_send[c, (2 * t + 1) * ranks + k] = jnp.where(upper, half_turn(tile), lse)
        far_recv[c, me] = far_send[c, me]
        for step in range(1, everyone):
            peer = all_peer(step)
            remote(
                far_send.at[c, peer],
                far_recv.at[c, me],
                fa_ss.at[c, step],
                fa_rs.at[c, step],
                flat(peer),
            )

    choose = (
        rows_of((HEAD_DIM, 128)) == kv * span + lax.rem(lanes_of((HEAD_DIM, 128)), span)
    ).astype(jnp.bfloat16)
    used = 8 * count_tiles
    diagonal = (row_id == lax.rem(lane_id, 8)).astype(jnp.float32)
    slot_id = rows_of((slots, 128)).astype(jnp.float32)
    wide_lane = lanes_of((slots, 128))
    slot_lanes = [jnp.sum(column * diagonal, axis=0, keepdims=True) for column in slot_rows]

    def wait_far(c):
        for step in range(1, everyone):
            source = all_from(step)
            arrive(
                far_send.at[c, source],
                far_recv.at[c, source],
                fa_ss.at[c, step],
                fa_rs.at[c, step],
                flat(source),
            )

    def combine(c):
        for k in range(ranks):
            all_acc[8 * k : 8 * k + 8, :] = near_recv[k, c, :8]
            all_lse[8 * k : 8 * k + 8, :] = near_recv[k, c, 8:]
            for t in range(tiles):
                at = 8 * (ranks + k * tiles + t)
                one, two = far_recv[c, (2 * t) * ranks + k], far_recv[c, (2 * t + 1) * ranks + k]
                all_acc[at : at + 8, :] = jnp.where(upper, one, half_turn(two))
                all_lse[at : at + 8, :] = jnp.where(upper, half_turn(one), two)
        top = jnp.full((slots, 128), neg_fill, jnp.float32)
        for i, owner_lane in enumerate(slot_lanes):
            value = jnp.sum(all_lse[8 * i : 8 * i + 8, :] * diagonal, axis=0, keepdims=True)
            top = jnp.maximum(top, jnp.where(slot_id == owner_lane, value, neg_fill))
        for shift in (1, 2, 4):
            up = pltpu.roll(top, shift, 1)
            down = pltpu.roll(top, 128 - shift, 1)
            top = jnp.maximum(top, jnp.where((wide_lane & shift) != 0, up, down))
        widen = (
            rows_of((128, 128)) == c * ratio + lanes_of((128, 128)) // span
        ).astype(jnp.bfloat16)
        high, middle, low = split3(own_all)
        own_score = mm(high, widen) + mm(middle, widen) + mm(low, widen)
        top = jnp.maximum(top, own_score)
        high, middle, low = split3(top)
        page_top = mm(hot, high) + mm(hot, middle) + mm(hot, low)
        page_weight = jnp.exp(all_lse[...] - page_top)
        own_weight = jnp.exp(own_score - top)
        hot_t = onehot_t[...]
        high, low = split2(page_weight)
        total = mm(hot_t, high) + mm(hot_t, low) + own_weight
        high, low = split2(all_acc[...] * page_weight)
        gathered = mm(hot_t, high) + mm(hot_t, low)
        values = token_v[:, :, c * HEAD_DIM : (c + 1) * HEAD_DIM].astype(jnp.float32)[:, 1]
        own_piece = mm(values.astype(jnp.bfloat16), choose)
        return (gathered + own_weight * own_piece) / total

    far_attention(0)
    sort_pages(1, 1)
    far_attention(1)
    forward_pages(1, 1)
    sort_pages(2, 0)
    sort_pages(2, 1)
    far_attention(2)
    middle = groups // 2
    forward_pages(2, 0, (middle,), False)
    onehot_t[...] = jnp.transpose(onehot[...]).astype(jnp.bfloat16)
    for at in range(used, all_lse.shape[0], 8):
        all_lse[at : at + 8, :] = jnp.zeros((8, 128), jnp.float32)
        all_acc[at : at + 8, :] = jnp.zeros((8, 128), jnp.float32)
    for step in range(1, ranks):
        source = kv_from(step)
        arrive(own_send, own_recv.at[source], own_ss.at[step], own_rs.at[step], {"kv": source})
        arrive(
            near_send.at[source],
            near_recv.at[source],
            na_ss.at[step],
            na_rs.at[step],
            {"kv": source},
        )
    own_t[...] = jnp.zeros((128, slots), jnp.float32)
    own_sum = own_recv[0]
    for k in range(1, ranks):
        own_sum = own_sum + own_recv[k]
    own_t[:heads, :] = own_sum * row_scale
    own_all = jnp.transpose(own_t[...])
    rows16 = piece_v.shape[2]
    half = ranks * rows16
    for i in range(feature_v.shape[0]):
        mine = hidden[:, i * cw : (i + 1) * cw].reshape(ranks, 2, rows16, cw)
        mine = jnp.where(tp == 0, mine[:, 0], mine[:, 1]).reshape(half, cw)
        feature_v[i] = mine.astype(jnp.float32)
    sort_pages(3, 0)
    sort_pages(3, 1)
    far_attention(3)
    forward_pages(2, 0, tuple(step for step in every_step if step != middle))
    forward_pages(2, 1)
    forward_pages(3, 0)
    forward_pages(3, 1)
    fits = 128 // chunk_lanes
    for c in range(kv_here):
        wait_far(c)
        turned = combine(c)
        if fits > 1:
            turned = pltpu.roll(turned, (c * chunk_lanes) % 128, 1)
        if c % fits == 0:
            merged = turned
        else:
            merged = jnp.where(wide_lane // chunk_lanes == c % fits, turned, merged)
        if c % fits == fits - 1:
            last = c // fits
            piece_v[:, :, :, last * 128 : (last + 1) * 128] = merged.astype(jnp.bfloat16).reshape(
                ranks, 2, rows16, 128
            )
            ordered = jnp.concatenate(
                [
                    piece_v[:, side, :, last * 128 : (last + 1) * 128].reshape(half, 128)
                    for side in (1 - tp, tp)
                ],
                axis=0,
            )
            if c == 0 or fits > 1:
                load_o.wait()
            if c < kv_here - 1:
                for d in range(chunks):
                    value = mm(
                        ordered, wo_v[last * 128 : (last + 1) * 128, d * cw : (d + 1) * cw]
                    )
                    branch_v[d] = value if last == 0 else branch_v[d] + value

    def scatter_start(c, value, send, recv, ss, rs):
        send[c] = value[:half].astype(jnp.bfloat16)
        remote(send.at[c], recv.at[c], ss.at[c], rs.at[c], partner)
        keep_v[c] = value[half:]

    def scatter_middle(c, extra, first, second, sems1, sems2):
        arrive(first[0].at[c], first[1].at[c], sems1[0].at[c], sems1[1].at[c], partner)
        both = keep_v[c] + first[1][c].astype(jnp.float32)
        if extra is not None:
            both = both + extra
        second[0][c] = both.astype(jnp.bfloat16).reshape(ranks, rows16, cw)
        second[1][c, kv] = second[0][c, kv]
        for step in range(1, ranks):
            peer = kv_peer(step)
            remote(
                second[0].at[c, peer],
                second[1].at[c, kv],
                sems2[0].at[c, step],
                sems2[1].at[c, step],
                {"kv": peer},
            )

    def scatter_end(c, second, sems2):
        for step in range(1, ranks):
            source = kv_from(step)
            arrive(
                second[0].at[c, source],
                second[1].at[c, source],
                sems2[0].at[c, step],
                sems2[1].at[c, step],
                {"kv": source},
            )
        total = second[1][c, 0].astype(jnp.float32)
        for j in range(1, ranks):
            total = total + second[1][c, j].astype(jnp.float32)
        return total

    width_here = hidden.shape[1]
    lag = 2
    for c in range(chunks + lag):
        if c < chunks:
            value = mm(ordered, wo_v[last * 128 : (last + 1) * 128, c * cw : (c + 1) * cw])
            if last > 0:
                value = value + branch_v[c]
            scatter_start(c, value, r1_send, r1_recv, r1_ss, r1_rs)
        if c >= lag:
            d = c - lag
            mine = feature_v[d % feature_v.shape[0]]
            mine = jnp.where(kv == (d * cw) // width_here, mine, 0.0)
            scatter_middle(
                d, mine, (r1_send, r1_recv), (r2_send, r2_recv), (r1_ss, r1_rs), (r2_ss, r2_rs)
            )
    for c in range(chunks):
        block = scatter_end(c, (r2_send, r2_recv), (r2_ss, r2_rs)).astype(jnp.bfloat16)
        kept_v[c] = block
        resid_v[c, 1, kv] = block
        for step in range(1, ranks):
            remote(
                kept_v.at[c],
                resid_v.at[c, 1, kv],
                g_ss.at[c, step],
                g_rs.at[c, step],
                {"kv": kv_peer(step)},
            )
        remote(kept_v.at[c], resid_v.at[c, 0, kv], gp_ss.at[c, 0], gp_rs.at[c, 0], partner)
    square_sum = jnp.zeros((2 * half, 1), jnp.float32)
    for c in range(chunks + 1):
        if c < chunks:
            for step in range(1, ranks):
                source = kv_from(step)
                arrive(
                    kept_v.at[c],
                    resid_v.at[c, 1, source],
                    g_ss.at[c, step],
                    g_rs.at[c, step],
                    {"kv": source},
                )
                remote(
                    resid_v.at[c, 1, source],
                    resid_v.at[c, 0, source],
                    gp_ss.at[c, step],
                    gp_rs.at[c, step],
                    partner,
                )
        if c >= 1:
            d = c - 1
            for step in range(ranks):
                source = kv_from(step)
                arrive(
                    kept_v.at[d],
                    resid_v.at[d, 0, source],
                    gp_ss.at[d, step],
                    gp_rs.at[d, step],
                    partner,
                )
            block = resid_v[d].reshape(2 * half, cw).astype(jnp.float32)
            square_sum = square_sum + jnp.sum(block * block, axis=1, keepdims=True)
            normed = (block * mlp_gain[:, d * cw : (d + 1) * cw]).astype(jnp.bfloat16)
            slot = d % ring
            for copy in gate_loads(d):
                copy.wait()
            if d == 0:
                gate_v[...] = mm(normed, wg_v[slot])
                up_v[...] = mm(normed, wu_v[slot])
            else:
                gate_v[...] += mm(normed, wg_v[slot])
                up_v[...] += mm(normed, wu_v[slot])
            if d + ring < chunks:
                for copy in gate_loads(d + ring):
                    copy.start()
    mlp_scale = lax.rsqrt(square_sum / D + norm_eps)
    gate = gate_v[...] * mlp_scale
    units_v[...] = (gate / (1.0 + jnp.exp(-gate)) * (up_v[...] * mlp_scale)).astype(jnp.bfloat16)
    for c in range(chunks + lag):
        if c < chunks:
            down_load(c).wait()
            value = mm(units_v[...], wd_v[c % down_ring])
            scatter_start(c, value, d1_send, d1_recv, d1_ss, d1_rs)
            if c + down_ring < chunks:
                down_load(c + down_ring).start()
        if c >= lag:
            scatter_middle(
                c - lag,
                None,
                (d1_send, d1_recv),
                (d2_send, d2_recv),
                (d1_ss, d1_rs),
                (d2_ss, d2_rs),
            )
    for c in range(chunks):
        total = scatter_end(c, (d2_send, d2_recv), (d2_ss, d2_rs))
        total = total + kept_v[c].astype(jnp.float32)
        mixed_out[:, c * cw : (c + 1) * cw] = total.astype(jnp.bfloat16)
    for c in range(kv_here):
        cols = pl.ds(c * HEAD_DIM, HEAD_DIM)
        for kind in range(2):
            for step in range(1, groups):
                source = grp_from(step)
                arrive(
                    sorted_v[c].at[kind, pages_of(source)],
                    arrived_out.at[pages_of(source), kind, :, cols],
                    z_ss.at[c, kind, step],
                    z_rs.at[c, kind, step],
                    {"grp": source},
                )
    for store in stores:
        store.wait()
    for copy in pending:
        copy.wait_send()


def fused_step(dims, *args):
    owner, hidden, token_kv, wq, pool, res, wo = (args[i] for i in (0, 6, 8, 9, 10, 11, 12))
    wg, wu, wd = args[14:]
    groups, ranks, cap, kv_here, heads = (dims[name] for name in ("groups", "ranks", "cap", "kv_here", "heads"))
    hgw = heads // ranks * HEAD_DIM
    part = heads * HEAD_DIM // ranks
    everyone = groups * ranks
    pages = groups * NPR
    tiles = pages // 8
    slots = hidden.shape[0]
    tokens = pool.shape[2]
    rows = 8 * (ranks + ranks * tiles)
    rows = -(-rows // 128) * 128
    model = wo.shape[1]
    cw = min(512, hidden.shape[1])
    chunks = model // cw
    block = slots // (2 * ranks)
    half_rows = slots // 2
    ring = min(RING, chunks)
    down_ring = min(DOWN_RING, chunks)
    wide = -(-owner.shape[1] // 128) * 128
    half = lambda width: width // 2 if width >= 256 else width
    f32, bf16 = jnp.float32, jnp.bfloat16
    whole = lambda count: pltpu.VMEM((count, 2, tokens, HEAD_DIM), bf16)
    pair = lambda count: pltpu.VMEM((2, count, tokens, HEAD_DIM), bf16)
    single = lambda count: pltpu.VMEM((count, tokens, HEAD_DIM), bf16)
    dma = lambda *shape: pltpu.SemaphoreType.DMA(shape)
    scratch = [
        pltpu.SMEM((2 * pages,), jnp.int32),
        pltpu.VMEM((8, wide), jnp.int32),
        pltpu.VMEM((8, wide), jnp.int32),
        pltpu.VMEM((8, 128), jnp.int32),
        pltpu.VMEM(hidden.shape, bf16),
        pltpu.VMEM(token_kv.shape, bf16),
        [whole(pool.shape[0]) for _ in range(kv_here)],
        [pair(pages) for _ in range(kv_here)],
        [single(pages) for _ in range(2 * kv_here)],
        [pair(pages) for _ in range(kv_here)],
        pltpu.VMEM(res.shape, bf16),
        pltpu.VMEM(wq.shape, bf16),
        pltpu.VMEM(wo.shape, bf16),
        pltpu.VMEM((everyone, 8, 128), jnp.int32),
        pltpu.VMEM((ranks, slots, hgw), f32),
        pltpu.VMEM((8, slots), f32),
        pltpu.VMEM((ranks, 8, slots), f32),
        pltpu.VMEM((rows, slots), f32),
        pltpu.VMEM((slots, rows), bf16),
        pltpu.VMEM((ranks, 8, heads * HEAD_DIM), f32),
        pltpu.VMEM((ranks, 8, heads * HEAD_DIM), f32),
        pltpu.VMEM((ranks, 8 * ranks * tiles, hgw), f32),
        pltpu.VMEM((ranks, 8 * ranks * tiles, hgw), f32),
        pltpu.VMEM((everyone, 8, half(hgw)), f32),
        pltpu.VMEM((everyone, 8, half(hgw)), f32),
        pltpu.VMEM((128, slots), f32),
        pltpu.VMEM((heads, slots), f32),
        pltpu.VMEM((ranks, heads, slots), f32),
        pltpu.VMEM((ranks, kv_here, 16, 128), f32),
        pltpu.VMEM((ranks, kv_here, 16, 128), f32),
        pltpu.VMEM((kv_here, everyone, 8, 128), f32),
        pltpu.VMEM((kv_here, everyone, 8, 128), f32),
        pltpu.VMEM((rows, 128), f32),
        pltpu.VMEM((rows, 128), f32),
        pltpu.VMEM((ranks, 2, block, part), bf16),
        pltpu.VMEM((chunks, slots, cw), f32),
        pltpu.VMEM((hidden.shape[1] // cw, half_rows, cw), f32),
        pltpu.VMEM((chunks, half_rows, cw), f32),
        pltpu.VMEM((chunks, half_rows, cw), bf16),
        pltpu.VMEM((chunks, half_rows, cw), bf16),
        pltpu.VMEM((chunks, ranks, block, cw), bf16),
        pltpu.VMEM((chunks, ranks, block, cw), bf16),
        pltpu.VMEM((chunks, half_rows, cw), bf16),
        pltpu.VMEM((chunks, half_rows, cw), bf16),
        pltpu.VMEM((chunks, ranks, block, cw), bf16),
        pltpu.VMEM((chunks, ranks, block, cw), bf16),
        pltpu.VMEM((chunks, block, cw), bf16),
        pltpu.VMEM((chunks, 2, ranks, block, cw), bf16),
        pltpu.VMEM((slots, wg.shape[1]), f32),
        pltpu.VMEM((slots, wg.shape[1]), f32),
        pltpu.VMEM((slots, wg.shape[1]), bf16),
        pltpu.VMEM((ring, cw, wg.shape[1]), bf16),
        pltpu.VMEM((ring, cw, wg.shape[1]), bf16),
        pltpu.VMEM((down_ring, wd.shape[0], cw), bf16),
        dma(kv_here + 5),
        dma(2, ring),
        dma(down_ring),
        dma(everyone),
        dma(everyone),
        dma(kv_here, 2, ranks),
        dma(kv_here, 2, ranks),
        dma(ranks),
        dma(ranks),
        dma(ranks),
        dma(ranks),
        dma(ranks),
        dma(ranks),
        dma(everyone),
        dma(everyone),
        dma(ranks),
        dma(ranks),
        dma(ranks),
        dma(ranks),
        dma(kv_here, everyone),
        dma(kv_here, everyone),
        dma(kv_here, 2, groups),
        dma(kv_here, 2, groups),
        dma(kv_here, 2),
        dma(chunks),
        dma(chunks),
        dma(chunks, ranks),
        dma(chunks, ranks),
        dma(chunks),
        dma(chunks),
        dma(chunks, ranks),
        dma(chunks, ranks),
        dma(chunks, ranks),
        dma(chunks, ranks),
        dma(chunks, ranks),
        dma(chunks, ranks),
    ]
    vmem = pl.BlockSpec(memory_space=pltpu.VMEM)
    hbm = pl.BlockSpec(memory_space=pl.ANY)
    return pl.pallas_call(
        functools.partial(step_kernel, dims),
        out_shape=(
            jax.ShapeDtypeStruct((block, model), bf16),
            jax.ShapeDtypeStruct((pages,) + pool.shape[1:], bf16),
            jax.ShapeDtypeStruct((8, 128), jnp.int32),
        ),
        in_specs=[vmem] * 6 + [hbm, vmem] + [hbm] * 5 + [vmem] + [hbm] * 3,
        out_specs=(vmem, hbm, vmem),
        scratch_shapes=scratch,
        compiler_params=pltpu.CompilerParams(
            collective_id=1, has_side_effects=True, vmem_limit_bytes=67043328
        ),
        name="fused_step",
    )(*args)


def settle_kernel(facts, arrived, mixed, pages_out, mixed_out, pages_v, mixed_v, in_sem, out_sem):
    count = pages_v.shape[0]
    copy_in = pltpu.make_async_copy(mixed, mixed_v, in_sem.at[count])
    copy_in.start()
    reads = []
    for c in range(count):
        read = pltpu.make_async_copy(arrived.at[facts[4, c]], pages_v.at[c], in_sem.at[c])
        read.start()
        reads.append(read)
    copy_in.wait()
    writes = [pltpu.make_async_copy(mixed_v, mixed_out, out_sem.at[count])]
    writes[0].start()
    for c in range(count):
        reads[c].wait()
        write = pltpu.make_async_copy(pages_v.at[c], pages_out.at[c], out_sem.at[c])
        write.start()
        writes.append(write)
    for write in writes:
        write.wait()


def settle(facts, arrived, mixed):
    hbm = pl.BlockSpec(memory_space=pl.ANY)
    count = arrived.shape[0]
    return pl.pallas_call(
        settle_kernel,
        out_shape=(
            jax.ShapeDtypeStruct(arrived.shape, arrived.dtype),
            jax.ShapeDtypeStruct(mixed.shape, mixed.dtype),
        ),
        in_specs=[pl.BlockSpec(memory_space=pltpu.SMEM), hbm, hbm],
        out_specs=(hbm, hbm),
        scratch_shapes=[
            pltpu.VMEM(arrived.shape, arrived.dtype),
            pltpu.VMEM(mixed.shape, mixed.dtype),
            pltpu.SemaphoreType.DMA((count + 1,)),
            pltpu.SemaphoreType.DMA((count + 1,)),
        ],
        name="settle",
    )(facts, arrived, mixed)


def per_device(
    hidden_states,
    attn_gain,
    mlp_gain,
    w_query,
    w_out,
    w_gate,
    w_up,
    w_down,
    kv_pool,
    resident_cache,
    resident_slot,
    resident_len,
    new_owner,
    new_local,
    new_slot,
    new_len,
    token_kv,
):
    groups = lax.axis_size("grp")
    ranks = lax.axis_size("kv")
    heads_here = w_query.shape[1] // HEAD_DIM
    kv_here = token_kv.shape[2] // HEAD_DIM
    dims = {
        "groups": groups,
        "ranks": ranks,
        "cap": groups * NPR // ranks,
        "kv_here": kv_here,
        "heads": heads_here,
    }
    mixed, arrived, facts = fused_step(
        dims,
        new_owner,
        new_local,
        new_slot,
        new_len,
        resident_slot,
        resident_len,
        hidden_states,
        attn_gain[None],
        token_kv,
        w_query,
        kv_pool,
        resident_cache[0],
        w_out.reshape(-1, w_out.shape[2]),
        mlp_gain[None],
        w_gate,
        w_up,
        w_down,
    )
    new_pages, mixed = settle(facts, arrived, mixed)
    return (mixed, new_pages[None])


def solution(mesh):
    return jax.shard_map(
        per_device,
        mesh=mesh,
        in_specs=(
            P("grp", "kv"),
            P("kv"),
            P(),
            P("kv", "tp"),
            P("tp", "kv", None),
            P(None, ("kv", "tp")),
            P(None, ("kv", "tp")),
            P(("kv", "tp"), None),
            P(("grp", "kv"), None, None, "tp"),
            P("grp", "kv", None, None, "tp"),
            P("grp", "kv"),
            P("grp", "kv"),
            P(),
            P(),
            P("grp", "kv"),
            P("grp", "kv"),
            P("grp", None, "tp"),
        ),
        out_specs=(P(("grp", "kv", "tp"), None), P("grp", "kv", None, None, "tp")),
        check_vma=False,
    )
```

```python
import functools

import jax
import jax.numpy as jnp
from jax import lax
from jax.experimental import pallas as pl
from jax.experimental.pallas import tpu as pltpu
from jax.sharding import PartitionSpec as P

D = 4096
HEADS = 32
KV_HEADS = 8
HEAD_DIM = 128
NPR = 4


neg_fill = -1e30
norm_eps = 1e-05


RING = 4
DOWN_RING = 4


def split2(x):
    high = x.astype(jnp.bfloat16)
    return high, (x - high.astype(jnp.float32)).astype(jnp.bfloat16)


def split3(x):
    high = x.astype(jnp.bfloat16)
    rest = x - high.astype(jnp.float32)
    middle = rest.astype(jnp.bfloat16)
    return high, middle, (rest - middle.astype(jnp.float32)).astype(jnp.bfloat16)


def mm(a, b):
    return jnp.dot(a, b, preferred_element_type=jnp.float32)


def mm_nt(a, b):
    return lax.dot_general(a, b, (((1,), (1,)), ((), ())), preferred_element_type=jnp.float32)


def rows_of(shape):
    return lax.broadcasted_iota(jnp.int32, shape, 0)


def lanes_of(shape):
    return lax.broadcasted_iota(jnp.int32, shape, 1)


def half_turn(x):
    return pltpu.roll(x, 4, 0)


def fold(tile, odd):
    if tile.shape[1] < 256:
        return tile
    half = tile.shape[1] // 2
    low, high = tile[:, :half], tile[:, half:]
    top = rows_of(low.shape) < 4
    if odd:
        return jnp.where(top, half_turn(low), high)
    return jnp.where(top, low, half_turn(high))


def pick_rows(first, second, odd):
    first = jnp.where(odd, half_turn(first), first)
    second = jnp.where(odd, second, half_turn(second))
    return jnp.where(rows_of(first.shape) < 4, first, second)


def unfold(first, second, width, odd):
    if width < 256:
        return pick_rows(first, second, odd)
    top = rows_of(first.shape) < 4
    low = jnp.where(top, first, half_turn(second))
    high = jnp.where(top, half_turn(first), second)
    return jnp.concatenate([low, high], axis=1)


def column_of(row, keys, offset):
    wide = jnp.broadcast_to(row, (8, 128)).astype(jnp.float32)
    hit = jnp.broadcast_to(keys, (8, 128)) == rows_of((8, 128)) + offset
    return jnp.sum(jnp.where(hit, wide, 0.0), axis=1, keepdims=True)


def place_in_group(groups, ranks):
    grp = lax.axis_index("grp")
    kv = lax.axis_index("kv")
    me = grp * ranks + kv

    def flat(index):
        return {"grp": index // ranks, "kv": lax.rem(index, ranks)}

    return grp, kv, me, flat


def step_kernel(
    dims,
    owner,
    local,
    new_slot,
    new_len,
    kept_slot,
    kept_len,
    hidden_hbm,
    gain,
    token_hbm,
    wq_hbm,
    pool_hbm,
    res_hbm,
    wo_hbm,
    mlp_gain,
    wg_hbm,
    wu_hbm,
    wd_hbm,
    mixed_out,
    arrived_out,
    meta_out,
    table,
    owner_v,
    local_v,
    meta,
    hidden,
    token_v,
    pool_v,
    send_v,
    recv_v,
    sorted_v,
    res_v,
    wq_v,
    wo_v,
    meta_v,
    qpart,
    ss_send,
    ss_recv,
    onehot,
    onehot_t,
    near_q_send,
    near_q_recv,
    rows_send,
    rows_recv,
    far_q_send,
    far_q_recv,
    own_t,
    own_send,
    own_recv,
    near_send,
    near_recv,
    far_send,
    far_recv,
    all_lse,
    all_acc,
    piece_v,
    branch_v,
    feature_v,
    keep_v,
    r1_send,
    r1_recv,
    r2_send,
    r2_recv,
    d1_send,
    d1_recv,
    d2_send,
    d2_recv,
    kept_v,
    resid_v,
    gate_v,
    up_v,
    units_v,
    wg_v,
    wu_v,
    wd_v,
    load_sem,
    gate_sem,
    down_sem,
    meta_ss,
    meta_rs,
    page_ss,
    page_rs,
    q_ss,
    q_rs,
    s_ss,
    s_rs,
    nq_ss,
    nq_rs,
    fq_ss,
    fq_rs,
    own_ss,
    own_rs,
    na_ss,
    na_rs,
    fa_ss,
    fa_rs,
    z_ss,
    z_rs,
    z_own,
    r1_ss,
    r1_rs,
    r2_ss,
    r2_rs,
    d1_ss,
    d1_rs,
    d2_ss,
    d2_rs,
    g_ss,
    g_rs,
    gp_ss,
    gp_rs,
):
    groups, ranks, cap, kv_here, heads = (dims[name] for name in ("groups", "ranks", "cap", "kv_here", "heads"))
    ratio = heads // kv_here
    hg = heads // ranks
    hgw = hg * HEAD_DIM
    span = HEAD_DIM // ranks
    part = heads * span
    per_tile = HEAD_DIM // span
    everyone = groups * ranks
    tiles = groups * NPR // 8
    count_tiles = ranks + ranks * tiles
    grp, kv, me, flat = place_in_group(groups, ranks)
    tp = lax.axis_index("tp")
    partner = {"tp": 1 - tp}
    odd_here = lax.rem(grp, 2) == 1
    slots = hidden.shape[0]

    def kv_peer(step):
        return lax.rem(kv + step, ranks)

    def kv_from(step):
        return lax.rem(kv - step + ranks, ranks)

    def all_peer(step):
        return lax.rem(me + step, everyone)

    def all_from(step):
        return lax.rem(me - step + everyone, everyone)

    pending = []

    def remote(src, dst, ss, rs, where):
        copy = pltpu.make_async_remote_copy(
            src_ref=src,
            dst_ref=dst,
            send_sem=ss,
            recv_sem=rs,
            device_id=where,
            device_id_type=pl.DeviceIdType.MESH,
        )
        copy.start()
        pending.append(copy)

    def arrive(src, dst, ss, rs, where):
        pltpu.make_async_remote_copy(
            src_ref=src,
            dst_ref=dst,
            send_sem=ss,
            recv_sem=rs,
            device_id=where,
            device_id_type=pl.DeviceIdType.MESH,
        ).wait_recv()

    loads = []
    for c in range(kv_here):
        cols = pl.ds(c * HEAD_DIM, HEAD_DIM)
        loads.append(
            pltpu.make_async_copy(pool_hbm.at[:, :, :, cols], pool_v[c], load_sem.at[c])
        )
    load_q = pltpu.make_async_copy(wq_hbm, wq_v, load_sem.at[kv_here])
    load_r = pltpu.make_async_copy(res_hbm, res_v, load_sem.at[kv_here + 1])
    load_o = pltpu.make_async_copy(wo_hbm, wo_v, load_sem.at[kv_here + 2])
    load_h = pltpu.make_async_copy(hidden_hbm, hidden, load_sem.at[kv_here + 3])
    load_t = pltpu.make_async_copy(token_hbm, token_v, load_sem.at[kv_here + 4])
    loads[0].start()
    load_h.start()
    load_q.start()
    for copy in loads[1:]:
        copy.start()
    load_r.start()
    load_t.start()
    load_o.start()

    barrier = pltpu.get_barrier_semaphore()
    for step in range(1, everyone):
        pl.semaphore_signal(
            barrier, inc=1, device_id=flat(all_peer(step)), device_id_type=pl.DeviceIdType.MESH
        )
    pl.semaphore_signal(
        barrier, inc=1, device_id=partner, device_id_type=pl.DeviceIdType.MESH
    )
    per = owner.shape[1] // ranks
    wide = owner_v.shape[1]
    owner_v[...] = jnp.full((8, wide), -1, jnp.int32)
    local_v[...] = jnp.zeros((8, wide), jnp.int32)
    owner_v[: owner.shape[0], : owner.shape[1]] = owner[...]
    local_v[: owner.shape[0], : owner.shape[1]] = local[...]
    owners, locals_ = owner_v[...], local_v[...]
    table_row, table_lane = rows_of((8, wide)), lanes_of((8, wide))
    place = lax.rem(table_lane, per)
    column = table_lane // per

    def before(match):
        count = match.astype(jnp.int32)
        ahead, behind = count, count
        shift = 1
        while shift < per:
            ahead = ahead + jnp.where(place >= shift, pltpu.roll(ahead, shift, 1), 0)
            behind = behind + jnp.where(
                place < per - shift, pltpu.roll(behind, wide - shift, 1), 0
            )
            shift *= 2
        return ahead - count, ahead - count + behind

    def order(match):
        ahead, whole = before(match)
        for shift in range(1, groups):
            ahead = ahead + jnp.where(table_row >= shift, pltpu.roll(whole, shift, 0), 0)
        return ahead

    def total_of(values):
        return jnp.sum(jnp.sum(values, axis=0, keepdims=True))

    mine = owners == me
    mine_order = order(mine)
    for k in range(ranks):
        for a in range(cap):
            hit = mine & (mine_order == a) & (column == k)
            table[k * cap + a] = total_of(jnp.where(hit, locals_, 0))
    row_base = grp * ranks
    here = (owners >= row_base) & (owners < row_base + ranks) & (column == kv)
    here_order = order(here)
    landed = jnp.zeros((8, wide), jnp.int32)
    for k in range(ranks):
        match = here & (owners == row_base + k)
        landed = landed + jnp.where(match, k * cap + order(match), 0)
    for i in range(groups * NPR):
        hit = here & (here_order == i)
        table[ranks * cap + i] = total_of(jnp.where(hit, landed, 0))
    spot = jnp.zeros((8, wide), jnp.int32)
    for g in range(groups):
        match = (owners >= g * ranks) & (owners < (g + 1) * ranks)
        spot = spot + jnp.where(match, g * NPR + before(match)[0], 0)
    spot = jnp.where((table_row == grp) & (column == kv), spot, 0)
    spot = jnp.broadcast_to(jnp.sum(spot, axis=0, keepdims=True), (8, wide))
    spot = pltpu.roll(spot, lax.rem(wide - kv * per, wide), 1)[:1, :128]
    meta[...] = jnp.zeros((8, 128), jnp.int32)
    meta[0:1, :per] = new_slot[...]
    meta[1:2, :per] = new_len[...]
    meta[2:3, : kept_slot.shape[1]] = kept_slot[...]
    meta[3:4, : kept_slot.shape[1]] = kept_len[...]
    meta[4:5, :] = jnp.where(lanes_of((1, 128)) < per, spot, -1)
    meta[5:6, :] = lanes_of((1, 128))
    meta_out[...] = meta[...]
    pl.semaphore_wait(barrier, everyone)

    for step in range(1, everyone):
        remote(meta, meta_v.at[me], meta_ss.at[step], meta_rs.at[step], flat(all_peer(step)))
    meta_v[me] = meta[...]

    loaded = set()

    half_page = recv_v[0].shape[1]
    parts = [(0, 0, 0), (0, 0, half_page)]
    parts += [(c, kind, 0) for c in range(kv_here) for kind in range(2) if c + kind]

    def send_pages(n):
        c, kind, first = parts[n]
        tokens = pl.ds(first, recv_v[n].shape[1])
        if c not in loaded:
            loads[c].wait()
            loaded.add(c)

        def pick(i, carry):
            for a in range(cap):
                target = lax.rem(kv + i, ranks) * cap + a
                send_v[c][kind, i * cap + a, tokens] = pool_v[c][table[target], kind, tokens]
            return carry

        for a in range(cap):
            recv_v[n][kv * cap + a] = pool_v[c][table[kv * cap + a], kind, tokens]
        lax.fori_loop(1, ranks, pick, 0)
        for step in range(1, ranks):
            remote(
                send_v[c].at[kind, pl.ds(step * cap, cap), tokens],
                recv_v[n].at[pl.ds(kv * cap, cap)],
                page_ss.at[n, step],
                page_rs.at[n, step],
                {"kv": kv_peer(step)},
            )

    def sort_pages(n):
        c, kind, first = parts[n]
        tokens = pl.ds(first, recv_v[n].shape[1])
        for step in range(1, ranks):
            source = kv_from(step)
            arrive(
                send_v[c].at[kind, pl.ds(step * cap, cap), tokens],
                recv_v[n].at[pl.ds(source * cap, cap)],
                page_ss.at[n, step],
                page_rs.at[n, step],
                {"kv": source},
            )

        def sort(i, carry):
            sorted_v[c][kind, i, tokens] = recv_v[n][table[ranks * cap + i]]
            return carry

        lax.fori_loop(0, groups * NPR, sort, 0)

    def pages_of(group):
        return pl.ds(pl.multiple_of(group * NPR, NPR), NPR)

    def grp_peer(step):
        return lax.rem(grp + step, groups)

    def grp_from(step):
        return lax.rem(grp - step + groups, groups)

    stores = []

    every_step = tuple(range(1, groups))

    def forward_pages(n, steps=every_step, own=True):
        c, kind, first = parts[n]
        tokens = pl.ds(first, recv_v[n].shape[1])
        cols = pl.ds(c * HEAD_DIM, HEAD_DIM)
        for step in steps:
            peer = grp_peer(step)
            remote(
                sorted_v[c].at[kind, pages_of(peer), tokens],
                arrived_out.at[pages_of(grp), kind, tokens, cols],
                z_ss.at[n, step],
                z_rs.at[n, step],
                {"grp": peer},
            )
        if not own:
            return
        store = pltpu.make_async_copy(
            sorted_v[c].at[kind, pages_of(grp), tokens],
            arrived_out.at[pages_of(grp), kind, tokens, cols],
            z_own.at[n],
        )
        store.start()
        stores.append(store)

    send_pages(0)
    send_pages(1)
    send_pages(2)

    load_h.wait()
    load_q.wait()
    features = hidden[...].astype(jnp.float32)
    normed = (features * gain[...]).astype(jnp.bfloat16)
    for j in range(ranks):
        qpart[j] = mm(normed, wq_v[:, j * hgw : (j + 1) * hgw])
    ring, cw = wg_v.shape[0], wg_v.shape[1]
    chunks = wd_hbm.shape[1] // cw
    down_ring = wd_v.shape[0]

    def gate_loads(n):
        rows = pl.ds(n * cw, cw)
        slot = n % ring
        return (
            pltpu.make_async_copy(wg_hbm.at[rows], wg_v.at[slot], gate_sem.at[0, slot]),
            pltpu.make_async_copy(wu_hbm.at[rows], wu_v.at[slot], gate_sem.at[1, slot]),
        )

    def down_load(c):
        slot = c % down_ring
        return pltpu.make_async_copy(
            wd_hbm.at[:, pl.ds(c * cw, cw)], wd_v.at[slot], down_sem.at[slot]
        )

    for n in range(ring):
        for copy in gate_loads(n):
            copy.start()
    for c in range(down_ring):
        down_load(c).start()
    squares = jnp.sum(features * features, axis=1, keepdims=True)
    ss_send[...] = jnp.transpose(jnp.broadcast_to(squares, (slots, 128)))[:8]
    ss_recv[kv] = ss_send[...]
    for step in range(1, ranks):
        peer = kv_peer(step)
        remote(ss_send, ss_recv.at[kv], s_ss.at[step], s_rs.at[step], {"kv": peer})
    load_t.wait()
    own_keys = token_v[...].astype(jnp.float32)[:, 0]
    slot_lane = lanes_of((slots, 128))
    own = jnp.zeros((slots, 128), jnp.float32)
    for head in range(heads):
        at = (head % hg) * HEAD_DIM
        key = own_keys[:, (head // ratio) * HEAD_DIM : (head // ratio + 1) * HEAD_DIM]
        score = jnp.sum(qpart[head // hg, :, at : at + HEAD_DIM] * key, axis=1, keepdims=True)
        own = jnp.where(slot_lane == head, score, own)
    own_send[...] = jnp.transpose(own)[:heads]
    own_recv[kv] = own_send[...]

    for step in range(1, everyone):
        source = all_from(step)
        arrive(meta, meta_v.at[source], meta_ss.at[step], meta_rs.at[step], flat(source))
    slot_rows = []
    for k in range(ranks):
        facts = meta_v[grp * ranks + k]
        slot_rows.append(column_of(facts[2:3], facts[5:6], 0))
    for k in range(ranks):
        facts = meta_v[grp * ranks + k]
        for t in range(tiles):
            slot_rows.append(column_of(facts[0:1], facts[4:5], 8 * t))
    for i, column in enumerate(slot_rows):
        onehot[8 * i : 8 * i + 8, :] = (
            column == lanes_of((8, slots)).astype(jnp.float32)
        ).astype(jnp.float32)
    for i in range(8 * count_tiles, onehot.shape[0], 8):
        onehot[i : i + 8, :] = jnp.zeros((8, slots), jnp.float32)

    hot = onehot[...].astype(jnp.bfloat16)

    def spread_rows(value):
        high, middle, low = split3(value)
        return mm(hot, high) + mm(hot, middle) + mm(hot, low)

    far_rows = 8 * ranks * tiles
    for j in range(ranks):
        chosen = spread_rows(qpart[j])
        for k in range(ranks):
            near_q_send[k, :, j * hgw : (j + 1) * hgw] = chosen[8 * k : 8 * k + 8]
        rows_send[j] = chosen[8 * ranks : 8 * ranks + far_rows]
    for step in range(1, ranks):
        peer = kv_peer(step)
        remote(rows_send.at[peer], rows_recv.at[kv], q_ss.at[step], q_rs.at[step], {"kv": peer})
        remote(
            near_q_send.at[peer], near_q_recv.at[kv], nq_ss.at[step], nq_rs.at[step], {"kv": peer}
        )
        remote(own_send, own_recv.at[kv], own_ss.at[step], own_rs.at[step], {"kv": peer})
    send_pages(3)
    send_pages(4)
    sort_pages(0)
    forward_pages(0)
    sort_pages(1)
    forward_pages(1)
    sort_pages(2)
    forward_pages(2)

    for step in range(1, ranks):
        source = kv_from(step)
        arrive(ss_send, ss_recv.at[source], s_ss.at[step], s_rs.at[step], {"kv": source})
        arrive(
            rows_send.at[source], rows_recv.at[source], q_ss.at[step], q_rs.at[step], {"kv": source}
        )
    total_ss = ss_recv[0]
    for j in range(1, ranks):
        total_ss = total_ss + ss_recv[j]
    row_scale = lax.rsqrt(total_ss[0:1] / D + norm_eps) * HEAD_DIM ** (-0.5)
    page_scale = spread_rows(jnp.transpose(jnp.broadcast_to(row_scale, (128, slots))))
    far_scale = page_scale[8 * ranks : 8 * ranks + far_rows]
    chosen = []
    for i in range(hg):
        cols = slice(i * HEAD_DIM, (i + 1) * HEAD_DIM)
        total = rows_send[kv, :, cols]
        for step in range(1, ranks):
            total = total + rows_recv[kv_from(step), :, cols]
        chosen.append(total * far_scale)
    chosen = jnp.concatenate(chosen, axis=1)
    for k in range(ranks):
        for t in range(tiles):
            at = 8 * (k * tiles + t)
            tile = chosen[at : at + 8]
            far_q_send[(2 * t) * ranks + k] = fold(tile, False)
            far_q_send[(2 * t + 1) * ranks + k] = fold(tile, True)
    far_q_recv[me] = far_q_send[me]
    for step in range(1, everyone):
        peer = all_peer(step)
        remote(
            far_q_send.at[peer], far_q_recv.at[me], fq_ss.at[step], fq_rs.at[step], flat(peer)
        )

    send_pages(5)
    sort_pages(3)
    forward_pages(3)

    row_id = rows_of((8, 128))
    row_masks = [
        jnp.concatenate([(row_id == p).astype(jnp.bfloat16)] * ratio, axis=0) for p in range(8)
    ]

    def page_tile(queries, keys, values, lengths):
        q_high, q_middle, q_low = split3(jnp.concatenate(queries, axis=0))
        rows = 8 * ratio
        scores = jnp.zeros((3 * rows, HEAD_DIM), jnp.float32)
        for p in range(8):
            mask = row_masks[p]
            stacked = jnp.concatenate([q_high * mask, q_middle * mask, q_low * mask], axis=0)
            scores = scores + mm_nt(stacked, keys(p))
        scores = scores[:rows] + scores[rows : 2 * rows] + scores[2 * rows :]
        usable = lanes_of((rows, 128)).astype(jnp.float32) < jnp.concatenate(
            [lengths] * ratio, axis=0
        )
        scores = jnp.where(usable, scores, neg_fill)
        top = jnp.max(scores, axis=1, keepdims=True)
        weights = jnp.where(usable, jnp.exp(scores - top), 0.0)
        total = jnp.sum(weights, axis=1, keepdims=True)
        w_high, w_low = split2(weights)
        acc = jnp.zeros((2 * rows, HEAD_DIM), jnp.float32)
        for p in range(8):
            mask = row_masks[p]
            stacked = jnp.concatenate([w_high * mask, w_low * mask], axis=0)
            acc = acc + mm(stacked, values(p))
        acc = (acc[:rows] + acc[rows:]) / total
        return acc, top + jnp.log(total)

    lane_id = lanes_of((8, 128))

    lane_part = lane_id // span
    chunk_lanes = ratio * span

    def pack_acc(acc, k):
        merged = None
        for i in range(ratio):
            turn = (span * (i - k)) % HEAD_DIM
            moved = acc[8 * i : 8 * i + 8]
            if turn:
                moved = pltpu.roll(moved, turn, 1)
            merged = moved if merged is None else jnp.where(lane_part == i, moved, merged)
        return merged

    def pack_lse(lse):
        merged = jnp.zeros((8, 128), jnp.float32)
        for i in range(ratio):
            merged = jnp.where(lane_part == i, lse[8 * i : 8 * i + 8], merged)
        return merged

    for step in range(1, ranks):
        source = kv_from(step)
        arrive(
            near_q_send.at[source],
            near_q_recv.at[source],
            nq_ss.at[step],
            nq_rs.at[step],
            {"kv": source},
        )
    load_r.wait()
    near_scale = jnp.zeros((8, 128), jnp.float32)
    for k in range(ranks):
        near_scale = jnp.where(kv == k, page_scale[8 * k : 8 * k + 8], near_scale)
    near_length = column_of(meta[3:4], meta[5:6], 0)
    for j in range(kv_here):
        queries = []
        for i in range(ratio):
            head = j * ratio + i
            cols = slice(head * HEAD_DIM, (head + 1) * HEAD_DIM)
            total = near_q_send[kv, :, cols]
            for step in range(1, ranks):
                total = total + near_q_recv[kv_from(step), :, cols]
            queries.append(total * near_scale)
        cols = slice(j * HEAD_DIM, (j + 1) * HEAD_DIM)
        acc, lse = page_tile(
            queries,
            lambda p: res_v[p, 0, :, cols],
            lambda p: res_v[p, 1, :, cols],
            near_length,
        )
        near_lse = pack_lse(lse)
        for k in range(ranks):
            near_send[k, j, :8] = pack_acc(acc, k)
            near_send[k, j, 8:] = near_lse
    near_recv[kv] = near_send[kv]
    for step in range(1, ranks):
        peer = kv_peer(step)
        remote(near_send.at[peer], near_recv.at[kv], na_ss.at[step], na_rs.at[step], {"kv": peer})
    send_pages(6)
    send_pages(7)
    send_pages(8)

    sort_pages(4)
    forward_pages(4)
    for step in range(1, everyone):
        source = all_from(step)
        arrive(
            far_q_send.at[source],
            far_q_recv.at[source],
            fq_ss.at[step],
            fq_rs.at[step],
            flat(source),
        )
    far_lengths = []
    for t in range(tiles):
        offset = grp * NPR
        one, two = meta_v[(2 * t) * ranks + kv], meta_v[(2 * t + 1) * ranks + kv]
        first = column_of(one[1:2], one[4:5], offset)
        second = column_of(two[1:2], two[4:5], offset - 4)
        far_lengths.append(jnp.where(rows_of((8, 1)) < 4, first, second))
    upper = rows_of((8, 128)) < 4

    def far_attention(c):
        for t in range(tiles):
            queries = []
            for i in range(ratio):
                head = c * ratio + i
                k = head // hg
                wide_q = unfold(
                    far_q_recv[(2 * t) * ranks + k],
                    far_q_recv[(2 * t + 1) * ranks + k],
                    hgw,
                    odd_here,
                )
                at = (head % hg) * HEAD_DIM
                queries.append(wide_q[:, at : at + HEAD_DIM])
            acc, lse = page_tile(
                queries,
                lambda p: sorted_v[c][0, 8 * t + p],
                lambda p: sorted_v[c][1, 8 * t + p],
                far_lengths[t],
            )
            lse = pack_lse(lse)
            for k in range(ranks):
                tile = pack_acc(acc, k)
                far_send[c, (2 * t) * ranks + k] = jnp.where(upper, tile, half_turn(lse))
                far_send[c, (2 * t + 1) * ranks + k] = jnp.where(upper, half_turn(tile), lse)
        far_recv[c, me] = far_send[c, me]
        for step in range(1, everyone):
            peer = all_peer(step)
            remote(
                far_send.at[c, peer],
                far_recv.at[c, me],
                fa_ss.at[c, step],
                fa_rs.at[c, step],
                flat(peer),
            )

    choose = (
        rows_of((HEAD_DIM, 128)) == kv * span + lax.rem(lanes_of((HEAD_DIM, 128)), span)
    ).astype(jnp.bfloat16)
    used = 8 * count_tiles
    diagonal = (row_id == lax.rem(lane_id, 8)).astype(jnp.float32)
    slot_id = rows_of((slots, 128)).astype(jnp.float32)
    wide_lane = lanes_of((slots, 128))
    slot_lanes = [jnp.sum(column * diagonal, axis=0, keepdims=True) for column in slot_rows]

    def wait_far(c):
        for step in range(1, everyone):
            source = all_from(step)
            arrive(
                far_send.at[c, source],
                far_recv.at[c, source],
                fa_ss.at[c, step],
                fa_rs.at[c, step],
                flat(source),
            )

    def combine(c):
        for k in range(ranks):
            all_acc[8 * k : 8 * k + 8, :] = near_recv[k, c, :8]
            all_lse[8 * k : 8 * k + 8, :] = near_recv[k, c, 8:]
            for t in range(tiles):
                at = 8 * (ranks + k * tiles + t)
                one, two = far_recv[c, (2 * t) * ranks + k], far_recv[c, (2 * t + 1) * ranks + k]
                all_acc[at : at + 8, :] = jnp.where(upper, one, half_turn(two))
                all_lse[at : at + 8, :] = jnp.where(upper, half_turn(one), two)
        top = jnp.full((slots, 128), neg_fill, jnp.float32)
        for i, owner_lane in enumerate(slot_lanes):
            value = jnp.sum(all_lse[8 * i : 8 * i + 8, :] * diagonal, axis=0, keepdims=True)
            top = jnp.maximum(top, jnp.where(slot_id == owner_lane, value, neg_fill))
        for shift in (1, 2, 4):
            up = pltpu.roll(top, shift, 1)
            down = pltpu.roll(top, 128 - shift, 1)
            top = jnp.maximum(top, jnp.where((wide_lane & shift) != 0, up, down))
        widen = (
            rows_of((128, 128)) == c * ratio + lanes_of((128, 128)) // span
        ).astype(jnp.bfloat16)
        high, middle, low = split3(own_all)
        own_score = mm(high, widen) + mm(middle, widen) + mm(low, widen)
        top = jnp.maximum(top, own_score)
        high, middle, low = split3(top)
        page_top = mm(hot, high) + mm(hot, middle) + mm(hot, low)
        page_weight = jnp.exp(all_lse[...] - page_top)
        own_weight = jnp.exp(own_score - top)
        hot_t = onehot_t[...]
        high, low = split2(page_weight)
        total = mm(hot_t, high) + mm(hot_t, low) + own_weight
        high, low = split2(all_acc[...] * page_weight)
        gathered = mm(hot_t, high) + mm(hot_t, low)
        values = token_v[:, :, c * HEAD_DIM : (c + 1) * HEAD_DIM].astype(jnp.float32)[:, 1]
        own_piece = mm(values.astype(jnp.bfloat16), choose)
        return (gathered + own_weight * own_piece) / total

    far_attention(0)
    far_attention(1)
    sort_pages(5)
    middle = groups // 2
    forward_pages(5, (middle,), False)
    sort_pages(6)
    far_attention(2)
    onehot_t[...] = jnp.transpose(onehot[...]).astype(jnp.bfloat16)
    for at in range(used, all_lse.shape[0], 8):
        all_lse[at : at + 8, :] = jnp.zeros((8, 128), jnp.float32)
        all_acc[at : at + 8, :] = jnp.zeros((8, 128), jnp.float32)
    for step in range(1, ranks):
        source = kv_from(step)
        arrive(own_send, own_recv.at[source], own_ss.at[step], own_rs.at[step], {"kv": source})
        arrive(
            near_send.at[source],
            near_recv.at[source],
            na_ss.at[step],
            na_rs.at[step],
            {"kv": source},
        )
    own_t[...] = jnp.zeros((128, slots), jnp.float32)
    own_sum = own_recv[0]
    for k in range(1, ranks):
        own_sum = own_sum + own_recv[k]
    own_t[:heads, :] = own_sum * row_scale
    own_all = jnp.transpose(own_t[...])
    rows16 = piece_v.shape[2]
    half = ranks * rows16
    for i in range(feature_v.shape[0]):
        mine = hidden[:, i * cw : (i + 1) * cw].reshape(ranks, 2, rows16, cw)
        mine = jnp.where(tp == 0, mine[:, 0], mine[:, 1]).reshape(half, cw)
        feature_v[i] = mine.astype(jnp.float32)
    sort_pages(7)
    sort_pages(8)
    far_attention(3)
    forward_pages(5, tuple(step for step in every_step if step != middle))
    forward_pages(6)
    forward_pages(7)
    forward_pages(8)
    fits = 128 // chunk_lanes
    for c in range(kv_here):
        wait_far(c)
        turned = combine(c)
        if fits > 1:
            turned = pltpu.roll(turned, (c * chunk_lanes) % 128, 1)
        if c % fits == 0:
            merged = turned
        else:
            merged = jnp.where(wide_lane // chunk_lanes == c % fits, turned, merged)
        if c % fits == fits - 1:
            last = c // fits
            piece_v[:, :, :, last * 128 : (last + 1) * 128] = merged.astype(jnp.bfloat16).reshape(
                ranks, 2, rows16, 128
            )
            ordered = jnp.concatenate(
                [
                    piece_v[:, side, :, last * 128 : (last + 1) * 128].reshape(half, 128)
                    for side in (1 - tp, tp)
                ],
                axis=0,
            )
            if c == 0 or fits > 1:
                load_o.wait()
            if c < kv_here - 1:
                for d in range(chunks):
                    value = mm(
                        ordered, wo_v[last * 128 : (last + 1) * 128, d * cw : (d + 1) * cw]
                    )
                    branch_v[d] = value if last == 0 else branch_v[d] + value

    def scatter_start(c, value, send, recv, ss, rs):
        send[c] = value[:half].astype(jnp.bfloat16)
        remote(send.at[c], recv.at[c], ss.at[c], rs.at[c], partner)
        keep_v[c] = value[half:]

    def scatter_middle(c, extra, first, second, sems1, sems2):
        arrive(first[0].at[c], first[1].at[c], sems1[0].at[c], sems1[1].at[c], partner)
        both = keep_v[c] + first[1][c].astype(jnp.float32)
        if extra is not None:
            both = both + extra
        second[0][c] = both.astype(jnp.bfloat16).reshape(ranks, rows16, cw)
        second[1][c, kv] = second[0][c, kv]
        for step in range(1, ranks):
            peer = kv_peer(step)
            remote(
                second[0].at[c, peer],
                second[1].at[c, kv],
                sems2[0].at[c, step],
                sems2[1].at[c, step],
                {"kv": peer},
            )

    def scatter_end(c, second, sems2):
        for step in range(1, ranks):
            source = kv_from(step)
            arrive(
                second[0].at[c, source],
                second[1].at[c, source],
                sems2[0].at[c, step],
                sems2[1].at[c, step],
                {"kv": source},
            )
        total = second[1][c, 0].astype(jnp.float32)
        for j in range(1, ranks):
            total = total + second[1][c, j].astype(jnp.float32)
        return total

    width_here = hidden.shape[1]
    lag = 2
    for c in range(chunks + lag):
        if c < chunks:
            value = mm(ordered, wo_v[last * 128 : (last + 1) * 128, c * cw : (c + 1) * cw])
            if last > 0:
                value = value + branch_v[c]
            scatter_start(c, value, r1_send, r1_recv, r1_ss, r1_rs)
        if c >= lag:
            d = c - lag
            mine = feature_v[d % feature_v.shape[0]]
            mine = jnp.where(kv == (d * cw) // width_here, mine, 0.0)
            scatter_middle(
                d, mine, (r1_send, r1_recv), (r2_send, r2_recv), (r1_ss, r1_rs), (r2_ss, r2_rs)
            )
    for c in range(chunks):
        block = scatter_end(c, (r2_send, r2_recv), (r2_ss, r2_rs)).astype(jnp.bfloat16)
        kept_v[c] = block
        resid_v[c, 1, kv] = block
        for step in range(1, ranks):
            remote(
                kept_v.at[c],
                resid_v.at[c, 1, kv],
                g_ss.at[c, step],
                g_rs.at[c, step],
                {"kv": kv_peer(step)},
            )
        remote(kept_v.at[c], resid_v.at[c, 0, kv], gp_ss.at[c, 0], gp_rs.at[c, 0], partner)
    square_sum = jnp.zeros((2 * half, 1), jnp.float32)
    for c in range(chunks + 1):
        if c < chunks:
            for step in range(1, ranks):
                source = kv_from(step)
                arrive(
                    kept_v.at[c],
                    resid_v.at[c, 1, source],
                    g_ss.at[c, step],
                    g_rs.at[c, step],
                    {"kv": source},
                )
                remote(
                    resid_v.at[c, 1, source],
                    resid_v.at[c, 0, source],
                    gp_ss.at[c, step],
                    gp_rs.at[c, step],
                    partner,
                )
        if c >= 1:
            d = c - 1
            for step in range(ranks):
                source = kv_from(step)
                arrive(
                    kept_v.at[d],
                    resid_v.at[d, 0, source],
                    gp_ss.at[d, step],
                    gp_rs.at[d, step],
                    partner,
                )
            block = resid_v[d].reshape(2 * half, cw).astype(jnp.float32)
            square_sum = square_sum + jnp.sum(block * block, axis=1, keepdims=True)
            normed = (block * mlp_gain[:, d * cw : (d + 1) * cw]).astype(jnp.bfloat16)
            slot = d % ring
            for copy in gate_loads(d):
                copy.wait()
            if d == 0:
                gate_v[...] = mm(normed, wg_v[slot])
                up_v[...] = mm(normed, wu_v[slot])
            else:
                gate_v[...] += mm(normed, wg_v[slot])
                up_v[...] += mm(normed, wu_v[slot])
            if d + ring < chunks:
                for copy in gate_loads(d + ring):
                    copy.start()
    mlp_scale = lax.rsqrt(square_sum / D + norm_eps)
    gate = gate_v[...] * mlp_scale
    units_v[...] = (gate / (1.0 + jnp.exp(-gate)) * (up_v[...] * mlp_scale)).astype(jnp.bfloat16)
    for c in range(chunks + lag):
        if c < chunks:
            down_load(c).wait()
            value = mm(units_v[...], wd_v[c % down_ring])
            scatter_start(c, value, d1_send, d1_recv, d1_ss, d1_rs)
            if c + down_ring < chunks:
                down_load(c + down_ring).start()
        if c >= lag:
            scatter_middle(
                c - lag,
                None,
                (d1_send, d1_recv),
                (d2_send, d2_recv),
                (d1_ss, d1_rs),
                (d2_ss, d2_rs),
            )
    for c in range(chunks):
        total = scatter_end(c, (d2_send, d2_recv), (d2_ss, d2_rs))
        total = total + kept_v[c].astype(jnp.float32)
        mixed_out[:, c * cw : (c + 1) * cw] = total.astype(jnp.bfloat16)
    for n, (c, kind, first) in enumerate(parts):
        tokens = pl.ds(first, recv_v[n].shape[1])
        cols = pl.ds(c * HEAD_DIM, HEAD_DIM)
        for step in range(1, groups):
            source = grp_from(step)
            arrive(
                sorted_v[c].at[kind, pages_of(source), tokens],
                arrived_out.at[pages_of(source), kind, tokens, cols],
                z_ss.at[n, step],
                z_rs.at[n, step],
                {"grp": source},
            )
    for store in stores:
        store.wait()
    for copy in pending:
        copy.wait_send()


def fused_step(dims, *args):
    owner, hidden, token_kv, wq, pool, res, wo = (args[i] for i in (0, 6, 8, 9, 10, 11, 12))
    wg, wu, wd = args[14:]
    groups, ranks, cap, kv_here, heads = (dims[name] for name in ("groups", "ranks", "cap", "kv_here", "heads"))
    hgw = heads // ranks * HEAD_DIM
    part = heads * HEAD_DIM // ranks
    everyone = groups * ranks
    pages = groups * NPR
    tiles = pages // 8
    slots = hidden.shape[0]
    tokens = pool.shape[2]
    rows = 8 * (ranks + ranks * tiles)
    rows = -(-rows // 128) * 128
    model = wo.shape[1]
    cw = min(512, hidden.shape[1])
    chunks = model // cw
    block = slots // (2 * ranks)
    half_rows = slots // 2
    ring = min(RING, chunks)
    down_ring = min(DOWN_RING, chunks)
    wide = -(-owner.shape[1] // 128) * 128
    half = lambda width: width // 2 if width >= 256 else width
    f32, bf16 = jnp.float32, jnp.bfloat16
    whole = lambda count: pltpu.VMEM((count, 2, tokens, HEAD_DIM), bf16)
    pair = lambda count: pltpu.VMEM((2, count, tokens, HEAD_DIM), bf16)
    single = lambda count, length: pltpu.VMEM((count, length, HEAD_DIM), bf16)
    dma = lambda *shape: pltpu.SemaphoreType.DMA(shape)
    scratch = [
        pltpu.SMEM((2 * pages,), jnp.int32),
        pltpu.VMEM((8, wide), jnp.int32),
        pltpu.VMEM((8, wide), jnp.int32),
        pltpu.VMEM((8, 128), jnp.int32),
        pltpu.VMEM(hidden.shape, bf16),
        pltpu.VMEM(token_kv.shape, bf16),
        [whole(pool.shape[0]) for _ in range(kv_here)],
        [pair(pages) for _ in range(kv_here)],
        [single(pages, tokens // 2)] * 2 + [single(pages, tokens)] * (2 * kv_here - 1),
        [pair(pages) for _ in range(kv_here)],
        pltpu.VMEM(res.shape, bf16),
        pltpu.VMEM(wq.shape, bf16),
        pltpu.VMEM(wo.shape, bf16),
        pltpu.VMEM((everyone, 8, 128), jnp.int32),
        pltpu.VMEM((ranks, slots, hgw), f32),
        pltpu.VMEM((8, slots), f32),
        pltpu.VMEM((ranks, 8, slots), f32),
        pltpu.VMEM((rows, slots), f32),
        pltpu.VMEM((slots, rows), bf16),
        pltpu.VMEM((ranks, 8, heads * HEAD_DIM), f32),
        pltpu.VMEM((ranks, 8, heads * HEAD_DIM), f32),
        pltpu.VMEM((ranks, 8 * ranks * tiles, hgw), f32),
        pltpu.VMEM((ranks, 8 * ranks * tiles, hgw), f32),
        pltpu.VMEM((everyone, 8, half(hgw)), f32),
        pltpu.VMEM((everyone, 8, half(hgw)), f32),
        pltpu.VMEM((128, slots), f32),
        pltpu.VMEM((heads, slots), f32),
        pltpu.VMEM((ranks, heads, slots), f32),
        pltpu.VMEM((ranks, kv_here, 16, 128), f32),
        pltpu.VMEM((ranks, kv_here, 16, 128), f32),
        pltpu.VMEM((kv_here, everyone, 8, 128), f32),
        pltpu.VMEM((kv_here, everyone, 8, 128), f32),
        pltpu.VMEM((rows, 128), f32),
        pltpu.VMEM((rows, 128), f32),
        pltpu.VMEM((ranks, 2, block, part), bf16),
        pltpu.VMEM((chunks, slots, cw), f32),
        pltpu.VMEM((hidden.shape[1] // cw, half_rows, cw), f32),
        pltpu.VMEM((chunks, half_rows, cw), f32),
        pltpu.VMEM((chunks, half_rows, cw), bf16),
        pltpu.VMEM((chunks, half_rows, cw), bf16),
        pltpu.VMEM((chunks, ranks, block, cw), bf16),
        pltpu.VMEM((chunks, ranks, block, cw), bf16),
        pltpu.VMEM((chunks, half_rows, cw), bf16),
        pltpu.VMEM((chunks, half_rows, cw), bf16),
        pltpu.VMEM((chunks, ranks, block, cw), bf16),
        pltpu.VMEM((chunks, ranks, block, cw), bf16),
        pltpu.VMEM((chunks, block, cw), bf16),
        pltpu.VMEM((chunks, 2, ranks, block, cw), bf16),
        pltpu.VMEM((slots, wg.shape[1]), f32),
        pltpu.VMEM((slots, wg.shape[1]), f32),
        pltpu.VMEM((slots, wg.shape[1]), bf16),
        pltpu.VMEM((ring, cw, wg.shape[1]), bf16),
        pltpu.VMEM((ring, cw, wg.shape[1]), bf16),
        pltpu.VMEM((down_ring, wd.shape[0], cw), bf16),
        dma(kv_here + 5),
        dma(2, ring),
        dma(down_ring),
        dma(everyone),
        dma(everyone),
        dma(2 * kv_here + 1, ranks),
        dma(2 * kv_here + 1, ranks),
        dma(ranks),
        dma(ranks),
        dma(ranks),
        dma(ranks),
        dma(ranks),
        dma(ranks),
        dma(everyone),
        dma(everyone),
        dma(ranks),
        dma(ranks),
        dma(ranks),
        dma(ranks),
        dma(kv_here, everyone),
        dma(kv_here, everyone),
        dma(2 * kv_here + 1, groups),
        dma(2 * kv_here + 1, groups),
        dma(2 * kv_here + 1),
        dma(chunks),
        dma(chunks),
        dma(chunks, ranks),
        dma(chunks, ranks),
        dma(chunks),
        dma(chunks),
        dma(chunks, ranks),
        dma(chunks, ranks),
        dma(chunks, ranks),
        dma(chunks, ranks),
        dma(chunks, ranks),
        dma(chunks, ranks),
    ]
    vmem = pl.BlockSpec(memory_space=pltpu.VMEM)
    hbm = pl.BlockSpec(memory_space=pl.ANY)
    return pl.pallas_call(
        functools.partial(step_kernel, dims),
        out_shape=(
            jax.ShapeDtypeStruct((block, model), bf16),
            jax.ShapeDtypeStruct((pages,) + pool.shape[1:], bf16),
            jax.ShapeDtypeStruct((8, 128), jnp.int32),
        ),
        in_specs=[vmem] * 6 + [hbm, vmem] + [hbm] * 5 + [vmem] + [hbm] * 3,
        out_specs=(vmem, hbm, vmem),
        scratch_shapes=scratch,
        compiler_params=pltpu.CompilerParams(
            collective_id=1, has_side_effects=True, vmem_limit_bytes=67043328
        ),
        name="fused_step",
    )(*args)


def settle_kernel(facts, arrived, mixed, pages_out, mixed_out, pages_v, mixed_v, in_sem, out_sem):
    count = pages_v.shape[0]
    copy_in = pltpu.make_async_copy(mixed, mixed_v, in_sem.at[count])
    copy_in.start()
    reads = []
    for c in range(count):
        read = pltpu.make_async_copy(arrived.at[facts[4, c]], pages_v.at[c], in_sem.at[c])
        read.start()
        reads.append(read)
    copy_in.wait()
    writes = [pltpu.make_async_copy(mixed_v, mixed_out, out_sem.at[count])]
    writes[0].start()
    for c in range(count):
        reads[c].wait()
        write = pltpu.make_async_copy(pages_v.at[c], pages_out.at[c], out_sem.at[c])
        write.start()
        writes.append(write)
    for write in writes:
        write.wait()


def settle(facts, arrived, mixed):
    hbm = pl.BlockSpec(memory_space=pl.ANY)
    count = arrived.shape[0]
    return pl.pallas_call(
        settle_kernel,
        out_shape=(
            jax.ShapeDtypeStruct(arrived.shape, arrived.dtype),
            jax.ShapeDtypeStruct(mixed.shape, mixed.dtype),
        ),
        in_specs=[pl.BlockSpec(memory_space=pltpu.SMEM), hbm, hbm],
        out_specs=(hbm, hbm),
        scratch_shapes=[
            pltpu.VMEM(arrived.shape, arrived.dtype),
            pltpu.VMEM(mixed.shape, mixed.dtype),
            pltpu.SemaphoreType.DMA((count + 1,)),
            pltpu.SemaphoreType.DMA((count + 1,)),
        ],
        name="settle",
    )(facts, arrived, mixed)


def per_device(
    hidden_states,
    attn_gain,
    mlp_gain,
    w_query,
    w_out,
    w_gate,
    w_up,
    w_down,
    kv_pool,
    resident_cache,
    resident_slot,
    resident_len,
    new_owner,
    new_local,
    new_slot,
    new_len,
    token_kv,
):
    groups = lax.axis_size("grp")
    ranks = lax.axis_size("kv")
    heads_here = w_query.shape[1] // HEAD_DIM
    kv_here = token_kv.shape[2] // HEAD_DIM
    dims = {
        "groups": groups,
        "ranks": ranks,
        "cap": groups * NPR // ranks,
        "kv_here": kv_here,
        "heads": heads_here,
    }
    mixed, arrived, facts = fused_step(
        dims,
        new_owner,
        new_local,
        new_slot,
        new_len,
        resident_slot,
        resident_len,
        hidden_states,
        attn_gain[None],
        token_kv,
        w_query,
        kv_pool,
        resident_cache[0],
        w_out.reshape(-1, w_out.shape[2]),
        mlp_gain[None],
        w_gate,
        w_up,
        w_down,
    )
    new_pages, mixed = settle(facts, arrived, mixed)
    return (mixed, new_pages[None])


def solution(mesh):
    return jax.shard_map(
        per_device,
        mesh=mesh,
        in_specs=(
            P("grp", "kv"),
            P("kv"),
            P(),
            P("kv", "tp"),
            P("tp", "kv", None),
            P(None, ("kv", "tp")),
            P(None, ("kv", "tp")),
            P(("kv", "tp"), None),
            P(("grp", "kv"), None, None, "tp"),
            P("grp", "kv", None, None, "tp"),
            P("grp", "kv"),
            P("grp", "kv"),
            P(),
            P(),
            P("grp", "kv"),
            P("grp", "kv"),
            P("grp", None, "tp"),
        ),
        out_specs=(P(("grp", "kv", "tp"), None), P("grp", "kv", None, None, "tp")),
        check_vma=False,
    )
```

```python
import functools

import jax
import jax.numpy as jnp
from jax import lax
from jax.experimental import pallas as pl
from jax.experimental.pallas import tpu as pltpu
from jax.sharding import PartitionSpec as P

D = 4096
HEADS = 32
KV_HEADS = 8
HEAD_DIM = 128
NPR = 4


neg_fill = -1e30
norm_eps = 1e-05


RING = 4
DOWN_RING = 4


def split2(x):
    high = x.astype(jnp.bfloat16)
    return high, (x - high.astype(jnp.float32)).astype(jnp.bfloat16)


def split3(x):
    high = x.astype(jnp.bfloat16)
    rest = x - high.astype(jnp.float32)
    middle = rest.astype(jnp.bfloat16)
    return high, middle, (rest - middle.astype(jnp.float32)).astype(jnp.bfloat16)


def mm(a, b):
    return jnp.dot(a, b, preferred_element_type=jnp.float32)


def mm_nt(a, b):
    return lax.dot_general(a, b, (((1,), (1,)), ((), ())), preferred_element_type=jnp.float32)


def rows_of(shape):
    return lax.broadcasted_iota(jnp.int32, shape, 0)


def lanes_of(shape):
    return lax.broadcasted_iota(jnp.int32, shape, 1)


def half_turn(x):
    return pltpu.roll(x, 4, 0)


def fold(tile, odd):
    if tile.shape[1] < 256:
        return tile
    half = tile.shape[1] // 2
    low, high = tile[:, :half], tile[:, half:]
    top = rows_of(low.shape) < 4
    if odd:
        return jnp.where(top, half_turn(low), high)
    return jnp.where(top, low, half_turn(high))


def pick_rows(first, second, odd):
    first = jnp.where(odd, half_turn(first), first)
    second = jnp.where(odd, second, half_turn(second))
    return jnp.where(rows_of(first.shape) < 4, first, second)


def unfold(first, second, width, odd):
    if width < 256:
        return pick_rows(first, second, odd)
    top = rows_of(first.shape) < 4
    low = jnp.where(top, first, half_turn(second))
    high = jnp.where(top, half_turn(first), second)
    return jnp.concatenate([low, high], axis=1)


def column_of(row, keys, offset):
    wide = jnp.broadcast_to(row, (8, 128)).astype(jnp.float32)
    hit = jnp.broadcast_to(keys, (8, 128)) == rows_of((8, 128)) + offset
    return jnp.sum(jnp.where(hit, wide, 0.0), axis=1, keepdims=True)


def place_in_group(groups, ranks):
    grp = lax.axis_index("grp")
    kv = lax.axis_index("kv")
    me = grp * ranks + kv

    def flat(index):
        return {"grp": index // ranks, "kv": lax.rem(index, ranks)}

    return grp, kv, me, flat


def step_kernel(
    dims,
    owner,
    local,
    new_slot,
    new_len,
    kept_slot,
    kept_len,
    hidden_hbm,
    gain,
    token_hbm,
    wq_hbm,
    pool_hbm,
    res_hbm,
    wo_hbm,
    mlp_gain,
    wg_hbm,
    wu_hbm,
    wd_hbm,
    mixed_out,
    arrived_out,
    meta_out,
    table,
    owner_v,
    local_v,
    meta,
    hidden,
    token_v,
    pool_v,
    send_v,
    recv_v,
    sorted_v,
    res_v,
    wq_v,
    wo_v,
    meta_v,
    qpart,
    ss_send,
    ss_recv,
    onehot,
    onehot_t,
    near_q_send,
    near_q_recv,
    rows_send,
    rows_recv,
    far_q_send,
    far_q_recv,
    own_t,
    own_send,
    own_recv,
    near_send,
    near_recv,
    far_send,
    far_recv,
    all_lse,
    all_acc,
    piece_v,
    branch_v,
    feature_v,
    keep_v,
    r1_send,
    r1_recv,
    r2_send,
    r2_recv,
    d1_send,
    d1_recv,
    d2_send,
    d2_recv,
    kept_v,
    resid_v,
    gate_v,
    up_v,
    units_v,
    wg_v,
    wu_v,
    wd_v,
    load_sem,
    gate_sem,
    down_sem,
    meta_ss,
    meta_rs,
    page_ss,
    page_rs,
    q_ss,
    q_rs,
    s_ss,
    s_rs,
    nq_ss,
    nq_rs,
    fq_ss,
    fq_rs,
    own_ss,
    own_rs,
    na_ss,
    na_rs,
    fa_ss,
    fa_rs,
    z_ss,
    z_rs,
    z_own,
    r1_ss,
    r1_rs,
    r2_ss,
    r2_rs,
    d1_ss,
    d1_rs,
    d2_ss,
    d2_rs,
    g_ss,
    g_rs,
    gp_ss,
    gp_rs,
):
    groups, ranks, cap, kv_here, heads = (dims[name] for name in ("groups", "ranks", "cap", "kv_here", "heads"))
    ratio = heads // kv_here
    hg = heads // ranks
    hgw = hg * HEAD_DIM
    span = HEAD_DIM // ranks
    part = heads * span
    per_tile = HEAD_DIM // span
    everyone = groups * ranks
    tiles = groups * NPR // 8
    count_tiles = ranks + ranks * tiles
    grp, kv, me, flat = place_in_group(groups, ranks)
    tp = lax.axis_index("tp")
    partner = {"tp": 1 - tp}
    odd_here = lax.rem(grp, 2) == 1
    slots = hidden.shape[0]

    def kv_peer(step):
        return lax.rem(kv + step, ranks)

    def kv_from(step):
        return lax.rem(kv - step + ranks, ranks)

    def all_peer(step):
        return lax.rem(me + step, everyone)

    def all_from(step):
        return lax.rem(me - step + everyone, everyone)

    pending = []

    def remote(src, dst, ss, rs, where):
        copy = pltpu.make_async_remote_copy(
            src_ref=src,
            dst_ref=dst,
            send_sem=ss,
            recv_sem=rs,
            device_id=where,
            device_id_type=pl.DeviceIdType.MESH,
        )
        copy.start()
        pending.append(copy)

    def arrive(src, dst, ss, rs, where):
        pltpu.make_async_remote_copy(
            src_ref=src,
            dst_ref=dst,
            send_sem=ss,
            recv_sem=rs,
            device_id=where,
            device_id_type=pl.DeviceIdType.MESH,
        ).wait_recv()

    loads = []
    for c in range(kv_here):
        cols = pl.ds(c * HEAD_DIM, HEAD_DIM)
        loads.append(
            pltpu.make_async_copy(pool_hbm.at[:, :, :, cols], pool_v[c], load_sem.at[c])
        )
    load_q = pltpu.make_async_copy(wq_hbm, wq_v, load_sem.at[kv_here])
    load_r = pltpu.make_async_copy(res_hbm, res_v, load_sem.at[kv_here + 1])
    load_o = pltpu.make_async_copy(wo_hbm, wo_v, load_sem.at[kv_here + 2])
    load_h = pltpu.make_async_copy(hidden_hbm, hidden, load_sem.at[kv_here + 3])
    load_t = pltpu.make_async_copy(token_hbm, token_v, load_sem.at[kv_here + 4])
    loads[0].start()
    load_h.start()
    load_q.start()
    for copy in loads[1:]:
        copy.start()
    load_r.start()
    load_t.start()
    load_o.start()

    barrier = pltpu.get_barrier_semaphore()
    for step in range(1, everyone):
        pl.semaphore_signal(
            barrier, inc=1, device_id=flat(all_peer(step)), device_id_type=pl.DeviceIdType.MESH
        )
    pl.semaphore_signal(
        barrier, inc=1, device_id=partner, device_id_type=pl.DeviceIdType.MESH
    )
    per = owner.shape[1] // ranks
    wide = owner_v.shape[1]
    owner_v[...] = jnp.full((8, wide), -1, jnp.int32)
    local_v[...] = jnp.zeros((8, wide), jnp.int32)
    owner_v[: owner.shape[0], : owner.shape[1]] = owner[...]
    local_v[: owner.shape[0], : owner.shape[1]] = local[...]
    owners, locals_ = owner_v[...], local_v[...]
    table_row, table_lane = rows_of((8, wide)), lanes_of((8, wide))
    place = lax.rem(table_lane, per)
    column = table_lane // per

    def before(match):
        count = match.astype(jnp.int32)
        ahead, behind = count, count
        shift = 1
        while shift < per:
            ahead = ahead + jnp.where(place >= shift, pltpu.roll(ahead, shift, 1), 0)
            behind = behind + jnp.where(
                place < per - shift, pltpu.roll(behind, wide - shift, 1), 0
            )
            shift *= 2
        return ahead - count, ahead - count + behind

    def order(match):
        ahead, whole = before(match)
        for shift in range(1, groups):
            ahead = ahead + jnp.where(table_row >= shift, pltpu.roll(whole, shift, 0), 0)
        return ahead

    def total_of(values):
        return jnp.sum(jnp.sum(values, axis=0, keepdims=True))

    mine = owners == me
    mine_order = order(mine)
    for k in range(ranks):
        for a in range(cap):
            hit = mine & (mine_order == a) & (column == k)
            table[k * cap + a] = total_of(jnp.where(hit, locals_, 0))
    row_base = grp * ranks
    here = (owners >= row_base) & (owners < row_base + ranks) & (column == kv)
    here_order = order(here)
    landed = jnp.zeros((8, wide), jnp.int32)
    for k in range(ranks):
        match = here & (owners == row_base + k)
        landed = landed + jnp.where(match, k * cap + order(match), 0)
    for i in range(groups * NPR):
        hit = here & (here_order == i)
        table[ranks * cap + i] = total_of(jnp.where(hit, landed, 0))
    spot = jnp.zeros((8, wide), jnp.int32)
    for g in range(groups):
        match = (owners >= g * ranks) & (owners < (g + 1) * ranks)
        spot = spot + jnp.where(match, g * NPR + before(match)[0], 0)
    spot = jnp.where((table_row == grp) & (column == kv), spot, 0)
    spot = jnp.broadcast_to(jnp.sum(spot, axis=0, keepdims=True), (8, wide))
    spot = pltpu.roll(spot, lax.rem(wide - kv * per, wide), 1)[:1, :128]
    meta[...] = jnp.zeros((8, 128), jnp.int32)
    meta[0:1, :per] = new_slot[...]
    meta[1:2, :per] = new_len[...]
    meta[2:3, : kept_slot.shape[1]] = kept_slot[...]
    meta[3:4, : kept_slot.shape[1]] = kept_len[...]
    meta[4:5, :] = jnp.where(lanes_of((1, 128)) < per, spot, -1)
    meta[5:6, :] = lanes_of((1, 128))
    meta_out[...] = meta[...]
    pl.semaphore_wait(barrier, everyone)

    for step in range(1, everyone):
        remote(meta, meta_v.at[me], meta_ss.at[step], meta_rs.at[step], flat(all_peer(step)))
    meta_v[me] = meta[...]

    loaded = set()

    half_page = recv_v[0].shape[1]
    parts = [(0, 0, 0), (0, 0, half_page)]
    parts += [(c, kind, 0) for c in range(kv_here) for kind in range(2) if c + kind]

    def send_pages(n):
        c, kind, first = parts[n]
        tokens = pl.ds(first, recv_v[n].shape[1])
        if c not in loaded:
            loads[c].wait()
            loaded.add(c)

        def pick(i, carry):
            for a in range(cap):
                target = lax.rem(kv + i, ranks) * cap + a
                send_v[c][kind, i * cap + a, tokens] = pool_v[c][table[target], kind, tokens]
            return carry

        for a in range(cap):
            recv_v[n][kv * cap + a] = pool_v[c][table[kv * cap + a], kind, tokens]
        lax.fori_loop(1, ranks, pick, 0)
        for step in range(1, ranks):
            remote(
                send_v[c].at[kind, pl.ds(step * cap, cap), tokens],
                recv_v[n].at[pl.ds(kv * cap, cap)],
                page_ss.at[n, step],
                page_rs.at[n, step],
                {"kv": kv_peer(step)},
            )

    def sort_pages(n):
        c, kind, first = parts[n]
        tokens = pl.ds(first, recv_v[n].shape[1])
        for step in range(1, ranks):
            source = kv_from(step)
            arrive(
                send_v[c].at[kind, pl.ds(step * cap, cap), tokens],
                recv_v[n].at[pl.ds(source * cap, cap)],
                page_ss.at[n, step],
                page_rs.at[n, step],
                {"kv": source},
            )

        def sort(i, carry):
            sorted_v[c][kind, i, tokens] = recv_v[n][table[ranks * cap + i]]
            return carry

        lax.fori_loop(0, groups * NPR, sort, 0)

    def pages_of(group):
        return pl.ds(pl.multiple_of(group * NPR, NPR), NPR)

    def grp_peer(step):
        return lax.rem(grp + step, groups)

    def grp_from(step):
        return lax.rem(grp - step + groups, groups)

    stores = []

    every_step = tuple(sorted(range(1, groups), key=lambda step: step != groups // 2))

    def forward_pages(n, steps=every_step, own=True):
        c, kind, first = parts[n]
        tokens = pl.ds(first, recv_v[n].shape[1])
        cols = pl.ds(c * HEAD_DIM, HEAD_DIM)
        for step in steps:
            peer = grp_peer(step)
            remote(
                sorted_v[c].at[kind, pages_of(peer), tokens],
                arrived_out.at[pages_of(grp), kind, tokens, cols],
                z_ss.at[n, step],
                z_rs.at[n, step],
                {"grp": peer},
            )
        if not own:
            return
        store = pltpu.make_async_copy(
            sorted_v[c].at[kind, pages_of(grp), tokens],
            arrived_out.at[pages_of(grp), kind, tokens, cols],
            z_own.at[n],
        )
        store.start()
        stores.append(store)

    send_pages(0)
    send_pages(1)
    send_pages(2)

    load_h.wait()
    load_q.wait()
    features = hidden[...].astype(jnp.float32)
    normed = (features * gain[...]).astype(jnp.bfloat16)
    for j in range(ranks):
        qpart[j] = mm(normed, wq_v[:, j * hgw : (j + 1) * hgw])
    ring, cw = wg_v.shape[0], wg_v.shape[1]
    chunks = wd_hbm.shape[1] // cw
    down_ring = wd_v.shape[0]

    def gate_loads(n):
        rows = pl.ds(n * cw, cw)
        slot = n % ring
        return (
            pltpu.make_async_copy(wg_hbm.at[rows], wg_v.at[slot], gate_sem.at[0, slot]),
            pltpu.make_async_copy(wu_hbm.at[rows], wu_v.at[slot], gate_sem.at[1, slot]),
        )

    def down_load(c):
        slot = c % down_ring
        return pltpu.make_async_copy(
            wd_hbm.at[:, pl.ds(c * cw, cw)], wd_v.at[slot], down_sem.at[slot]
        )

    for n in range(ring):
        for copy in gate_loads(n):
            copy.start()
    for c in range(down_ring):
        down_load(c).start()
    squares = jnp.sum(features * features, axis=1, keepdims=True)
    ss_send[...] = jnp.transpose(jnp.broadcast_to(squares, (slots, 128)))[:8]
    ss_recv[kv] = ss_send[...]
    for step in range(1, ranks):
        peer = kv_peer(step)
        remote(ss_send, ss_recv.at[kv], s_ss.at[step], s_rs.at[step], {"kv": peer})
    load_t.wait()
    own_keys = token_v[...].astype(jnp.float32)[:, 0]
    slot_lane = lanes_of((slots, 128))
    own = jnp.zeros((slots, 128), jnp.float32)
    for head in range(heads):
        at = (head % hg) * HEAD_DIM
        key = own_keys[:, (head // ratio) * HEAD_DIM : (head // ratio + 1) * HEAD_DIM]
        score = jnp.sum(qpart[head // hg, :, at : at + HEAD_DIM] * key, axis=1, keepdims=True)
        own = jnp.where(slot_lane == head, score, own)
    own_send[...] = jnp.transpose(own)[:heads]
    own_recv[kv] = own_send[...]

    for step in range(1, everyone):
        source = all_from(step)
        arrive(meta, meta_v.at[source], meta_ss.at[step], meta_rs.at[step], flat(source))
    slot_rows = []
    for k in range(ranks):
        facts = meta_v[grp * ranks + k]
        slot_rows.append(column_of(facts[2:3], facts[5:6], 0))
    for k in range(ranks):
        facts = meta_v[grp * ranks + k]
        for t in range(tiles):
            slot_rows.append(column_of(facts[0:1], facts[4:5], 8 * t))
    for i, column in enumerate(slot_rows):
        onehot[8 * i : 8 * i + 8, :] = (
            column == lanes_of((8, slots)).astype(jnp.float32)
        ).astype(jnp.float32)
    for i in range(8 * count_tiles, onehot.shape[0], 8):
        onehot[i : i + 8, :] = jnp.zeros((8, slots), jnp.float32)

    hot = onehot[...].astype(jnp.bfloat16)

    def spread_rows(value):
        high, middle, low = split3(value)
        return mm(hot, high) + mm(hot, middle) + mm(hot, low)

    far_rows = 8 * ranks * tiles
    for j in range(ranks):
        chosen = spread_rows(qpart[j])
        for k in range(ranks):
            near_q_send[k, :, j * hgw : (j + 1) * hgw] = chosen[8 * k : 8 * k + 8]
        rows_send[j] = chosen[8 * ranks : 8 * ranks + far_rows]
    for step in range(1, ranks):
        peer = kv_peer(step)
        remote(rows_send.at[peer], rows_recv.at[kv], q_ss.at[step], q_rs.at[step], {"kv": peer})
        remote(
            near_q_send.at[peer], near_q_recv.at[kv], nq_ss.at[step], nq_rs.at[step], {"kv": peer}
        )
        remote(own_send, own_recv.at[kv], own_ss.at[step], own_rs.at[step], {"kv": peer})
    send_pages(3)
    send_pages(4)
    sort_pages(0)
    forward_pages(0)
    sort_pages(1)
    forward_pages(1)
    sort_pages(2)
    forward_pages(2)

    for step in range(1, ranks):
        source = kv_from(step)
        arrive(ss_send, ss_recv.at[source], s_ss.at[step], s_rs.at[step], {"kv": source})
        arrive(
            rows_send.at[source], rows_recv.at[source], q_ss.at[step], q_rs.at[step], {"kv": source}
        )
    total_ss = ss_recv[0]
    for j in range(1, ranks):
        total_ss = total_ss + ss_recv[j]
    row_scale = lax.rsqrt(total_ss[0:1] / D + norm_eps) * HEAD_DIM ** (-0.5)
    page_scale = spread_rows(jnp.transpose(jnp.broadcast_to(row_scale, (128, slots))))
    far_scale = page_scale[8 * ranks : 8 * ranks + far_rows]
    chosen = []
    for i in range(hg):
        cols = slice(i * HEAD_DIM, (i + 1) * HEAD_DIM)
        total = rows_send[kv, :, cols]
        for step in range(1, ranks):
            total = total + rows_recv[kv_from(step), :, cols]
        chosen.append(total * far_scale)
    chosen = jnp.concatenate(chosen, axis=1)
    for k in range(ranks):
        for t in range(tiles):
            at = 8 * (k * tiles + t)
            tile = chosen[at : at + 8]
            far_q_send[(2 * t) * ranks + k] = fold(tile, False)
            far_q_send[(2 * t + 1) * ranks + k] = fold(tile, True)
    far_q_recv[me] = far_q_send[me]
    for step in range(1, everyone):
        peer = all_peer(step)
        remote(
            far_q_send.at[peer], far_q_recv.at[me], fq_ss.at[step], fq_rs.at[step], flat(peer)
        )

    send_pages(5)
    sort_pages(3)
    forward_pages(3)

    row_id = rows_of((8, 128))
    row_masks = [
        jnp.concatenate([(row_id == p).astype(jnp.bfloat16)] * ratio, axis=0) for p in range(8)
    ]

    def page_tile(queries, keys, values, lengths):
        q_high, q_middle, q_low = split3(jnp.concatenate(queries, axis=0))
        rows = 8 * ratio
        scores = jnp.zeros((3 * rows, HEAD_DIM), jnp.float32)
        for p in range(8):
            mask = row_masks[p]
            stacked = jnp.concatenate([q_high * mask, q_middle * mask, q_low * mask], axis=0)
            scores = scores + mm_nt(stacked, keys(p))
        scores = scores[:rows] + scores[rows : 2 * rows] + scores[2 * rows :]
        usable = lanes_of((rows, 128)).astype(jnp.float32) < jnp.concatenate(
            [lengths] * ratio, axis=0
        )
        scores = jnp.where(usable, scores, neg_fill)
        top = jnp.max(scores, axis=1, keepdims=True)
        weights = jnp.where(usable, jnp.exp(scores - top), 0.0)
        total = jnp.sum(weights, axis=1, keepdims=True)
        w_high, w_low = split2(weights)
        acc = jnp.zeros((2 * rows, HEAD_DIM), jnp.float32)
        for p in range(8):
            mask = row_masks[p]
            stacked = jnp.concatenate([w_high * mask, w_low * mask], axis=0)
            acc = acc + mm(stacked, values(p))
        acc = (acc[:rows] + acc[rows:]) / total
        return acc, top + jnp.log(total)

    lane_id = lanes_of((8, 128))

    lane_part = lane_id // span
    chunk_lanes = ratio * span

    def pack_acc(acc, k):
        merged = None
        for i in range(ratio):
            turn = (span * (i - k)) % HEAD_DIM
            moved = acc[8 * i : 8 * i + 8]
            if turn:
                moved = pltpu.roll(moved, turn, 1)
            merged = moved if merged is None else jnp.where(lane_part == i, moved, merged)
        return merged

    def pack_lse(lse):
        merged = jnp.zeros((8, 128), jnp.float32)
        for i in range(ratio):
            merged = jnp.where(lane_part == i, lse[8 * i : 8 * i + 8], merged)
        return merged

    for step in range(1, ranks):
        source = kv_from(step)
        arrive(
            near_q_send.at[source],
            near_q_recv.at[source],
            nq_ss.at[step],
            nq_rs.at[step],
            {"kv": source},
        )
    load_r.wait()
    near_scale = jnp.zeros((8, 128), jnp.float32)
    for k in range(ranks):
        near_scale = jnp.where(kv == k, page_scale[8 * k : 8 * k + 8], near_scale)
    near_length = column_of(meta[3:4], meta[5:6], 0)
    for j in range(kv_here):
        queries = []
        for i in range(ratio):
            head = j * ratio + i
            cols = slice(head * HEAD_DIM, (head + 1) * HEAD_DIM)
            total = near_q_send[kv, :, cols]
            for step in range(1, ranks):
                total = total + near_q_recv[kv_from(step), :, cols]
            queries.append(total * near_scale)
        cols = slice(j * HEAD_DIM, (j + 1) * HEAD_DIM)
        acc, lse = page_tile(
            queries,
            lambda p: res_v[p, 0, :, cols],
            lambda p: res_v[p, 1, :, cols],
            near_length,
        )
        near_lse = pack_lse(lse)
        for k in range(ranks):
            near_send[k, j, :8] = pack_acc(acc, k)
            near_send[k, j, 8:] = near_lse
    near_recv[kv] = near_send[kv]
    for step in range(1, ranks):
        peer = kv_peer(step)
        remote(near_send.at[peer], near_recv.at[kv], na_ss.at[step], na_rs.at[step], {"kv": peer})
    send_pages(6)
    send_pages(7)
    send_pages(8)

    sort_pages(4)
    forward_pages(4)
    for step in range(1, everyone):
        source = all_from(step)
        arrive(
            far_q_send.at[source],
            far_q_recv.at[source],
            fq_ss.at[step],
            fq_rs.at[step],
            flat(source),
        )
    far_lengths = []
    for t in range(tiles):
        offset = grp * NPR
        one, two = meta_v[(2 * t) * ranks + kv], meta_v[(2 * t + 1) * ranks + kv]
        first = column_of(one[1:2], one[4:5], offset)
        second = column_of(two[1:2], two[4:5], offset - 4)
        far_lengths.append(jnp.where(rows_of((8, 1)) < 4, first, second))
    upper = rows_of((8, 128)) < 4

    def far_attention(c):
        for t in range(tiles):
            queries = []
            for i in range(ratio):
                head = c * ratio + i
                k = head // hg
                wide_q = unfold(
                    far_q_recv[(2 * t) * ranks + k],
                    far_q_recv[(2 * t + 1) * ranks + k],
                    hgw,
                    odd_here,
                )
                at = (head % hg) * HEAD_DIM
                queries.append(wide_q[:, at : at + HEAD_DIM])
            acc, lse = page_tile(
                queries,
                lambda p: sorted_v[c][0, 8 * t + p],
                lambda p: sorted_v[c][1, 8 * t + p],
                far_lengths[t],
            )
            lse = pack_lse(lse)
            for k in range(ranks):
                tile = pack_acc(acc, k)
                far_send[c, (2 * t) * ranks + k] = jnp.where(upper, tile, half_turn(lse))
                far_send[c, (2 * t + 1) * ranks + k] = jnp.where(upper, half_turn(tile), lse)
        far_recv[c, me] = far_send[c, me]
        for step in range(1, everyone):
            peer = all_peer(step)
            remote(
                far_send.at[c, peer],
                far_recv.at[c, me],
                fa_ss.at[c, step],
                fa_rs.at[c, step],
                flat(peer),
            )

    choose = (
        rows_of((HEAD_DIM, 128)) == kv * span + lax.rem(lanes_of((HEAD_DIM, 128)), span)
    ).astype(jnp.bfloat16)
    used = 8 * count_tiles
    diagonal = (row_id == lax.rem(lane_id, 8)).astype(jnp.float32)
    slot_id = rows_of((slots, 128)).astype(jnp.float32)
    wide_lane = lanes_of((slots, 128))
    slot_lanes = [jnp.sum(column * diagonal, axis=0, keepdims=True) for column in slot_rows]

    def wait_far(c):
        for step in range(1, everyone):
            source = all_from(step)
            arrive(
                far_send.at[c, source],
                far_recv.at[c, source],
                fa_ss.at[c, step],
                fa_rs.at[c, step],
                flat(source),
            )

    def combine(c):
        for k in range(ranks):
            all_acc[8 * k : 8 * k + 8, :] = near_recv[k, c, :8]
            all_lse[8 * k : 8 * k + 8, :] = near_recv[k, c, 8:]
            for t in range(tiles):
                at = 8 * (ranks + k * tiles + t)
                one, two = far_recv[c, (2 * t) * ranks + k], far_recv[c, (2 * t + 1) * ranks + k]
                all_acc[at : at + 8, :] = jnp.where(upper, one, half_turn(two))
                all_lse[at : at + 8, :] = jnp.where(upper, half_turn(one), two)
        top = jnp.full((slots, 128), neg_fill, jnp.float32)
        for i, owner_lane in enumerate(slot_lanes):
            value = jnp.sum(all_lse[8 * i : 8 * i + 8, :] * diagonal, axis=0, keepdims=True)
            top = jnp.maximum(top, jnp.where(slot_id == owner_lane, value, neg_fill))
        for shift in (1, 2, 4):
            up = pltpu.roll(top, shift, 1)
            down = pltpu.roll(top, 128 - shift, 1)
            top = jnp.maximum(top, jnp.where((wide_lane & shift) != 0, up, down))
        widen = (
            rows_of((128, 128)) == c * ratio + lanes_of((128, 128)) // span
        ).astype(jnp.bfloat16)
        high, middle, low = split3(own_all)
        own_score = mm(high, widen) + mm(middle, widen) + mm(low, widen)
        top = jnp.maximum(top, own_score)
        high, middle, low = split3(top)
        page_top = mm(hot, high) + mm(hot, middle) + mm(hot, low)
        page_weight = jnp.exp(all_lse[...] - page_top)
        own_weight = jnp.exp(own_score - top)
        hot_t = onehot_t[...]
        high, low = split2(page_weight)
        total = mm(hot_t, high) + mm(hot_t, low) + own_weight
        high, low = split2(all_acc[...] * page_weight)
        gathered = mm(hot_t, high) + mm(hot_t, low)
        values = token_v[:, :, c * HEAD_DIM : (c + 1) * HEAD_DIM].astype(jnp.float32)[:, 1]
        own_piece = mm(values.astype(jnp.bfloat16), choose)
        return (gathered + own_weight * own_piece) / total

    far_attention(0)
    far_attention(1)
    sort_pages(5)
    middle = groups // 2
    forward_pages(5, (middle,), False)
    sort_pages(6)
    far_attention(2)
    onehot_t[...] = jnp.transpose(onehot[...]).astype(jnp.bfloat16)
    for at in range(used, all_lse.shape[0], 8):
        all_lse[at : at + 8, :] = jnp.zeros((8, 128), jnp.float32)
        all_acc[at : at + 8, :] = jnp.zeros((8, 128), jnp.float32)
    for step in range(1, ranks):
        source = kv_from(step)
        arrive(own_send, own_recv.at[source], own_ss.at[step], own_rs.at[step], {"kv": source})
        arrive(
            near_send.at[source],
            near_recv.at[source],
            na_ss.at[step],
            na_rs.at[step],
            {"kv": source},
        )
    own_t[...] = jnp.zeros((128, slots), jnp.float32)
    own_sum = own_recv[0]
    for k in range(1, ranks):
        own_sum = own_sum + own_recv[k]
    own_t[:heads, :] = own_sum * row_scale
    own_all = jnp.transpose(own_t[...])
    rows16 = piece_v.shape[2]
    half = ranks * rows16
    for i in range(feature_v.shape[0]):
        mine = hidden[:, i * cw : (i + 1) * cw].reshape(ranks, 2, rows16, cw)
        mine = jnp.where(tp == 0, mine[:, 0], mine[:, 1]).reshape(half, cw)
        feature_v[i] = mine.astype(jnp.float32)
    sort_pages(7)
    sort_pages(8)
    far_attention(3)
    forward_pages(5, tuple(step for step in every_step if step != middle))
    forward_pages(6)
    forward_pages(7)
    forward_pages(8)
    fits = 128 // chunk_lanes
    for c in range(kv_here):
        wait_far(c)
        turned = combine(c)
        if fits > 1:
            turned = pltpu.roll(turned, (c * chunk_lanes) % 128, 1)
        if c % fits == 0:
            merged = turned
        else:
            merged = jnp.where(wide_lane // chunk_lanes == c % fits, turned, merged)
        if c % fits == fits - 1:
            last = c // fits
            piece_v[:, :, :, last * 128 : (last + 1) * 128] = merged.astype(jnp.bfloat16).reshape(
                ranks, 2, rows16, 128
            )
            ordered = jnp.concatenate(
                [
                    piece_v[:, side, :, last * 128 : (last + 1) * 128].reshape(half, 128)
                    for side in (1 - tp, tp)
                ],
                axis=0,
            )
            if c == 0 or fits > 1:
                load_o.wait()
            if c < kv_here - 1:
                for d in range(chunks):
                    value = mm(
                        ordered, wo_v[last * 128 : (last + 1) * 128, d * cw : (d + 1) * cw]
                    )
                    branch_v[d] = value if last == 0 else branch_v[d] + value

    def scatter_start(c, value, send, recv, ss, rs):
        send[c] = value[:half].astype(jnp.bfloat16)
        remote(send.at[c], recv.at[c], ss.at[c], rs.at[c], partner)
        keep_v[c] = value[half:]

    def scatter_middle(c, extra, first, second, sems1, sems2):
        arrive(first[0].at[c], first[1].at[c], sems1[0].at[c], sems1[1].at[c], partner)
        both = keep_v[c] + first[1][c].astype(jnp.float32)
        if extra is not None:
            both = both + extra
        second[0][c] = both.astype(jnp.bfloat16).reshape(ranks, rows16, cw)
        second[1][c, kv] = second[0][c, kv]
        for step in range(1, ranks):
            peer = kv_peer(step)
            remote(
                second[0].at[c, peer],
                second[1].at[c, kv],
                sems2[0].at[c, step],
                sems2[1].at[c, step],
                {"kv": peer},
            )

    def scatter_end(c, second, sems2):
        for step in range(1, ranks):
            source = kv_from(step)
            arrive(
                second[0].at[c, source],
                second[1].at[c, source],
                sems2[0].at[c, step],
                sems2[1].at[c, step],
                {"kv": source},
            )
        total = second[1][c, 0].astype(jnp.float32)
        for j in range(1, ranks):
            total = total + second[1][c, j].astype(jnp.float32)
        return total

    width_here = hidden.shape[1]
    lag = 2
    for c in range(chunks + lag):
        if c < chunks:
            value = mm(ordered, wo_v[last * 128 : (last + 1) * 128, c * cw : (c + 1) * cw])
            if last > 0:
                value = value + branch_v[c]
            scatter_start(c, value, r1_send, r1_recv, r1_ss, r1_rs)
        if c >= lag:
            d = c - lag
            mine = feature_v[d % feature_v.shape[0]]
            mine = jnp.where(kv == (d * cw) // width_here, mine, 0.0)
            scatter_middle(
                d, mine, (r1_send, r1_recv), (r2_send, r2_recv), (r1_ss, r1_rs), (r2_ss, r2_rs)
            )
    for c in range(chunks):
        block = scatter_end(c, (r2_send, r2_recv), (r2_ss, r2_rs)).astype(jnp.bfloat16)
        kept_v[c] = block
        resid_v[c, 1, kv] = block
        for step in range(1, ranks):
            remote(
                kept_v.at[c],
                resid_v.at[c, 1, kv],
                g_ss.at[c, step],
                g_rs.at[c, step],
                {"kv": kv_peer(step)},
            )
        remote(kept_v.at[c], resid_v.at[c, 0, kv], gp_ss.at[c, 0], gp_rs.at[c, 0], partner)
    square_sum = jnp.zeros((2 * half, 1), jnp.float32)
    for c in range(chunks + 1):
        if c < chunks:
            for step in range(1, ranks):
                source = kv_from(step)
                arrive(
                    kept_v.at[c],
                    resid_v.at[c, 1, source],
                    g_ss.at[c, step],
                    g_rs.at[c, step],
                    {"kv": source},
                )
                remote(
                    resid_v.at[c, 1, source],
                    resid_v.at[c, 0, source],
                    gp_ss.at[c, step],
                    gp_rs.at[c, step],
                    partner,
                )
        if c >= 1:
            d = c - 1
            for step in range(ranks):
                source = kv_from(step)
                arrive(
                    kept_v.at[d],
                    resid_v.at[d, 0, source],
                    gp_ss.at[d, step],
                    gp_rs.at[d, step],
                    partner,
                )
            block = resid_v[d].reshape(2 * half, cw).astype(jnp.float32)
            square_sum = square_sum + jnp.sum(block * block, axis=1, keepdims=True)
            normed = (block * mlp_gain[:, d * cw : (d + 1) * cw]).astype(jnp.bfloat16)
            slot = d % ring
            for copy in gate_loads(d):
                copy.wait()
            if d == 0:
                gate_v[...] = mm(normed, wg_v[slot])
                up_v[...] = mm(normed, wu_v[slot])
            else:
                gate_v[...] += mm(normed, wg_v[slot])
                up_v[...] += mm(normed, wu_v[slot])
            if d + ring < chunks:
                for copy in gate_loads(d + ring):
                    copy.start()
    mlp_scale = lax.rsqrt(square_sum / D + norm_eps)
    gate = gate_v[...] * mlp_scale
    units_v[...] = (gate / (1.0 + jnp.exp(-gate)) * (up_v[...] * mlp_scale)).astype(jnp.bfloat16)
    for c in range(chunks + lag):
        if c < chunks:
            down_load(c).wait()
            value = mm(units_v[...], wd_v[c % down_ring])
            scatter_start(c, value, d1_send, d1_recv, d1_ss, d1_rs)
            if c + down_ring < chunks:
                down_load(c + down_ring).start()
        if c >= lag:
            scatter_middle(
                c - lag,
                None,
                (d1_send, d1_recv),
                (d2_send, d2_recv),
                (d1_ss, d1_rs),
                (d2_ss, d2_rs),
            )
    for c in range(chunks):
        total = scatter_end(c, (d2_send, d2_recv), (d2_ss, d2_rs))
        total = total + kept_v[c].astype(jnp.float32)
        mixed_out[:, c * cw : (c + 1) * cw] = total.astype(jnp.bfloat16)
    for n, (c, kind, first) in enumerate(parts):
        tokens = pl.ds(first, recv_v[n].shape[1])
        cols = pl.ds(c * HEAD_DIM, HEAD_DIM)
        for step in range(1, groups):
            source = grp_from(step)
            arrive(
                sorted_v[c].at[kind, pages_of(source), tokens],
                arrived_out.at[pages_of(source), kind, tokens, cols],
                z_ss.at[n, step],
                z_rs.at[n, step],
                {"grp": source},
            )
    for store in stores:
        store.wait()
    for copy in pending:
        copy.wait_send()


def fused_step(dims, *args):
    owner, hidden, token_kv, wq, pool, res, wo = (args[i] for i in (0, 6, 8, 9, 10, 11, 12))
    wg, wu, wd = args[14:]
    groups, ranks, cap, kv_here, heads = (dims[name] for name in ("groups", "ranks", "cap", "kv_here", "heads"))
    hgw = heads // ranks * HEAD_DIM
    part = heads * HEAD_DIM // ranks
    everyone = groups * ranks
    pages = groups * NPR
    tiles = pages // 8
    slots = hidden.shape[0]
    tokens = pool.shape[2]
    rows = 8 * (ranks + ranks * tiles)
    rows = -(-rows // 128) * 128
    model = wo.shape[1]
    cw = min(512, hidden.shape[1])
    chunks = model // cw
    block = slots // (2 * ranks)
    half_rows = slots // 2
    ring = min(RING, chunks)
    down_ring = min(DOWN_RING, chunks)
    wide = -(-owner.shape[1] // 128) * 128
    half = lambda width: width // 2 if width >= 256 else width
    f32, bf16 = jnp.float32, jnp.bfloat16
    whole = lambda count: pltpu.VMEM((count, 2, tokens, HEAD_DIM), bf16)
    pair = lambda count: pltpu.VMEM((2, count, tokens, HEAD_DIM), bf16)
    single = lambda count, length: pltpu.VMEM((count, length, HEAD_DIM), bf16)
    dma = lambda *shape: pltpu.SemaphoreType.DMA(shape)
    scratch = [
        pltpu.SMEM((2 * pages,), jnp.int32),
        pltpu.VMEM((8, wide), jnp.int32),
        pltpu.VMEM((8, wide), jnp.int32),
        pltpu.VMEM((8, 128), jnp.int32),
        pltpu.VMEM(hidden.shape, bf16),
        pltpu.VMEM(token_kv.shape, bf16),
        [whole(pool.shape[0]) for _ in range(kv_here)],
        [pair(pages) for _ in range(kv_here)],
        [single(pages, tokens // 2)] * 2 + [single(pages, tokens)] * (2 * kv_here - 1),
        [pair(pages) for _ in range(kv_here)],
        pltpu.VMEM(res.shape, bf16),
        pltpu.VMEM(wq.shape, bf16),
        pltpu.VMEM(wo.shape, bf16),
        pltpu.VMEM((everyone, 8, 128), jnp.int32),
        pltpu.VMEM((ranks, slots, hgw), f32),
        pltpu.VMEM((8, slots), f32),
        pltpu.VMEM((ranks, 8, slots), f32),
        pltpu.VMEM((rows, slots), f32),
        pltpu.VMEM((slots, rows), bf16),
        pltpu.VMEM((ranks, 8, heads * HEAD_DIM), f32),
        pltpu.VMEM((ranks, 8, heads * HEAD_DIM), f32),
        pltpu.VMEM((ranks, 8 * ranks * tiles, hgw), f32),
        pltpu.VMEM((ranks, 8 * ranks * tiles, hgw), f32),
        pltpu.VMEM((everyone, 8, half(hgw)), f32),
        pltpu.VMEM((everyone, 8, half(hgw)), f32),
        pltpu.VMEM((128, slots), f32),
        pltpu.VMEM((heads, slots), f32),
        pltpu.VMEM((ranks, heads, slots), f32),
        pltpu.VMEM((ranks, kv_here, 16, 128), f32),
        pltpu.VMEM((ranks, kv_here, 16, 128), f32),
        pltpu.VMEM((kv_here, everyone, 8, 128), f32),
        pltpu.VMEM((kv_here, everyone, 8, 128), f32),
        pltpu.VMEM((rows, 128), f32),
        pltpu.VMEM((rows, 128), f32),
        pltpu.VMEM((ranks, 2, block, part), bf16),
        pltpu.VMEM((chunks, slots, cw), f32),
        pltpu.VMEM((hidden.shape[1] // cw, half_rows, cw), f32),
        pltpu.VMEM((chunks, half_rows, cw), f32),
        pltpu.VMEM((chunks, half_rows, cw), bf16),
        pltpu.VMEM((chunks, half_rows, cw), bf16),
        pltpu.VMEM((chunks, ranks, block, cw), bf16),
        pltpu.VMEM((chunks, ranks, block, cw), bf16),
        pltpu.VMEM((chunks, half_rows, cw), bf16),
        pltpu.VMEM((chunks, half_rows, cw), bf16),
        pltpu.VMEM((chunks, ranks, block, cw), bf16),
        pltpu.VMEM((chunks, ranks, block, cw), bf16),
        pltpu.VMEM((chunks, block, cw), bf16),
        pltpu.VMEM((chunks, 2, ranks, block, cw), bf16),
        pltpu.VMEM((slots, wg.shape[1]), f32),
        pltpu.VMEM((slots, wg.shape[1]), f32),
        pltpu.VMEM((slots, wg.shape[1]), bf16),
        pltpu.VMEM((ring, cw, wg.shape[1]), bf16),
        pltpu.VMEM((ring, cw, wg.shape[1]), bf16),
        pltpu.VMEM((down_ring, wd.shape[0], cw), bf16),
        dma(kv_here + 5),
        dma(2, ring),
        dma(down_ring),
        dma(everyone),
        dma(everyone),
        dma(2 * kv_here + 1, ranks),
        dma(2 * kv_here + 1, ranks),
        dma(ranks),
        dma(ranks),
        dma(ranks),
        dma(ranks),
        dma(ranks),
        dma(ranks),
        dma(everyone),
        dma(everyone),
        dma(ranks),
        dma(ranks),
        dma(ranks),
        dma(ranks),
        dma(kv_here, everyone),
        dma(kv_here, everyone),
        dma(2 * kv_here + 1, groups),
        dma(2 * kv_here + 1, groups),
        dma(2 * kv_here + 1),
        dma(chunks),
        dma(chunks),
        dma(chunks, ranks),
        dma(chunks, ranks),
        dma(chunks),
        dma(chunks),
        dma(chunks, ranks),
        dma(chunks, ranks),
        dma(chunks, ranks),
        dma(chunks, ranks),
        dma(chunks, ranks),
        dma(chunks, ranks),
    ]
    vmem = pl.BlockSpec(memory_space=pltpu.VMEM)
    hbm = pl.BlockSpec(memory_space=pl.ANY)
    return pl.pallas_call(
        functools.partial(step_kernel, dims),
        out_shape=(
            jax.ShapeDtypeStruct((block, model), bf16),
            jax.ShapeDtypeStruct((pages,) + pool.shape[1:], bf16),
            jax.ShapeDtypeStruct((8, 128), jnp.int32),
        ),
        in_specs=[vmem] * 6 + [hbm, vmem] + [hbm] * 5 + [vmem] + [hbm] * 3,
        out_specs=(vmem, hbm, vmem),
        scratch_shapes=scratch,
        compiler_params=pltpu.CompilerParams(
            collective_id=1, has_side_effects=True, vmem_limit_bytes=67043328
        ),
        name="fused_step",
    )(*args)


def settle_kernel(facts, arrived, mixed, pages_out, mixed_out, pages_v, mixed_v, in_sem, out_sem):
    count = pages_v.shape[0]
    copy_in = pltpu.make_async_copy(mixed, mixed_v, in_sem.at[count])
    copy_in.start()
    reads = []
    for c in range(count):
        read = pltpu.make_async_copy(arrived.at[facts[4, c]], pages_v.at[c], in_sem.at[c])
        read.start()
        reads.append(read)
    copy_in.wait()
    writes = [pltpu.make_async_copy(mixed_v, mixed_out, out_sem.at[count])]
    writes[0].start()
    for c in range(count):
        reads[c].wait()
        write = pltpu.make_async_copy(pages_v.at[c], pages_out.at[c], out_sem.at[c])
        write.start()
        writes.append(write)
    for write in writes:
        write.wait()


def settle(facts, arrived, mixed):
    hbm = pl.BlockSpec(memory_space=pl.ANY)
    count = arrived.shape[0]
    return pl.pallas_call(
        settle_kernel,
        out_shape=(
            jax.ShapeDtypeStruct(arrived.shape, arrived.dtype),
            jax.ShapeDtypeStruct(mixed.shape, mixed.dtype),
        ),
        in_specs=[pl.BlockSpec(memory_space=pltpu.SMEM), hbm, hbm],
        out_specs=(hbm, hbm),
        scratch_shapes=[
            pltpu.VMEM(arrived.shape, arrived.dtype),
            pltpu.VMEM(mixed.shape, mixed.dtype),
            pltpu.SemaphoreType.DMA((count + 1,)),
            pltpu.SemaphoreType.DMA((count + 1,)),
        ],
        name="settle",
    )(facts, arrived, mixed)


def per_device(
    hidden_states,
    attn_gain,
    mlp_gain,
    w_query,
    w_out,
    w_gate,
    w_up,
    w_down,
    kv_pool,
    resident_cache,
    resident_slot,
    resident_len,
    new_owner,
    new_local,
    new_slot,
    new_len,
    token_kv,
):
    groups = lax.axis_size("grp")
    ranks = lax.axis_size("kv")
    heads_here = w_query.shape[1] // HEAD_DIM
    kv_here = token_kv.shape[2] // HEAD_DIM
    dims = {
        "groups": groups,
        "ranks": ranks,
        "cap": groups * NPR // ranks,
        "kv_here": kv_here,
        "heads": heads_here,
    }
    mixed, arrived, facts = fused_step(
        dims,
        new_owner,
        new_local,
        new_slot,
        new_len,
        resident_slot,
        resident_len,
        hidden_states,
        attn_gain[None],
        token_kv,
        w_query,
        kv_pool,
        resident_cache[0],
        w_out.reshape(-1, w_out.shape[2]),
        mlp_gain[None],
        w_gate,
        w_up,
        w_down,
    )
    new_pages, mixed = settle(facts, arrived, mixed)
    return (mixed, new_pages[None])


def solution(mesh):
    return jax.shard_map(
        per_device,
        mesh=mesh,
        in_specs=(
            P("grp", "kv"),
            P("kv"),
            P(),
            P("kv", "tp"),
            P("tp", "kv", None),
            P(None, ("kv", "tp")),
            P(None, ("kv", "tp")),
            P(("kv", "tp"), None),
            P(("grp", "kv"), None, None, "tp"),
            P("grp", "kv", None, None, "tp"),
            P("grp", "kv"),
            P("grp", "kv"),
            P(),
            P(),
            P("grp", "kv"),
            P("grp", "kv"),
            P("grp", None, "tp"),
        ),
        out_specs=(P(("grp", "kv", "tp"), None), P("grp", "kv", None, None, "tp")),
        check_vma=False,
    )
```
